8 devices in a mesh: dp: 2 (over z, y), col: 2 (over x), row: 2 (over core).
Axes of the slice: x: 2, y: 2, z: 1, core: 2. Of those that a mesh axis runs over, the one named last changes fastest.
Arguments:
- x_attn: bfloat16 [16384, 1024], P('dp', 'row')
- dy_attn: bfloat16 [16384, 1024], P('dp', 'col')
- x_mlp: bfloat16 [16384, 1024], P('dp', 'row')
- dy_gate: bfloat16 [16384, 4096], P('dp', 'col')
- dy_up: bfloat16 [16384, 4096], P('dp', 'col')
- h_mlp: bfloat16 [16384, 4096], P('dp', 'row')
- dy_out: bfloat16 [16384, 1024], P('dp', 'col')
- w_attn: float32 [1024, 1024], P('row', 'col')
- w_gate: float32 [1024, 4096], P('row', 'col')
- w_up: float32 [1024, 4096], P('row', 'col')
- w_down: float32 [4096, 1024], P('row', 'col')
- r_attn: float32 [1024], P('row')
- c_attn: float32 [1024], P('col')
- r_gate: float32 [1024], P('row')
- c_gate: float32 [4096], P('col')
- r_up: float32 [1024], P('row')
- c_up: float32 [4096], P('col')
- r_down: float32 [4096], P('row')
- c_down: float32 [1024], P('col')
- hyper_params: float32 [3], replicated
Outputs:
- output 1: float32 [1024, 1024], P('row', 'col')
- output 2: float32 [1024], P('row')
- output 3: float32 [1024], P('col')
- output 4: float32 [1024, 4096], P('row', 'col')
- output 5: float32 [1024], P('row')
- output 6: float32 [4096], P('col')
- output 7: float32 [1024, 4096], P('row', 'col')
- output 8: float32 [1024], P('row')
- output 9: float32 [4096], P('col')
- output 10: float32 [4096, 1024], P('row', 'col')
- output 11: float32 [4096], P('row')
- output 12: float32 [1024], P('col')
All inputs are finite; a program needn't handle non-finite values.
Results may differ from the reference program's by a relative error of at most 0.001.
Values are sent between devices in bfloat16 or wider.
A program may use at most 1 GiB of HBM per device.

```python
import jax
import jax.numpy as jnp

D_MODEL = 1024
D_FF = 4096
TOKENS = 16384

EPS_ONE = 1e-30
EPS_TWO = 1e-3


def draw_act(key, rows, cols, scale):
    k_val, k_slope, k_one, k_two = jax.random.split(key, 4)
    position = jnp.linspace(-1.0, 1.0, cols)
    slope_val = jax.random.uniform(k_slope, (), jnp.float32, 0.8, 1.2)
    up_scale = jnp.exp(0.5 * slope_val * position) * jax.random.uniform(k_one, (cols,), jnp.float32, 0.7, 1.3)
    down_scale = jnp.exp(-0.5 * slope_val * position) * jax.random.uniform(k_two, (cols,), jnp.float32, 0.7, 1.3)
    group_scale = jnp.stack([up_scale, down_scale])
    values = jax.random.normal(k_val, (2, rows // 2, cols), jnp.float32) * group_scale[:, None, :]
    return (values.reshape(rows, cols) * scale).astype(jnp.bfloat16)


def draw_weight(key, rows, cols):
    k_val, k_row, k_col = jax.random.split(key, 3)
    row_trend = jax.random.uniform(k_row, (), jnp.float32, 0.8, 1.2) * jnp.linspace(-0.5, 0.5, rows)
    col_trend = jax.random.uniform(k_col, (), jnp.float32, 0.8, 1.2) * jnp.linspace(-0.5, 0.5, cols)
    values = jax.random.normal(k_val, (rows, cols), jnp.float32) * jnp.exp(row_trend[:, None] + col_trend[None, :])
    return values * rows ** -0.5


def draw_stat(key, length):
    return jax.random.uniform(key, (length,), jnp.float32, 0.2, 0.8)


def setup_inputs(seed: int = 0) -> dict:
    key_list = jax.random.split(jax.random.key(seed), 20)
    dy_scale = TOKENS ** -0.5
    hyper_keys = jax.random.split(key_list[19], 3)
    hyper_params = jnp.stack([
        jax.random.uniform(hyper_keys[0], (), jnp.float32, 0.5, 0.9),
        jax.random.uniform(hyper_keys[1], (), jnp.float32, 0.5, 1.0),
        jax.random.uniform(hyper_keys[2], (), jnp.float32, 0.3, 0.6)])
    return {
        'x_attn': draw_act(key_list[0], TOKENS, D_MODEL, 1.0),
        'dy_attn': draw_act(key_list[1], TOKENS, D_MODEL, dy_scale),
        'x_mlp': draw_act(key_list[2], TOKENS, D_MODEL, 1.0),
        'dy_gate': draw_act(key_list[3], TOKENS, D_FF, dy_scale),
        'dy_up': draw_act(key_list[4], TOKENS, D_FF, dy_scale),
        'h_mlp': draw_act(key_list[5], TOKENS, D_FF, 1.0),
        'dy_out': draw_act(key_list[6], TOKENS, D_MODEL, dy_scale),
        'w_attn': draw_weight(key_list[7], D_MODEL, D_MODEL),
        'w_gate': draw_weight(key_list[8], D_MODEL, D_FF),
        'w_up': draw_weight(key_list[9], D_MODEL, D_FF),
        'w_down': draw_weight(key_list[10], D_FF, D_MODEL),
        'r_attn': draw_stat(key_list[11], D_MODEL),
        'c_attn': draw_stat(key_list[12], D_MODEL),
        'r_gate': draw_stat(key_list[13], D_MODEL),
        'c_gate': draw_stat(key_list[14], D_FF),
        'r_up': draw_stat(key_list[15], D_MODEL),
        'c_up': draw_stat(key_list[16], D_FF),
        'r_down': draw_stat(key_list[17], D_FF),
        'c_down': draw_stat(key_list[18], D_MODEL),
        'hyper_params': hyper_params,
    }


def adafactor_step(x_act, dy_act, weight, row_old, col_old, hyper_params):
    beta_two = hyper_params[0]
    rho_step = hyper_params[1]
    clip_thr = hyper_params[2]
    full_grad = jnp.dot(x_act.T, dy_act, preferred_element_type=jnp.float32)
    sq_grad = full_grad * full_grad + EPS_ONE
    new_row = beta_two * row_old + (1.0 - beta_two) * jnp.mean(sq_grad, axis=1)
    new_col = beta_two * col_old + (1.0 - beta_two) * jnp.mean(sq_grad, axis=0)
    row_total = jnp.sum(new_row)
    second_est = new_row[:, None] * new_col[None, :] / row_total
    update = full_grad / jnp.sqrt(second_est)
    upd_rms = jnp.sqrt(jnp.mean(update * update))
    update = update / jnp.maximum(1.0, upd_rms / clip_thr)
    w_rms = jnp.sqrt(jnp.mean(weight * weight))
    step_size = rho_step * jnp.maximum(EPS_TWO, w_rms)
    return (weight - step_size * update, new_row, new_col)


def reference(x_attn, dy_attn, x_mlp, dy_gate, dy_up, h_mlp, dy_out, w_attn, w_gate, w_up, w_down,
              r_attn, c_attn, r_gate, c_gate, r_up, c_up, r_down, c_down, hyper_params):
    attn_res = adafactor_step(x_attn, dy_attn, w_attn, r_attn, c_attn, hyper_params)
    gate_res = adafactor_step(x_mlp, dy_gate, w_gate, r_gate, c_gate, hyper_params)
    up_res = adafactor_step(x_mlp, dy_up, w_up, r_up, c_up, hyper_params)
    down_res = adafactor_step(h_mlp, dy_out, w_down, r_down, c_down, hyper_params)
    return (attn_res[0], attn_res[1], attn_res[2], gate_res[0], gate_res[1], gate_res[2],
            up_res[0], up_res[1], up_res[2], down_res[0], down_res[1], down_res[2])
```

```python
import jax
import jax.numpy as jnp
from jax import lax
from jax.sharding import PartitionSpec as P

EPS_ONE = 1e-30
EPS_TWO = 1e-3
SWAP = [(0, 1), (1, 0)]


def swap_sum(value, axis):
    return value + lax.ppermute(value, axis, SWAP)


def plane_sum(value):
    return swap_sum(swap_sum(value, 'row'), 'col')


def finish(part_grad, recv_grad, w_block, row_old, col_old, hyper_vals):
    beta_two = hyper_vals[0]
    rho_step = hyper_vals[1]
    clip_thr = hyper_vals[2]
    m_total = w_block.shape[0] * 2
    n_total = w_block.shape[1] * 2
    grad_block = part_grad + recv_grad
    sq_grad = grad_block * grad_block + EPS_ONE
    row_sum = swap_sum(jnp.sum(sq_grad, axis=1), 'col')
    col_sum = swap_sum(jnp.sum(sq_grad, axis=0), 'row')
    new_row = beta_two * row_old + (1.0 - beta_two) * (row_sum / n_total)
    new_col = beta_two * col_old + (1.0 - beta_two) * (col_sum / m_total)
    row_total = swap_sum(jnp.sum(new_row), 'row')
    second_est = new_row[:, None] * new_col[None, :] / row_total
    update = grad_block / jnp.sqrt(second_est)
    upd_rms = jnp.sqrt(plane_sum(jnp.sum(update * update)) / (m_total * n_total))
    update = update / jnp.maximum(1.0, upd_rms / clip_thr)
    w_rms = jnp.sqrt(plane_sum(jnp.sum(w_block * w_block)) / (m_total * n_total))
    step_size = rho_step * jnp.maximum(EPS_TWO, w_rms)
    return (w_block - step_size * update, new_row, new_col)


def solution(mesh):
    act_spec = P('dp', 'row')
    grad_spec = P('dp', 'col')
    w_spec = P('row', 'col')
    row_spec = P('row')
    col_spec = P('col')
    in_specs = (act_spec, grad_spec, act_spec, grad_spec, grad_spec, act_spec, grad_spec,
                w_spec, w_spec, w_spec, w_spec,
                row_spec, col_spec, row_spec, col_spec, row_spec, col_spec, row_spec, col_spec, P())
    out_specs = (w_spec, row_spec, col_spec) * 4

    def per_device(x_attn, dy_attn, x_mlp, dy_gate, dy_up, h_mlp, dy_out, w_attn, w_gate, w_up, w_down,
                   r_attn, c_attn, r_gate, c_gate, r_up, c_up, r_down, c_down, hyper_params):
        results = []
        for x_block, dy_block, w_block, row_old, col_old in (
                (x_mlp, dy_gate, w_gate, r_gate, c_gate),
                (x_mlp, dy_up, w_up, r_up, c_up),
                (h_mlp, dy_out, w_down, r_down, c_down),
                (x_attn, dy_attn, w_attn, r_attn, c_attn)):
            part_grad = jnp.einsum('tm,tn->mn', x_block, dy_block, preferred_element_type=jnp.float32)
            recv_grad = lax.ppermute(part_grad, 'dp', SWAP)
            results.append(finish(part_grad, recv_grad, w_block, row_old, col_old, hyper_params))
        gate, up, down, attn = results
        return attn + gate + up + down

    return jax.shard_map(per_device, mesh=mesh, in_specs=in_specs, out_specs=out_specs, check_vma=False)
```

```python
import functools
import jax
import jax.numpy as jnp
from jax import lax
from jax.experimental import pallas as pl
from jax.experimental.pallas import tpu as pltpu
from jax.sharding import PartitionSpec as P

EPS_ONE = 1e-30
EPS_TWO = 1e-3
SWAP = [(0, 1), (1, 0)]
MESH = pl.DeviceIdType.MESH
LANES = 128
NAMES = ('gate', 'up', 'down', 'attn')
GATE_WIDTHS = (256, 768, 1024)


def peers():
    row_other = 1 - lax.axis_index('row')
    col_other = 1 - lax.axis_index('col')
    return ({'row': row_other}, {'col': col_other}, {'row': row_other, 'col': col_other})


def stats_kernel(n_token, widths, step, m_total, n_total, *refs):
    n_piece = len(widths)
    refs = refs[n_token:]
    hyper, w_sq, row_old, col_old = refs[:4]
    parts = refs[4:4 + n_piece]
    recvs = refs[4 + n_piece:4 + 2 * n_piece]
    (grad, row_scale, col_scale, new_row, new_col,
     row_acc, row_col, send_row, send_col, recv_row, recv_col, send_val, recv_val,
     vec_send, vec_recv, val_send, val_recv) = refs[4 + 2 * n_piece:]
    rows, cols = grad.shape
    others = peers()
    row_peer, col_peer, _ = others

    barrier = pltpu.get_barrier_semaphore()
    for other in others:
        pl.semaphore_signal(barrier, inc=1, device_id=other, device_id_type=MESH)

    def first(i, col_acc):
        band = pl.ds(pl.multiple_of(i * step, step), step)
        lane_sum = jnp.zeros((step, LANES), jnp.float32)
        sums = []
        start = 0
        for part, recv, width in zip(parts, recvs, widths):
            piece = part[band, :] + recv[band, :]
            grad[band, start:start + width] = piece
            sq = piece * piece + EPS_ONE
            for k in range(width // LANES):
                lane_sum = lane_sum + sq[:, k * LANES:(k + 1) * LANES]
            sums.append(sq.reshape(step // 8, 8, width).sum(axis=0))
            start += width
        row_acc[band, :] = lane_sum
        return tuple(a + s for a, s in zip(col_acc, sums))

    col_acc = lax.fori_loop(0, rows // step, first, tuple(jnp.zeros((8, w), jnp.float32) for w in widths))
    start = 0
    for acc, width in zip(col_acc, widths):
        send_col[:, start:start + width] = jnp.sum(acc, axis=0, keepdims=True)
        start += width
    for k in range(rows // LANES):
        tile = row_acc[k * LANES:(k + 1) * LANES, :].T
        send_row[:, k * LANES:(k + 1) * LANES] = jnp.sum(tile, axis=0, keepdims=True)
    pl.semaphore_wait(barrier, 3)
    row_copy = pltpu.make_async_remote_copy(send_row, recv_row, vec_send.at[0], vec_recv.at[0],
                                            device_id=col_peer, device_id_type=MESH)
    col_copy = pltpu.make_async_remote_copy(send_col, recv_col, vec_send.at[1], vec_recv.at[1],
                                            device_id=row_peer, device_id_type=MESH)
    row_copy.start()
    col_copy.start()
    row_copy.wait()
    col_copy.wait()
    beta_two = hyper[0]
    row_now = beta_two * row_old[...] + (1.0 - beta_two) * ((send_row[...] + recv_row[...]) / n_total)
    col_now = beta_two * col_old[...] + (1.0 - beta_two) * ((send_col[...] + recv_col[...]) / m_total)
    new_row[...] = row_now
    new_col[...] = col_now
    row_inv = 1.0 / jnp.sqrt(row_now)
    col_inv = 1.0 / jnp.sqrt(col_now)
    col_scale[...] = col_inv
    for k in range(rows // LANES):
        tile = jnp.broadcast_to(row_inv[:, k * LANES:(k + 1) * LANES], (LANES, LANES))
        row_col[k * LANES:(k + 1) * LANES, :] = tile.T

    def second(i, col_acc):
        band = pl.ds(pl.multiple_of(i * step, step), step)
        scale = row_col[band, :]
        sums = []
        for k in range(cols // LANES):
            upd = grad[band, k * LANES:(k + 1) * LANES] * scale
            sums.append((upd * upd).reshape(step // 8, 8, LANES).sum(axis=0))
        return tuple(a + s for a, s in zip(col_acc, sums))

    col_acc = lax.fori_loop(0, rows // step, second,
                            tuple(jnp.zeros((8, LANES), jnp.float32) for _ in range(cols // LANES)))
    lane_sum = jnp.zeros((8, LANES), jnp.float32)
    col_sq = col_inv * col_inv
    for k, acc in enumerate(col_acc):
        lane_sum = lane_sum + acc * col_sq[:, k * LANES:(k + 1) * LANES]
    upd_sq = jnp.sum(lane_sum)
    row_part = jnp.sum(row_now)
    which = lax.broadcasted_iota(jnp.int32, (8, LANES), 0)
    send_val[...] = jnp.where(which == 0, upd_sq, jnp.where(which == 1, row_part, w_sq[0, 0]))
    copies = [pltpu.make_async_remote_copy(send_val, recv_val.at[k], val_send.at[k], val_recv.at[k],
                                           device_id=other, device_id_type=MESH)
              for k, other in enumerate(others)]
    for copy in copies:
        copy.start()
    for copy in copies:
        copy.wait()
    pair = send_val[...] + recv_val[0]
    total = pair + (recv_val[1] + recv_val[2])
    size = m_total * n_total
    row_total = pair[1:2, :1]
    upd_rms = jnp.sqrt(row_total * total[0:1, :1] / size)
    w_rms = jnp.sqrt(total[2:3, :1] / size)
    clip = jnp.maximum(1.0, upd_rms / hyper[2])
    factor = hyper[1] * jnp.maximum(EPS_TWO, w_rms) * jnp.sqrt(row_total) / clip
    row_scale[...] = row_inv * factor


def statistics(tokens, parts, recvs, w_sq, row_old, col_old, hyper, index):
    rows = parts[0].shape[0]
    widths = tuple(p.shape[1] for p in parts)
    cols = sum(widths)
    n_piece = len(parts)
    vmem = pl.BlockSpec(memory_space=pltpu.VMEM)
    smem = pl.BlockSpec(memory_space=pltpu.SMEM)
    anyw = pl.BlockSpec(memory_space=pl.ANY)
    f32 = jnp.float32
    return pl.pallas_call(
        functools.partial(stats_kernel, len(tokens), widths, 16, 2 * rows, 2 * cols),
        out_shape=[jax.ShapeDtypeStruct(s, f32) for s in ((rows, cols), (1, rows), (1, cols), (1, rows), (1, cols))],
        in_specs=[anyw] * len(tokens) + [smem] * 2 + [vmem] * (2 + 2 * n_piece),
        out_specs=[vmem] * 5,
        scratch_shapes=[
            pltpu.VMEM((rows, LANES), f32), pltpu.VMEM((rows, LANES), f32),
            pltpu.VMEM((1, rows), f32), pltpu.VMEM((1, cols), f32),
            pltpu.VMEM((1, rows), f32), pltpu.VMEM((1, cols), f32),
            pltpu.VMEM((8, LANES), f32), pltpu.VMEM((3, 8, LANES), f32),
            pltpu.SemaphoreType.DMA((2,)), pltpu.SemaphoreType.DMA((2,)),
            pltpu.SemaphoreType.DMA((3,)), pltpu.SemaphoreType.DMA((3,)),
        ],
        compiler_params=pltpu.CompilerParams(collective_id=index, has_side_effects=True,
                                             vmem_limit_bytes=32 * 1024 * 1024),
        cost_estimate=pl.CostEstimate(flops=8 * rows * cols * 100, bytes_accessed=12 * rows * cols, transcendentals=0),
    )(*tokens, hyper, w_sq.reshape(1, 1), row_old.reshape(1, rows), col_old.reshape(1, cols), *parts, *recvs)


def solution(mesh):
    act_spec = P('dp', 'row')
    grad_spec = P('dp', 'col')
    w_spec = P('row', 'col')
    row_spec = P('row')
    col_spec = P('col')
    in_specs = (act_spec, grad_spec, act_spec, grad_spec, grad_spec, act_spec, grad_spec,
                w_spec, w_spec, w_spec, w_spec,
                row_spec, col_spec, row_spec, col_spec, row_spec, col_spec, row_spec, col_spec, P())
    out_specs = (w_spec, row_spec, col_spec) * 4

    def product(x_block, dy_block):
        return jnp.einsum('tm,tn->mn', x_block, dy_block, preferred_element_type=jnp.float32)

    def per_device(x_attn, dy_attn, x_mlp, dy_gate, dy_up, h_mlp, dy_out, w_attn, w_gate, w_up, w_down,
                   r_attn, c_attn, r_gate, c_gate, r_up, c_up, r_down, c_down, hyper_params):
        order = []
        parts = {name: [] for name in NAMES}
        recvs = {name: [] for name in NAMES}
        start = 0
        for width in GATE_WIDTHS:
            order.append(('gate', x_mlp, dy_gate[:, start:start + width]))
            start += width
        order += [('up', x_mlp, dy_up), ('down', h_mlp, dy_out), ('attn', x_attn, dy_attn)]
        before = None
        for name, x_block, dy_block in order:
            if before is not None:
                x_block, before = lax.optimization_barrier((x_block, before))
            before = product(x_block, dy_block)
            recvs[name].append(lax.ppermute(before, 'dp', SWAP))
            parts[name].append(before)
        results = {}
        tokens = [parts['up'][0], parts['down'][0], parts['attn'][0]]
        weights = {'gate': w_gate, 'up': w_up, 'down': w_down, 'attn': w_attn}
        stats = {'gate': (r_gate, c_gate), 'up': (r_up, c_up), 'down': (r_down, c_down), 'attn': (r_attn, c_attn)}
        for index, name in enumerate(NAMES):
            weight = weights[name]
            rows, cols = weight.shape
            grad, row_scale, col_scale, new_row, new_col = statistics(
                tokens, parts[name], recvs[name], jnp.sum(weight * weight), *stats[name], hyper_params, index)
            new_weight = weight - (grad * row_scale.reshape(rows, 1)) * col_scale
            results[name] = (new_weight, new_row.reshape(rows), new_col.reshape(cols))
            tokens = [new_weight]
        return results['attn'] + results['gate'] + results['up'] + results['down']

    return jax.shard_map(per_device, mesh=mesh, in_specs=in_specs, out_specs=out_specs, check_vma=False)
```

```python
import functools
import jax
import jax.numpy as jnp
from jax import lax
from jax.experimental import pallas as pl
from jax.experimental.pallas import tpu as pltpu
from jax.sharding import PartitionSpec as P

EPS_ONE = 1e-30
EPS_TWO = 1e-3
SWAP = [(0, 1), (1, 0)]
MESH = pl.DeviceIdType.MESH
LANES = 128
NAMES = ('gate', 'up', 'down', 'attn')
GATE_BOXES = ((0, 0, 256, 256), (256, 0, 256, 256), (0, 256, 512, 256), (0, 512, 512, 512), (0, 1024, 512, 1024))
N_HEAD = 3


def peers():
    row_other = 1 - lax.axis_index('row')
    col_other = 1 - lax.axis_index('col')
    return ({'row': row_other}, {'col': col_other}, {'row': row_other, 'col': col_other})


def stats_kernel(n_token, boxes, step, m_total, n_total, *refs):
    n_piece = len(boxes)
    refs = refs[n_token:]
    hyper, w_sq, row_old, col_old = refs[:4]
    parts = refs[4:4 + n_piece]
    recvs = refs[4 + n_piece:4 + 2 * n_piece]
    (grad, row_scale, col_scale, new_row, new_col,
     row_acc, row_col, send_row, send_col, recv_row, recv_col, send_val, recv_val,
     vec_send, vec_recv, val_send, val_recv) = refs[4 + 2 * n_piece:4 + 2 * n_piece + 17]
    staged = refs[4 + 2 * n_piece + 17:]
    rows, cols = grad.shape
    others = peers()
    row_peer, col_peer, _ = others

    barrier = pltpu.get_barrier_semaphore()
    for other in others:
        pl.semaphore_signal(barrier, inc=1, device_id=other, device_id_type=MESH)

    part, recv = parts[0], recvs[0]
    if staged:
        part, recv, load = staged
        loads = []
        for k, (top, left) in enumerate(boxes):
            box = (pl.ds(top, parts[k].shape[0]), pl.ds(left, parts[k].shape[1]))
            loads.append(pltpu.make_async_copy(parts[k], part.at[box], load.at[2 * k]))
            loads.append(pltpu.make_async_copy(recvs[k], recv.at[box], load.at[2 * k + 1]))
        for copy in loads:
            copy.start()
        for copy in loads:
            copy.wait()

    def first(i, col_acc):
        band = pl.ds(pl.multiple_of(i * step, step), step)
        piece = part[band, :] + recv[band, :]
        grad[band, :] = piece
        sq = piece * piece + EPS_ONE
        lane_sum = sq[:, :LANES]
        for j in range(1, cols // LANES):
            lane_sum = lane_sum + sq[:, j * LANES:(j + 1) * LANES]
        row_acc[band, :] = lane_sum
        return col_acc + sq.reshape(step // 8, 8, cols).sum(axis=0)

    col_acc = lax.fori_loop(0, rows // step, first, jnp.zeros((8, cols), jnp.float32))
    send_col[...] = jnp.sum(col_acc, axis=0, keepdims=True)
    for k in range(rows // LANES):
        tile = row_acc[k * LANES:(k + 1) * LANES, :].T
        send_row[:, k * LANES:(k + 1) * LANES] = jnp.sum(tile, axis=0, keepdims=True)
    pl.semaphore_wait(barrier, 3)
    row_copy = pltpu.make_async_remote_copy(send_row, recv_row, vec_send.at[0], vec_recv.at[0],
                                            device_id=col_peer, device_id_type=MESH)
    col_copy = pltpu.make_async_remote_copy(send_col, recv_col, vec_send.at[1], vec_recv.at[1],
                                            device_id=row_peer, device_id_type=MESH)
    row_copy.start()
    col_copy.start()
    row_copy.wait()
    col_copy.wait()
    beta_two = hyper[0]
    row_now = beta_two * row_old[...] + (1.0 - beta_two) * ((send_row[...] + recv_row[...]) / n_total)
    col_now = beta_two * col_old[...] + (1.0 - beta_two) * ((send_col[...] + recv_col[...]) / m_total)
    new_row[...] = row_now
    new_col[...] = col_now
    row_inv = 1.0 / jnp.sqrt(row_now)
    col_inv = 1.0 / jnp.sqrt(col_now)
    col_scale[...] = col_inv
    for k in range(rows // LANES):
        tile = jnp.broadcast_to(row_inv[:, k * LANES:(k + 1) * LANES], (LANES, LANES))
        row_col[k * LANES:(k + 1) * LANES, :] = tile.T

    def second(i, col_acc):
        band = pl.ds(pl.multiple_of(i * step, step), step)
        scale = row_col[band, :]
        sums = []
        for k in range(cols // LANES):
            upd = grad[band, k * LANES:(k + 1) * LANES] * scale
            sums.append((upd * upd).reshape(step // 8, 8, LANES).sum(axis=0))
        return tuple(a + s for a, s in zip(col_acc, sums))

    col_acc = lax.fori_loop(0, rows // step, second,
                            tuple(jnp.zeros((8, LANES), jnp.float32) for _ in range(cols // LANES)))
    lane_sum = jnp.zeros((8, LANES), jnp.float32)
    col_sq = col_inv * col_inv
    for k, acc in enumerate(col_acc):
        lane_sum = lane_sum + acc * col_sq[:, k * LANES:(k + 1) * LANES]
    upd_sq = jnp.sum(lane_sum)
    row_part = jnp.sum(row_now)
    which = lax.broadcasted_iota(jnp.int32, (8, LANES), 0)
    send_val[...] = jnp.where(which == 0, upd_sq, jnp.where(which == 1, row_part, w_sq[0, 0]))
    copies = [pltpu.make_async_remote_copy(send_val, recv_val.at[k], val_send.at[k], val_recv.at[k],
                                           device_id=other, device_id_type=MESH)
              for k, other in enumerate(others)]
    for copy in copies:
        copy.start()
    for copy in copies:
        copy.wait()
    pair = send_val[...] + recv_val[0]
    total = pair + (recv_val[1] + recv_val[2])
    size = m_total * n_total
    row_total = pair[1:2, :1]
    upd_rms = jnp.sqrt(row_total * total[0:1, :1] / size)
    w_rms = jnp.sqrt(total[2:3, :1] / size)
    clip = jnp.maximum(1.0, upd_rms / hyper[2])
    factor = hyper[1] * jnp.maximum(EPS_TWO, w_rms) * jnp.sqrt(row_total) / clip
    row_scale[...] = row_inv * factor


def head_kernel(row_start, col_start, x_ref, dy_ref, out, x_buf, dy_buf, x_sem, dy_sem):
    n_step = x_sem.shape[0]
    depth = x_buf.shape[0] // n_step
    rows, cols = out.shape
    copies = []
    for k in range(n_step):
        band = pl.ds(k * depth, depth)
        copies.append((
            pltpu.make_async_copy(x_ref.at[band, pl.ds(row_start, rows)], x_buf.at[band, :], x_sem.at[k]),
            pltpu.make_async_copy(dy_ref.at[band, pl.ds(col_start, cols)], dy_buf.at[band, :], dy_sem.at[k])))
        copies[-1][0].start()
        copies[-1][1].start()
    for k in range(n_step):
        band = pl.ds(k * depth, depth)
        copies[k][0].wait()
        copies[k][1].wait()
        term = lax.dot_general(x_buf[band, :], dy_buf[band, :], (((0,), (0,)), ((), ())),
                               preferred_element_type=jnp.float32)
        if k == 0:
            out[...] = term
        else:
            out[...] += term


def head_product(x_block, dy_block, row_start, rows, col_start, cols):
    tokens = x_block.shape[0]
    anyw = pl.BlockSpec(memory_space=pl.ANY)
    return pl.pallas_call(
        functools.partial(head_kernel, row_start, col_start),
        out_shape=jax.ShapeDtypeStruct((rows, cols), jnp.float32),
        in_specs=[anyw, anyw],
        out_specs=pl.BlockSpec(memory_space=pltpu.VMEM),
        scratch_shapes=[pltpu.VMEM((tokens, rows), x_block.dtype), pltpu.VMEM((tokens, cols), dy_block.dtype),
                        pltpu.SemaphoreType.DMA((8,)), pltpu.SemaphoreType.DMA((8,))],
        compiler_params=pltpu.CompilerParams(vmem_limit_bytes=58 * 1024 * 1024),
        cost_estimate=pl.CostEstimate(flops=2 * tokens * rows * cols, bytes_accessed=2 * tokens * (rows + cols),
                                      transcendentals=0),
        name="head_product",
    )(x_block, dy_block)


def emit_kernel(*refs):
    half = len(refs) // 2
    for src, dst in zip(refs[:half], refs[half:]):
        dst[...] = src[...]


def emit(values):
    vmem = pl.BlockSpec(memory_space=pltpu.VMEM)
    return pl.pallas_call(
        emit_kernel,
        out_shape=[jax.ShapeDtypeStruct(v.shape, v.dtype) for v in values],
        in_specs=[vmem] * len(values), out_specs=[vmem] * len(values),
        cost_estimate=pl.CostEstimate(flops=100000, bytes_accessed=8 * sum(v.size for v in values), transcendentals=0),
        compiler_params=pltpu.CompilerParams(vmem_limit_bytes=1024 * 1024),
        name="emit",
    )(*values)


def finish_kernel(weight, grad, row_scale, col_scale, row_in, col_in, new_weight, new_row, new_col):
    rows = weight.shape[0]
    new_row[...] = row_in[...]
    new_col[...] = col_in[...]
    for k in range(rows // LANES):
        band = pl.ds(k * LANES, LANES)
        scale = jnp.broadcast_to(row_scale[:, k * LANES:(k + 1) * LANES], (LANES, LANES)).T
        for j in range(weight.shape[1] // LANES):
            lanes = pl.ds(j * LANES, LANES)
            new_weight[band, lanes] = weight[band, lanes] - grad[band, lanes] * scale * col_scale[:, lanes]


def finish(weight, grad, row_scale, col_scale, new_row, new_col):
    vmem = pl.BlockSpec(memory_space=pltpu.VMEM)
    return pl.pallas_call(
        finish_kernel,
        out_shape=[jax.ShapeDtypeStruct(v.shape, v.dtype) for v in (weight, new_row, new_col)],
        in_specs=[vmem] * 6, out_specs=[vmem] * 3,
        cost_estimate=pl.CostEstimate(flops=100000, bytes_accessed=12 * weight.size, transcendentals=0),
        compiler_params=pltpu.CompilerParams(vmem_limit_bytes=6 * 1024 * 1024),
        name="finish",
    )(weight, grad, row_scale, col_scale, new_row, new_col)


def statistics(tokens, boxes, parts, recvs, w_sq, row_old, col_old, hyper, index):
    rows, cols = row_old.shape[0], col_old.shape[0]
    n_piece = len(parts)
    vmem = pl.BlockSpec(memory_space=pltpu.VMEM)
    smem = pl.BlockSpec(memory_space=pltpu.SMEM)
    anyw = pl.BlockSpec(memory_space=pl.ANY)
    f32 = jnp.float32
    staged = rows * cols > 500000
    place = pl.BlockSpec(memory_space=pltpu.HBM) if staged else vmem
    stage = [pltpu.VMEM((rows, cols), f32)] * 2 + [pltpu.SemaphoreType.DMA((2 * n_piece,))] if staged else []
    space = pltpu.HBM if staged else pltpu.VMEM
    parts, recvs = ([pltpu.with_memory_space_constraint(v, space) for v in group] for group in (parts, recvs))
    return pl.pallas_call(
        functools.partial(stats_kernel, len(tokens), boxes, 16, 2 * rows, 2 * cols),
        out_shape=[jax.ShapeDtypeStruct(s, f32) for s in ((rows, cols), (1, rows), (1, cols), (1, rows), (1, cols))],
        in_specs=[anyw] * len(tokens) + [smem] * 2 + [vmem] * 2 + [place] * (2 * n_piece),
        out_specs=[vmem] * 5,
        scratch_shapes=[
            pltpu.VMEM((rows, LANES), f32), pltpu.VMEM((rows, LANES), f32),
            pltpu.VMEM((1, rows), f32), pltpu.VMEM((1, cols), f32),
            pltpu.VMEM((1, rows), f32), pltpu.VMEM((1, cols), f32),
            pltpu.VMEM((8, LANES), f32), pltpu.VMEM((3, 8, LANES), f32),
            pltpu.SemaphoreType.DMA((2,)), pltpu.SemaphoreType.DMA((2,)),
            pltpu.SemaphoreType.DMA((3,)), pltpu.SemaphoreType.DMA((3,)),
        ] + stage,
        compiler_params=pltpu.CompilerParams(collective_id=index, has_side_effects=True,
                                             vmem_limit_bytes=16 * 1024 * 1024 if staged else 6 * 1024 * 1024),
        cost_estimate=pl.CostEstimate(flops=8 * rows * cols * 100, bytes_accessed=12 * rows * cols, transcendentals=0),
    )(*tokens, hyper, w_sq.reshape(1, 1), row_old.reshape(1, rows), col_old.reshape(1, cols), *parts, *recvs)


def solution(mesh):
    act_spec = P('dp', 'row')
    grad_spec = P('dp', 'col')
    w_spec = P('row', 'col')
    row_spec = P('row')
    col_spec = P('col')
    in_specs = (act_spec, grad_spec, act_spec, grad_spec, grad_spec, act_spec, grad_spec,
                w_spec, w_spec, w_spec, w_spec,
                row_spec, col_spec, row_spec, col_spec, row_spec, col_spec, row_spec, col_spec, P())
    out_specs = (w_spec, row_spec, col_spec) * 4

    def product(x_block, dy_block):
        return jnp.einsum('tm,tn->mn', x_block, dy_block, preferred_element_type=jnp.float32)

    def per_device(x_attn, dy_attn, x_mlp, dy_gate, dy_up, h_mlp, dy_out, w_attn, w_gate, w_up, w_down,
                   r_attn, c_attn, r_gate, c_gate, r_up, c_up, r_down, c_down, hyper_params):
        order = [('gate', x_mlp, dy_gate, box) for box in GATE_BOXES]
        order += [('up', x_mlp, dy_up, None), ('down', h_mlp, dy_out, None), ('attn', x_attn, dy_attn, None)]
        parts = {name: [] for name in NAMES}
        recvs = {name: [] for name in NAMES}
        before = None
        for number, (name, x_block, dy_block, box) in enumerate(order):
            if before is not None:
                x_block, before = lax.optimization_barrier((x_block, before))
            if number < N_HEAD:
                before = head_product(x_block, dy_block, box[0], box[2], box[1], box[3])
            elif box is not None:
                before = product(x_block, dy_block[:, box[1]:box[1] + box[3]])
            else:
                before = product(x_block, dy_block)
            recvs[name].append(lax.ppermute(before, 'dp', SWAP))
            parts[name].append(before)
        results = {}
        tokens = [parts['up'][0], parts['down'][0], parts['attn'][0]]
        weights = {'gate': w_gate, 'up': w_up, 'down': w_down, 'attn': w_attn}
        stats = {'gate': (r_gate, c_gate), 'up': (r_up, c_up), 'down': (r_down, c_down), 'attn': (r_attn, c_attn)}
        for index, name in enumerate(NAMES):
            weight = weights[name]
            rows, cols = weight.shape
            grad, row_scale, col_scale, new_row, new_col = statistics(
                tokens, tuple(b[:2] for b in GATE_BOXES) if name == 'gate' else ((0, 0),), parts[name], recvs[name], jnp.sum(weight * weight), *stats[name], hyper_params, index)
            if index < 3:
                new_weight = weight - (grad * row_scale.reshape(rows, 1)) * col_scale
                new_row, new_col = emit((new_row, new_col))
            else:
                new_weight, new_row, new_col = finish(weight, grad, row_scale, col_scale, new_row, new_col)
            results[name] = (new_weight, new_row.reshape(rows), new_col.reshape(cols))
            tokens = [new_weight, new_row, new_col]
        return results['attn'] + results['gate'] + results['up'] + results['down']

    return jax.shard_map(per_device, mesh=mesh, in_specs=in_specs, out_specs=out_specs, check_vma=False)
```

```python
import functools
import jax
import jax.numpy as jnp
from jax import lax
from jax.experimental import pallas as pl
from jax.experimental.pallas import tpu as pltpu
from jax.sharding import PartitionSpec as P

EPS_ONE = 1e-30
EPS_TWO = 1e-3
SWAP = [(0, 1), (1, 0)]
MESH = pl.DeviceIdType.MESH
LANES = 128
NAMES = ('gate', 'up', 'down', 'attn')
GATE_BOXES = ((0, 0, 256, 256), (256, 0, 256, 512), (0, 256, 256, 256), (0, 512, 512, 512), (0, 1024, 512, 1024))
N_HEAD = 3
HEAD_LIMIT = 58 * 1024 * 1024


def peers():
    row_other = 1 - lax.axis_index('row')
    col_other = 1 - lax.axis_index('col')
    return ({'row': row_other}, {'col': col_other}, {'row': row_other, 'col': col_other})


def stats_kernel(n_token, boxes, near, direct, step, m_total, n_total, *refs):
    n_piece = len(boxes)
    refs = refs[n_token:]
    hyper, w_sq, row_old, col_old = refs[:4]
    parts = refs[4:4 + n_piece]
    recvs = refs[4 + n_piece:4 + 2 * n_piece]
    (grad, row_scale, new_row, new_col,
     row_acc, send_row, send_col, recv_row, recv_col, send_val, recv_val,
     vec_send, vec_recv, val_send, val_recv) = refs[4 + 2 * n_piece:4 + 2 * n_piece + 15]
    staged = refs[4 + 2 * n_piece + 15:]
    rows, cols = grad.shape
    others = peers()
    row_peer, col_peer, _ = others

    barrier = pltpu.get_barrier_semaphore()
    for other in others:
        pl.semaphore_signal(barrier, inc=1, device_id=other, device_id_type=MESH)

    part, recv = parts[0], recvs[0]
    if staged:
        part, recv, load = staged
        loads = []
        for k, (top, left) in enumerate(boxes):
            box = (pl.ds(top, parts[k].shape[0]), pl.ds(left, parts[k].shape[1]))
            loads.append(pltpu.make_async_copy(recvs[k], recv.at[box], load.at[2 * k + 1]))
            if k >= near:
                loads.append(pltpu.make_async_copy(parts[k], part.at[box], load.at[2 * k]))
        for copy in loads:
            copy.start()
        for k, (top, left) in enumerate(boxes[:near]):
            width = parts[k].shape[1]

            def place(i, carry):
                src = pl.ds(pl.multiple_of(i * step, step), step)
                dst = pl.ds(pl.multiple_of(top + i * step, step), step)
                part[dst, left:left + width] = parts[k][src, :]
                return carry

            lax.fori_loop(0, parts[k].shape[0] // step, place, 0)
        for copy in loads:
            copy.wait()

    def first(i, col_acc):
        band = pl.ds(pl.multiple_of(i * step, step), step)
        piece = part[band, :] + recv[band, :]
        grad[band, :] = piece
        sq = piece * piece + EPS_ONE
        lane_sum = sq[:, :LANES]
        for j in range(1, cols // LANES):
            lane_sum = lane_sum + sq[:, j * LANES:(j + 1) * LANES]
        row_acc[band, :] = lane_sum
        return col_acc + sq.reshape(step // 8, 8, cols).sum(axis=0)

    col_acc = lax.fori_loop(0, rows // step, first, jnp.zeros((8, cols), jnp.float32))
    send_col[...] = jnp.sum(col_acc, axis=0, keepdims=True)
    for k in range(rows // LANES):
        tile = row_acc[k * LANES:(k + 1) * LANES, :].T
        send_row[:, k * LANES:(k + 1) * LANES] = jnp.sum(tile, axis=0, keepdims=True)
    pl.semaphore_wait(barrier, 3)
    row_copy = pltpu.make_async_remote_copy(send_row, recv_row, vec_send.at[0], vec_recv.at[0],
                                            device_id=col_peer, device_id_type=MESH)
    col_copy = pltpu.make_async_remote_copy(send_col, recv_col, vec_send.at[1], vec_recv.at[1],
                                            device_id=row_peer, device_id_type=MESH)
    row_copy.start()
    col_copy.start()
    beta_two = hyper[0]

    col_copy.wait()
    col_now = beta_two * col_old[...] + (1.0 - beta_two) * ((send_col[...] + recv_col[...]) / m_total)
    new_col[...] = col_now
    col_inv = 1.0 / jnp.sqrt(col_now)

    def second(i, carry):
        band = pl.ds(pl.multiple_of(i * step, step), step)
        upd = grad[band, :] * col_inv
        grad[band, :] = upd
        sq = upd * upd
        lane_sum = sq[:, :LANES]
        for j in range(1, cols // LANES):
            lane_sum = lane_sum + sq[:, j * LANES:(j + 1) * LANES]
        row_acc[band, :] = lane_sum
        return carry

    lax.fori_loop(0, rows // step, second, 0)
    sums = [jnp.sum(row_acc[k * LANES:(k + 1) * LANES, :].T, axis=0, keepdims=True) for k in range(rows // LANES)]

    row_copy.wait()
    row_now = beta_two * row_old[...] + (1.0 - beta_two) * ((send_row[...] + recv_row[...]) / n_total)
    new_row[...] = row_now
    row_inv = 1.0 / jnp.sqrt(row_now)
    upd_sq = jnp.zeros((1, LANES), jnp.float32)
    row_part = jnp.zeros((1, LANES), jnp.float32)
    for k in range(rows // LANES):
        inv = row_inv[:, k * LANES:(k + 1) * LANES]
        upd_sq = upd_sq + sums[k] * (inv * inv)
        row_part = row_part + row_now[:, k * LANES:(k + 1) * LANES]
    which = lax.broadcasted_iota(jnp.int32, (8, LANES), 0)
    lane = lax.broadcasted_iota(jnp.int32, (8, LANES), 1)
    send_val[...] = jnp.where(which == 0, upd_sq, jnp.where(which == 1, row_part,
                                                            jnp.where(lane == 0, w_sq[0, 0], 0.0)))
    copies = [pltpu.make_async_remote_copy(send_val, recv_val.at[k], val_send.at[k], val_recv.at[k],
                                           device_id=other, device_id_type=MESH)
              for k, other in enumerate(others)]
    for copy in copies:
        copy.start()
    if direct:
        for k in range(rows // LANES):
            band = pl.ds(k * LANES, LANES)
            scale = jnp.broadcast_to(row_inv[:, k * LANES:(k + 1) * LANES], (LANES, LANES)).T
            for j in range(cols // LANES):
                lanes = pl.ds(j * LANES, LANES)
                grad[band, lanes] = grad[band, lanes] * scale
    for copy in copies:
        copy.wait()
    pair = send_val[...] + recv_val[0]
    total = jnp.sum(pair + (recv_val[1] + recv_val[2]), axis=1, keepdims=True)
    pair = jnp.sum(pair, axis=1, keepdims=True)
    size = m_total * n_total
    row_total = pair[1:2, :]
    upd_rms = jnp.sqrt(row_total * total[0:1, :] / size)
    w_rms = jnp.sqrt(total[2:3, :] / size)
    clip = jnp.maximum(1.0, upd_rms / hyper[2])
    factor = hyper[1] * jnp.maximum(EPS_TWO, w_rms) * jnp.sqrt(row_total) / clip
    if direct:
        row_scale[...] = jnp.broadcast_to(factor, (1, LANES))
    else:
        row_scale[...] = row_inv * factor


def head_kernel(row_start, col_start, x_ref, dy_ref, out, x_buf, dy_buf, x_sem, dy_sem):
    n_step = x_sem.shape[0]
    depth = x_buf.shape[0] // n_step
    rows, cols = out.shape
    copies = []
    for k in range(n_step):
        band = pl.ds(k * depth, depth)
        copies.append((
            pltpu.make_async_copy(x_ref.at[band, pl.ds(row_start, rows)], x_buf.at[band, :], x_sem.at[k]),
            pltpu.make_async_copy(dy_ref.at[band, pl.ds(col_start, cols)], dy_buf.at[band, :], dy_sem.at[k])))
        copies[-1][0].start()
        copies[-1][1].start()
    for k in range(n_step):
        band = pl.ds(k * depth, depth)
        copies[k][0].wait()
        copies[k][1].wait()
        term = lax.dot_general(x_buf[band, :], dy_buf[band, :], (((0,), (0,)), ((), ())),
                               preferred_element_type=jnp.float32)
        if k == 0:
            out[...] = term
        else:
            out[...] += term


def head_product(x_block, dy_block, row_start, rows, col_start, cols):
    tokens = x_block.shape[0]
    anyw = pl.BlockSpec(memory_space=pl.ANY)
    return pl.pallas_call(
        functools.partial(head_kernel, row_start, col_start),
        out_shape=jax.ShapeDtypeStruct((rows, cols), jnp.float32),
        in_specs=[anyw, anyw],
        out_specs=pl.BlockSpec(memory_space=pltpu.VMEM),
        scratch_shapes=[pltpu.VMEM((tokens, rows), x_block.dtype), pltpu.VMEM((tokens, cols), dy_block.dtype),
                        pltpu.SemaphoreType.DMA((8,)), pltpu.SemaphoreType.DMA((8,))],
        compiler_params=pltpu.CompilerParams(vmem_limit_bytes=HEAD_LIMIT if (row_start, col_start) != (0, 0) else 14 * 1024 * 1024),
        cost_estimate=pl.CostEstimate(flops=2 * tokens * rows * cols, bytes_accessed=2 * tokens * (rows + cols),
                                      transcendentals=0),
        name="head_product",
    )(pltpu.with_memory_space_constraint(x_block, pltpu.HBM), pltpu.with_memory_space_constraint(dy_block, pltpu.HBM))


def emit_kernel(*refs):
    half = len(refs) // 2
    for src, dst in zip(refs[:half], refs[half:]):
        dst[...] = src[...]


def emit(values):
    vmem = pl.BlockSpec(memory_space=pltpu.VMEM)
    return pl.pallas_call(
        emit_kernel,
        out_shape=[jax.ShapeDtypeStruct(v.shape, v.dtype) for v in values],
        in_specs=[vmem] * len(values), out_specs=[vmem] * len(values),
        cost_estimate=pl.CostEstimate(flops=100000, bytes_accessed=8 * sum(v.size for v in values), transcendentals=0),
        compiler_params=pltpu.CompilerParams(vmem_limit_bytes=1024 * 1024),
        name="emit",
    )(*values)


def finish_kernel(weight, update, factor, row_in, col_in, new_weight, new_row, new_col):
    new_row[...] = row_in[...]
    new_col[...] = col_in[...]
    scale = factor[...]
    for j in range(weight.shape[1] // LANES):
        lanes = pl.ds(j * LANES, LANES)
        new_weight[:, lanes] = weight[:, lanes] - update[:, lanes] * scale


def finish(weight, update, factor, new_row, new_col):
    vmem = pl.BlockSpec(memory_space=pltpu.VMEM)
    return pl.pallas_call(
        finish_kernel,
        out_shape=[jax.ShapeDtypeStruct(v.shape, v.dtype) for v in (weight, new_row, new_col)],
        in_specs=[vmem] * 5, out_specs=[vmem] * 3,
        cost_estimate=pl.CostEstimate(flops=100000, bytes_accessed=12 * weight.size, transcendentals=0),
        compiler_params=pltpu.CompilerParams(vmem_limit_bytes=6 * 1024 * 1024),
        name="finish",
    )(weight, update, factor, new_row, new_col)


def statistics(tokens, boxes, near, parts, recvs, w_sq, row_old, col_old, hyper, index):
    rows, cols = row_old.shape[0], col_old.shape[0]
    n_piece = len(parts)
    vmem = pl.BlockSpec(memory_space=pltpu.VMEM)
    smem = pl.BlockSpec(memory_space=pltpu.SMEM)
    anyw = pl.BlockSpec(memory_space=pl.ANY)
    f32 = jnp.float32
    staged = rows * cols > 500000
    near = near if staged else 1
    spaces = [pltpu.VMEM if k < near else pltpu.HBM for k in range(n_piece)]
    spaces += [pltpu.HBM if staged else pltpu.VMEM] * n_piece
    places = [pl.BlockSpec(memory_space=v) for v in spaces]
    stage = [pltpu.VMEM((rows, cols), f32)] * 2 + [pltpu.SemaphoreType.DMA((2 * n_piece,))] if staged else []
    halves = [pltpu.with_memory_space_constraint(v, space) for v, space in zip(parts + recvs, spaces)]
    shapes = ((rows, cols), (1, rows if staged else LANES), (1, rows), (1, cols))
    return pl.pallas_call(
        functools.partial(stats_kernel, len(tokens), boxes, near, not staged, 16, 2 * rows, 2 * cols),
        out_shape=[jax.ShapeDtypeStruct(s, f32) for s in shapes],
        in_specs=[anyw] * len(tokens) + [smem] * 2 + [vmem] * 2 + places,
        out_specs=[vmem] * 4,
        scratch_shapes=[
            pltpu.VMEM((rows, LANES), f32),
            pltpu.VMEM((1, rows), f32), pltpu.VMEM((1, cols), f32),
            pltpu.VMEM((1, rows), f32), pltpu.VMEM((1, cols), f32),
            pltpu.VMEM((8, LANES), f32), pltpu.VMEM((3, 8, LANES), f32),
            pltpu.SemaphoreType.DMA((2,)), pltpu.SemaphoreType.DMA((2,)),
            pltpu.SemaphoreType.DMA((3,)), pltpu.SemaphoreType.DMA((3,)),
        ] + stage,
        compiler_params=pltpu.CompilerParams(collective_id=index, has_side_effects=True,
                                             vmem_limit_bytes=16 * 1024 * 1024 if staged else 6 * 1024 * 1024),
        cost_estimate=pl.CostEstimate(flops=8 * rows * cols * 100, bytes_accessed=12 * rows * cols, transcendentals=0),
    )(*tokens, hyper, w_sq.reshape(1, 1), row_old.reshape(1, rows), col_old.reshape(1, cols), *halves)


def solution(mesh):
    act_spec = P('dp', 'row')
    grad_spec = P('dp', 'col')
    w_spec = P('row', 'col')
    row_spec = P('row')
    col_spec = P('col')
    in_specs = (act_spec, grad_spec, act_spec, grad_spec, grad_spec, act_spec, grad_spec,
                w_spec, w_spec, w_spec, w_spec,
                row_spec, col_spec, row_spec, col_spec, row_spec, col_spec, row_spec, col_spec, P())
    out_specs = (w_spec, row_spec, col_spec) * 4

    def product(x_block, dy_block):
        return jnp.einsum('tm,tn->mn', x_block, dy_block, preferred_element_type=jnp.float32)

    def per_device(x_attn, dy_attn, x_mlp, dy_gate, dy_up, h_mlp, dy_out, w_attn, w_gate, w_up, w_down,
                   r_attn, c_attn, r_gate, c_gate, r_up, c_up, r_down, c_down, hyper_params):
        order = [('gate', x_mlp, dy_gate, box) for box in GATE_BOXES]
        order += [('up', x_mlp, dy_up, None), ('down', h_mlp, dy_out, None), ('attn', x_attn, dy_attn, None)]
        parts = {name: [] for name in NAMES}
        recvs = {name: [] for name in NAMES}
        before = None
        for number, (name, x_block, dy_block, box) in enumerate(order):
            if before is not None:
                x_block, before = lax.optimization_barrier((x_block, before))
            if number < N_HEAD:
                before = head_product(x_block, dy_block, box[0], box[2], box[1], box[3])
            elif box is not None:
                before = product(x_block, dy_block[:, box[1]:box[1] + box[3]])
            else:
                before = product(x_block, dy_block)
            recvs[name].append(lax.ppermute(before, 'dp', SWAP))
            parts[name].append(before)
        results = {}
        tokens = [parts['up'][0], parts['down'][0], parts['attn'][0]]
        weights = {'gate': w_gate, 'up': w_up, 'down': w_down, 'attn': w_attn}
        stats = {'gate': (r_gate, c_gate), 'up': (r_up, c_up), 'down': (r_down, c_down), 'attn': (r_attn, c_attn)}
        for index, name in enumerate(NAMES):
            weight = weights[name]
            rows, cols = weight.shape
            grad, row_scale, new_row, new_col = statistics(
                tokens, tuple(b[:2] for b in GATE_BOXES) if name == 'gate' else ((0, 0),),
                N_HEAD if name == 'gate' else 0, parts[name], recvs[name],
                jnp.sum(weight * weight), *stats[name], hyper_params, index)
            if index < 3:
                new_weight = weight - grad * row_scale.reshape(rows, 1)
                new_row, new_col = emit((new_row, new_col))
            else:
                new_weight, new_row, new_col = finish(weight, grad, row_scale, new_row, new_col)
            results[name] = (new_weight, new_row.reshape(rows), new_col.reshape(cols))
            tokens = [new_weight, new_row, new_col]
        return results['attn'] + results['gate'] + results['up'] + results['down']

    return jax.shard_map(per_device, mesh=mesh, in_specs=in_specs, out_specs=out_specs, check_vma=False)
```

```python
import functools
import jax
import jax.numpy as jnp
from jax import lax
from jax.experimental import pallas as pl
from jax.experimental.pallas import tpu as pltpu
from jax.sharding import PartitionSpec as P

EPS_ONE = 1e-30
EPS_TWO = 1e-3
SWAP = [(0, 1), (1, 0)]
MESH = pl.DeviceIdType.MESH
LANES = 128
NAMES = ('gate', 'up', 'down', 'attn')
GATE_BOXES = ((0, 0, 256, 384), (256, 0, 256, 384), (0, 384, 512, 256), (0, 640, 512, 384), (0, 1024, 512, 1024))
N_HEAD = 3
HEAD_LIMIT = 58 * 1024 * 1024


def peers():
    row_other = 1 - lax.axis_index('row')
    col_other = 1 - lax.axis_index('col')
    return ({'row': row_other}, {'col': col_other}, {'row': row_other, 'col': col_other})


def stats_kernel(n_token, boxes, near, direct, step, m_total, n_total, *refs):
    n_piece = len(boxes)
    refs = refs[n_token:]
    w_sq, hyper, row_old, col_old = refs[:4]
    parts = refs[4:4 + n_piece]
    recvs = refs[4 + n_piece:4 + 2 * n_piece]
    (grad, row_scale, new_row, new_col,
     row_acc, send_row, send_col, recv_row, recv_col, send_val, recv_val,
     vec_send, vec_recv, val_send, val_recv) = refs[4 + 2 * n_piece:4 + 2 * n_piece + 15]
    staged = refs[4 + 2 * n_piece + 15:]
    rows, cols = grad.shape
    others = peers()
    row_peer, col_peer, _ = others

    barrier = pltpu.get_barrier_semaphore()
    for other in others:
        pl.semaphore_signal(barrier, inc=1, device_id=other, device_id_type=MESH)

    part, recv = parts[0], recvs[0]
    if staged:
        part, recv, load = staged
        loads = []
        for k, (top, left) in enumerate(boxes):
            box = (pl.ds(top, parts[k].shape[0]), pl.ds(left, parts[k].shape[1]))
            loads.append(pltpu.make_async_copy(recvs[k], recv.at[box], load.at[2 * k + 1]))
            if k >= near:
                loads.append(pltpu.make_async_copy(parts[k], part.at[box], load.at[2 * k]))
        for copy in loads:
            copy.start()
        for k, (top, left) in enumerate(boxes[:near]):
            width = parts[k].shape[1]

            def place(i, carry):
                src = pl.ds(pl.multiple_of(i * step, step), step)
                dst = pl.ds(pl.multiple_of(top + i * step, step), step)
                part[dst, left:left + width] = parts[k][src, :]
                return carry

            lax.fori_loop(0, parts[k].shape[0] // step, place, 0)
        for copy in loads:
            copy.wait()

    def first(i, col_acc):
        band = pl.ds(pl.multiple_of(i * step, step), step)
        piece = part[band, :] + recv[band, :]
        grad[band, :] = piece
        sq = piece * piece + EPS_ONE
        lane_sum = sq[:, :LANES]
        for j in range(1, cols // LANES):
            lane_sum = lane_sum + sq[:, j * LANES:(j + 1) * LANES]
        row_acc[band, :] = lane_sum
        return col_acc + sq.reshape(step // 8, 8, cols).sum(axis=0)

    col_acc = lax.fori_loop(0, rows // step, first, jnp.zeros((8, cols), jnp.float32))
    send_col[...] = jnp.sum(col_acc, axis=0, keepdims=True)
    for k in range(rows // LANES):
        tile = row_acc[k * LANES:(k + 1) * LANES, :].T
        send_row[:, k * LANES:(k + 1) * LANES] = jnp.sum(tile, axis=0, keepdims=True)
    pl.semaphore_wait(barrier, 3)
    row_copy = pltpu.make_async_remote_copy(send_row, recv_row, vec_send.at[0], vec_recv.at[0],
                                            device_id=col_peer, device_id_type=MESH)
    col_copy = pltpu.make_async_remote_copy(send_col, recv_col, vec_send.at[1], vec_recv.at[1],
                                            device_id=row_peer, device_id_type=MESH)
    row_copy.start()
    col_copy.start()
    beta_two = hyper[0:1, 0:1]

    col_copy.wait()
    col_now = beta_two * col_old[...] + (1.0 - beta_two) * ((send_col[...] + recv_col[...]) / m_total)
    new_col[...] = col_now
    col_inv = 1.0 / jnp.sqrt(col_now)

    def second(i, carry):
        band = pl.ds(pl.multiple_of(i * step, step), step)
        upd = grad[band, :] * col_inv
        grad[band, :] = upd
        sq = upd * upd
        lane_sum = sq[:, :LANES]
        for j in range(1, cols // LANES):
            lane_sum = lane_sum + sq[:, j * LANES:(j + 1) * LANES]
        row_acc[band, :] = lane_sum
        return carry

    lax.fori_loop(0, rows // step, second, 0)
    sums = [jnp.sum(row_acc[k * LANES:(k + 1) * LANES, :].T, axis=0, keepdims=True) for k in range(rows // LANES)]

    row_copy.wait()
    row_now = beta_two * row_old[...] + (1.0 - beta_two) * ((send_row[...] + recv_row[...]) / n_total)
    new_row[...] = row_now
    row_inv = 1.0 / jnp.sqrt(row_now)
    upd_sq = jnp.zeros((1, LANES), jnp.float32)
    row_part = jnp.zeros((1, LANES), jnp.float32)
    for k in range(rows // LANES):
        inv = row_inv[:, k * LANES:(k + 1) * LANES]
        upd_sq = upd_sq + sums[k] * (inv * inv)
        row_part = row_part + row_now[:, k * LANES:(k + 1) * LANES]
    which = lax.broadcasted_iota(jnp.int32, (8, LANES), 0)
    lane = lax.broadcasted_iota(jnp.int32, (8, LANES), 1)
    send_val[...] = jnp.where(which == 0, upd_sq, jnp.where(which == 1, row_part,
                                                            jnp.where(lane == 0, w_sq[0, 0], 0.0)))
    copies = [pltpu.make_async_remote_copy(send_val, recv_val.at[k], val_send.at[k], val_recv.at[k],
                                           device_id=other, device_id_type=MESH)
              for k, other in enumerate(others)]
    for copy in copies:
        copy.start()
    if direct:
        for k in range(rows // LANES):
            band = pl.ds(k * LANES, LANES)
            scale = jnp.broadcast_to(row_inv[:, k * LANES:(k + 1) * LANES], (LANES, LANES)).T
            for j in range(cols // LANES):
                lanes = pl.ds(j * LANES, LANES)
                grad[band, lanes] = grad[band, lanes] * scale
    for copy in copies:
        copy.wait()
    pair = send_val[...] + recv_val[0]
    total = jnp.sum(pair + (recv_val[1] + recv_val[2]), axis=1, keepdims=True)
    pair = jnp.sum(pair, axis=1, keepdims=True)
    size = m_total * n_total
    row_total = pair[1:2, :]
    upd_rms = jnp.sqrt(row_total * total[0:1, :] / size)
    w_rms = jnp.sqrt(total[2:3, :] / size)
    clip = jnp.maximum(1.0, upd_rms / hyper[2:3, 0:1])
    factor = hyper[1:2, 0:1] * jnp.maximum(EPS_TWO, w_rms) * jnp.sqrt(row_total) / clip
    if direct:
        row_scale[...] = jnp.broadcast_to(factor, (1, LANES))
    else:
        row_scale[...] = row_inv * factor


def head_kernel(row_start, col_start, x_ref, dy_ref, out, x_buf, dy_buf, x_sem, dy_sem):
    n_step = x_sem.shape[0]
    depth = x_buf.shape[0] // n_step
    rows, cols = out.shape

    def copies(k):
        band = pl.ds(pl.multiple_of(k * depth, depth), depth)
        return (pltpu.make_async_copy(x_ref.at[band, pl.ds(row_start, rows)], x_buf.at[band, :], x_sem.at[k]),
                pltpu.make_async_copy(dy_ref.at[band, pl.ds(col_start, cols)], dy_buf.at[band, :], dy_sem.at[k]))

    def begin(k, carry):
        for copy in copies(k):
            copy.start()
        return carry

    def multiply(k):
        for copy in copies(k):
            copy.wait()
        band = pl.ds(pl.multiple_of(k * depth, depth), depth)
        return lax.dot_general(x_buf[band, :], dy_buf[band, :], (((0,), (0,)), ((), ())),
                               preferred_element_type=jnp.float32)

    def follow(k, carry):
        out[...] += multiply(k)
        return carry

    lax.fori_loop(0, n_step, begin, 0, unroll=True)
    out[...] = jnp.zeros_like(out)
    lax.fori_loop(0, n_step, follow, 0)


def head_product(x_block, dy_block, row_start, rows, col_start, cols):
    tokens = x_block.shape[0]
    anyw = pl.BlockSpec(memory_space=pl.ANY)
    return pl.pallas_call(
        functools.partial(head_kernel, row_start, col_start),
        out_shape=jax.ShapeDtypeStruct((rows, cols), jnp.float32),
        in_specs=[anyw, anyw],
        out_specs=pl.BlockSpec(memory_space=pltpu.VMEM),
        scratch_shapes=[pltpu.VMEM((tokens, rows), x_block.dtype), pltpu.VMEM((tokens, cols), dy_block.dtype),
                        pltpu.SemaphoreType.DMA((8,)), pltpu.SemaphoreType.DMA((8,))],
        compiler_params=pltpu.CompilerParams(vmem_limit_bytes=HEAD_LIMIT if col_start else 14 * 1024 * 1024),
        cost_estimate=pl.CostEstimate(flops=2 * tokens * rows * cols, bytes_accessed=2 * tokens * (rows + cols),
                                      transcendentals=0),
        name="head_product",
    )(pltpu.with_memory_space_constraint(x_block, pltpu.HBM), pltpu.with_memory_space_constraint(dy_block, pltpu.HBM))


def emit_kernel(*refs):
    half = len(refs) // 2
    for src, dst in zip(refs[:half], refs[half:]):
        dst[...] = src[...]


def emit(values):
    vmem = pl.BlockSpec(memory_space=pltpu.VMEM)
    return pl.pallas_call(
        emit_kernel,
        out_shape=[jax.ShapeDtypeStruct(v.shape, v.dtype) for v in values],
        in_specs=[vmem] * len(values), out_specs=[vmem] * len(values),
        cost_estimate=pl.CostEstimate(flops=100000, bytes_accessed=8 * sum(v.size for v in values), transcendentals=0),
        compiler_params=pltpu.CompilerParams(vmem_limit_bytes=1024 * 1024),
        name="emit",
    )(*values)


def finish_kernel(weight, update, factor, row_in, col_in, new_weight, new_row, new_col):
    new_row[...] = row_in[...]
    new_col[...] = col_in[...]
    scale = factor[...]
    for j in range(weight.shape[1] // LANES):
        lanes = pl.ds(j * LANES, LANES)
        new_weight[:, lanes] = weight[:, lanes] - update[:, lanes] * scale


def finish(weight, update, factor, new_row, new_col):
    vmem = pl.BlockSpec(memory_space=pltpu.VMEM)
    return pl.pallas_call(
        finish_kernel,
        out_shape=[jax.ShapeDtypeStruct(v.shape, v.dtype) for v in (weight, new_row, new_col)],
        in_specs=[vmem] * 5, out_specs=[vmem] * 3,
        cost_estimate=pl.CostEstimate(flops=100000, bytes_accessed=12 * weight.size, transcendentals=0),
        compiler_params=pltpu.CompilerParams(vmem_limit_bytes=6 * 1024 * 1024),
        name="finish",
    )(weight, update, factor, new_row, new_col)


def statistics(tokens, boxes, near, parts, recvs, w_sq, row_old, col_old, hyper, index):
    rows, cols = row_old.shape[0], col_old.shape[0]
    n_piece = len(parts)
    vmem = pl.BlockSpec(memory_space=pltpu.VMEM)
    smem = pl.BlockSpec(memory_space=pltpu.SMEM)
    anyw = pl.BlockSpec(memory_space=pl.ANY)
    f32 = jnp.float32
    staged = rows * cols > 500000
    near = near if staged else 1
    spaces = [pltpu.VMEM if k < near else pltpu.HBM for k in range(n_piece)]
    spaces += [pltpu.HBM if staged else pltpu.VMEM] * n_piece
    places = [pl.BlockSpec(memory_space=v) for v in spaces]
    stage = [pltpu.VMEM((rows, cols), f32)] * 2 + [pltpu.SemaphoreType.DMA((2 * n_piece,))] if staged else []
    halves = [pltpu.with_memory_space_constraint(v, space) for v, space in zip(parts + recvs, spaces)]
    shapes = ((rows, cols), (1, rows if staged else LANES), (1, rows), (1, cols))
    return pl.pallas_call(
        functools.partial(stats_kernel, len(tokens), boxes, near, not staged, 16, 2 * rows, 2 * cols),
        out_shape=[jax.ShapeDtypeStruct(s, f32) for s in shapes],
        in_specs=[anyw] * len(tokens) + [smem] + [vmem] * 3 + places,
        out_specs=[vmem] * 4,
        scratch_shapes=[
            pltpu.VMEM((rows, LANES), f32),
            pltpu.VMEM((1, rows), f32), pltpu.VMEM((1, cols), f32),
            pltpu.VMEM((1, rows), f32), pltpu.VMEM((1, cols), f32),
            pltpu.VMEM((8, LANES), f32), pltpu.VMEM((3, 8, LANES), f32),
            pltpu.SemaphoreType.DMA((2,)), pltpu.SemaphoreType.DMA((2,)),
            pltpu.SemaphoreType.DMA((3,)), pltpu.SemaphoreType.DMA((3,)),
        ] + stage,
        compiler_params=pltpu.CompilerParams(collective_id=index, has_side_effects=True,
                                             vmem_limit_bytes=16 * 1024 * 1024 if staged else 6 * 1024 * 1024),
        cost_estimate=pl.CostEstimate(flops=8 * rows * cols * 100, bytes_accessed=12 * rows * cols, transcendentals=0),
    )(*tokens, w_sq.reshape(1, 1), hyper, row_old.reshape(1, rows), col_old.reshape(1, cols), *halves)


def solution(mesh):
    act_spec = P('dp', 'row')
    grad_spec = P('dp', 'col')
    w_spec = P('row', 'col')
    row_spec = P('row')
    col_spec = P('col')
    in_specs = (act_spec, grad_spec, act_spec, grad_spec, grad_spec, act_spec, grad_spec,
                w_spec, w_spec, w_spec, w_spec,
                row_spec, col_spec, row_spec, col_spec, row_spec, col_spec, row_spec, col_spec, P())
    out_specs = (w_spec, row_spec, col_spec) * 4

    def product(x_block, dy_block):
        return jnp.einsum('tm,tn->mn', x_block, dy_block, preferred_element_type=jnp.float32)

    def per_device(x_attn, dy_attn, x_mlp, dy_gate, dy_up, h_mlp, dy_out, w_attn, w_gate, w_up, w_down,
                   r_attn, c_attn, r_gate, c_gate, r_up, c_up, r_down, c_down, hyper_params):
        order = [('gate', x_mlp, dy_gate, box) for box in GATE_BOXES]
        order += [('up', x_mlp, dy_up, None), ('down', h_mlp, dy_out, None), ('attn', x_attn, dy_attn, None)]
        parts = {name: [] for name in NAMES}
        recvs = {name: [] for name in NAMES}
        before = None
        for number, (name, x_block, dy_block, box) in enumerate(order):
            if before is not None:
                x_block, before = lax.optimization_barrier((x_block, before))
            if number < N_HEAD:
                before = head_product(x_block, dy_block, box[0], box[2], box[1], box[3])
            elif box is not None:
                before = product(x_block, dy_block[:, box[1]:box[1] + box[3]])
            else:
                before = product(x_block, dy_block)
            recvs[name].append(lax.ppermute(before, 'dp', SWAP))
            parts[name].append(before)
        results = {}
        hyper_rows = jnp.broadcast_to(jnp.pad(hyper_params, (0, 5))[:, None], (8, LANES))
        tokens = [parts['up'][0], parts['down'][0], parts['attn'][0]]
        weights = {'gate': w_gate, 'up': w_up, 'down': w_down, 'attn': w_attn}
        stats = {'gate': (r_gate, c_gate), 'up': (r_up, c_up), 'down': (r_down, c_down), 'attn': (r_attn, c_attn)}
        for index, name in enumerate(NAMES):
            weight = weights[name]
            rows, cols = weight.shape
            grad, row_scale, new_row, new_col = statistics(
                tokens, tuple(b[:2] for b in GATE_BOXES) if name == 'gate' else ((0, 0),),
                N_HEAD if name == 'gate' else 0, parts[name], recvs[name],
                jnp.sum(weight * weight), *stats[name], hyper_rows, index)
            if index < 3:
                new_weight = weight - grad * row_scale.reshape(rows, 1)
                new_row, new_col = emit((new_row, new_col))
            else:
                new_weight, new_row, new_col = finish(weight, grad, row_scale, new_row, new_col)
            results[name] = (new_weight, new_row.reshape(rows), new_col.reshape(cols))
            tokens = [new_weight, new_row, new_col]
        return results['attn'] + results['gate'] + results['up'] + results['down']

    return jax.shard_map(per_device, mesh=mesh, in_specs=in_specs, out_specs=out_specs, check_vma=False)
```

```python
import functools
import jax
import jax.numpy as jnp
from jax import lax
from jax.experimental import pallas as pl
from jax.experimental.pallas import tpu as pltpu
from jax.sharding import PartitionSpec as P

EPS_ONE = 1e-30
EPS_TWO = 1e-3
SWAP = [(0, 1), (1, 0)]
MESH = pl.DeviceIdType.MESH
LANES = 128
NAMES = ('gate', 'up', 'down', 'attn')
GATE_BOXES = ((0, 0, 256, 384), (256, 0, 256, 384), (0, 384, 512, 256), (0, 640, 512, 384), (0, 1024, 512, 1024))
N_HEAD = 3
HEAD_LIMIT = 58 * 1024 * 1024


def peers():
    row_other = 1 - lax.axis_index('row')
    col_other = 1 - lax.axis_index('col')
    return ({'row': row_other}, {'col': col_other})


def stats_kernel(n_token, boxes, near, direct, step, m_total, n_total, *refs):
    n_piece = len(boxes)
    refs = refs[n_token:]
    w_sq, hyper, row_old, col_old = refs[:4]
    parts = refs[4:4 + n_piece]
    recvs = refs[4 + n_piece:4 + 2 * n_piece]
    (grad, row_scale, new_row, new_col,
     row_acc, send_row, send_col, recv_row, recv_col, send_upd, recv_upd, send_val, recv_val,
     swap_send, swap_recv) = refs[4 + 2 * n_piece:4 + 2 * n_piece + 15]
    staged = refs[4 + 2 * n_piece + 15:]
    rows, cols = grad.shape
    others = peers()
    row_peer, col_peer = others

    def swap(k, src, dst, other):
        return pltpu.make_async_remote_copy(src, dst, swap_send.at[k], swap_recv.at[k],
                                            device_id=other, device_id_type=MESH)

    barrier = pltpu.get_barrier_semaphore()
    for other in others:
        pl.semaphore_signal(barrier, inc=1, device_id=other, device_id_type=MESH)

    part, recv = parts[0], recvs[0]
    if staged:
        part, recv, load = staged
        loads = []
        for k, (top, left) in enumerate(boxes):
            box = (pl.ds(top, parts[k].shape[0]), pl.ds(left, parts[k].shape[1]))
            loads.append(pltpu.make_async_copy(recvs[k], recv.at[box], load.at[2 * k + 1]))
            if k >= near:
                loads.append(pltpu.make_async_copy(parts[k], part.at[box], load.at[2 * k]))
        for copy in loads:
            copy.start()
        for k, (top, left) in enumerate(boxes[:near]):
            width = parts[k].shape[1]

            def place(i, carry):
                src = pl.ds(pl.multiple_of(i * step, step), step)
                dst = pl.ds(pl.multiple_of(top + i * step, step), step)
                part[dst, left:left + width] = parts[k][src, :]
                return carry

            lax.fori_loop(0, parts[k].shape[0] // step, place, 0)
        for copy in loads:
            copy.wait()

    def first(i, col_acc):
        band = pl.ds(pl.multiple_of(i * step, step), step)
        piece = part[band, :] + recv[band, :]
        grad[band, :] = piece
        sq = piece * piece + EPS_ONE
        lane_sum = sq[:, :LANES]
        for j in range(1, cols // LANES):
            lane_sum = lane_sum + sq[:, j * LANES:(j + 1) * LANES]
        row_acc[band, :] = lane_sum
        return col_acc + sq.reshape(step // 8, 8, cols).sum(axis=0)

    col_acc = lax.fori_loop(0, rows // step, first, jnp.zeros((8, cols), jnp.float32))
    send_col[...] = jnp.sum(col_acc, axis=0, keepdims=True)
    for k in range(rows // LANES):
        tile = row_acc[k * LANES:(k + 1) * LANES, :].T
        send_row[:, k * LANES:(k + 1) * LANES] = jnp.sum(tile, axis=0, keepdims=True)
    pl.semaphore_wait(barrier, 2)
    row_copy = swap(0, send_row, recv_row, col_peer)
    col_copy = swap(1, send_col, recv_col, row_peer)
    row_copy.start()
    col_copy.start()
    beta_two = hyper[0:1, 0:1]

    col_copy.wait()
    col_now = beta_two * col_old[...] + (1.0 - beta_two) * ((send_col[...] + recv_col[...]) / m_total)
    new_col[...] = col_now
    col_inv = 1.0 / jnp.sqrt(col_now)

    def second(i, carry):
        band = pl.ds(pl.multiple_of(i * step, step), step)
        upd = grad[band, :] * col_inv
        grad[band, :] = upd
        sq = upd * upd
        lane_sum = sq[:, :LANES]
        for j in range(1, cols // LANES):
            lane_sum = lane_sum + sq[:, j * LANES:(j + 1) * LANES]
        row_acc[band, :] = lane_sum
        return carry

    lax.fori_loop(0, rows // step, second, 0)
    for k in range(rows // LANES):
        tile = row_acc[k * LANES:(k + 1) * LANES, :].T
        send_upd[:, k * LANES:(k + 1) * LANES] = jnp.sum(tile, axis=0, keepdims=True)
    lane = lax.broadcasted_iota(jnp.int32, (1, LANES), 1)
    send_upd[:, rows:] = jnp.where(lane == 0, w_sq[0, 0], 0.0)
    upd_copy = swap(2, send_upd, recv_upd, col_peer)
    upd_copy.start()

    row_copy.wait()
    row_now = beta_two * row_old[...] + (1.0 - beta_two) * ((send_row[...] + recv_row[...]) / n_total)
    new_row[...] = row_now
    row_inv = 1.0 / jnp.sqrt(row_now)
    row_part = jnp.zeros((1, LANES), jnp.float32)
    for k in range(rows // LANES):
        row_part = row_part + row_now[:, k * LANES:(k + 1) * LANES]
    if direct:
        for k in range(rows // LANES):
            band = pl.ds(k * LANES, LANES)
            scale = jnp.broadcast_to(row_inv[:, k * LANES:(k + 1) * LANES], (LANES, LANES)).T
            for j in range(cols // LANES):
                lanes = pl.ds(j * LANES, LANES)
                grad[band, lanes] = grad[band, lanes] * scale
    upd_copy.wait()
    upd_both = send_upd[...] + recv_upd[...]
    upd_sq = jnp.zeros((1, LANES), jnp.float32)
    for k in range(rows // LANES):
        inv = row_inv[:, k * LANES:(k + 1) * LANES]
        upd_sq = upd_sq + upd_both[:, k * LANES:(k + 1) * LANES] * (inv * inv)
    which = lax.broadcasted_iota(jnp.int32, (8, LANES), 0)
    send_val[...] = jnp.where(which == 0, upd_sq, jnp.where(which == 1, row_part, upd_both[:, rows:]))
    val_copy = swap(3, send_val, recv_val, row_peer)
    val_copy.start()
    val_copy.wait()
    total = jnp.sum(send_val[...] + recv_val[...], axis=1, keepdims=True)
    size = m_total * n_total
    row_total = total[1:2, :]
    upd_rms = jnp.sqrt(row_total * total[0:1, :] / size)
    w_rms = jnp.sqrt(total[2:3, :] / size)
    clip = jnp.maximum(1.0, upd_rms / hyper[2:3, 0:1])
    factor = hyper[1:2, 0:1] * jnp.maximum(EPS_TWO, w_rms) * jnp.sqrt(row_total) / clip
    if direct:
        row_scale[...] = jnp.broadcast_to(factor, (1, LANES))
    else:
        row_scale[...] = row_inv * factor


def head_kernel(row_start, col_start, x_ref, dy_ref, out, x_buf, dy_buf, x_sem, dy_sem):
    n_step = x_sem.shape[0]
    depth = x_buf.shape[0] // n_step
    rows, cols = out.shape

    def at(k):
        return k * depth if isinstance(k, int) else pl.multiple_of(k * depth, depth)

    def copies(k):
        band = pl.ds(at(k), depth)
        return (pltpu.make_async_copy(x_ref.at[band, pl.ds(row_start, rows)], x_buf.at[band, :], x_sem.at[k]),
                pltpu.make_async_copy(dy_ref.at[band, pl.ds(col_start, cols)], dy_buf.at[band, :], dy_sem.at[k]))

    def begin(k, carry):
        for copy in copies(k):
            copy.start()
        return carry

    def multiply(k):
        for copy in copies(k):
            copy.wait()
        band = pl.ds(at(k), depth)
        return lax.dot_general(x_buf[band, :], dy_buf[band, :], (((0,), (0,)), ((), ())),
                               preferred_element_type=jnp.float32)

    def follow(k, carry):
        out[...] += multiply(k)
        return carry

    lax.fori_loop(0, n_step, begin, 0, unroll=True)
    if rows < 512:
        out[...] = multiply(0)
        for k in range(1, n_step):
            out[...] += multiply(k)
    else:
        out[...] = jnp.zeros_like(out)
        lax.fori_loop(0, n_step, follow, 0)


def head_product(x_block, dy_block, row_start, rows, col_start, cols):
    tokens = x_block.shape[0]
    anyw = pl.BlockSpec(memory_space=pl.ANY)
    return pl.pallas_call(
        functools.partial(head_kernel, row_start, col_start),
        out_shape=jax.ShapeDtypeStruct((rows, cols), jnp.float32),
        in_specs=[anyw, anyw],
        out_specs=pl.BlockSpec(memory_space=pltpu.VMEM),
        scratch_shapes=[pltpu.VMEM((tokens, rows), x_block.dtype), pltpu.VMEM((tokens, cols), dy_block.dtype),
                        pltpu.SemaphoreType.DMA((8,)), pltpu.SemaphoreType.DMA((8,))],
        compiler_params=pltpu.CompilerParams(vmem_limit_bytes=HEAD_LIMIT if col_start else 14 * 1024 * 1024),
        cost_estimate=pl.CostEstimate(flops=2 * tokens * rows * cols, bytes_accessed=2 * tokens * (rows + cols),
                                      transcendentals=0),
        name="head_product",
    )(pltpu.with_memory_space_constraint(x_block, pltpu.HBM), pltpu.with_memory_space_constraint(dy_block, pltpu.HBM))


def emit_kernel(*refs):
    half = len(refs) // 2
    for src, dst in zip(refs[:half], refs[half:]):
        dst[...] = src[...]


def emit(values):
    vmem = pl.BlockSpec(memory_space=pltpu.VMEM)
    return pl.pallas_call(
        emit_kernel,
        out_shape=[jax.ShapeDtypeStruct(v.shape, v.dtype) for v in values],
        in_specs=[vmem] * len(values), out_specs=[vmem] * len(values),
        cost_estimate=pl.CostEstimate(flops=100000, bytes_accessed=8 * sum(v.size for v in values), transcendentals=0),
        compiler_params=pltpu.CompilerParams(vmem_limit_bytes=1024 * 1024),
        name="emit",
    )(*values)


def finish_kernel(weight, update, factor, row_in, col_in, new_weight, new_row, new_col):
    new_row[...] = row_in[...]
    new_col[...] = col_in[...]
    scale = factor[...]
    for j in range(weight.shape[1] // LANES):
        lanes = pl.ds(j * LANES, LANES)
        new_weight[:, lanes] = weight[:, lanes] - update[:, lanes] * scale


def finish(weight, update, factor, new_row, new_col):
    vmem = pl.BlockSpec(memory_space=pltpu.VMEM)
    return pl.pallas_call(
        finish_kernel,
        out_shape=[jax.ShapeDtypeStruct(v.shape, v.dtype) for v in (weight, new_row, new_col)],
        in_specs=[vmem] * 5, out_specs=[vmem] * 3,
        cost_estimate=pl.CostEstimate(flops=100000, bytes_accessed=12 * weight.size, transcendentals=0),
        compiler_params=pltpu.CompilerParams(vmem_limit_bytes=6 * 1024 * 1024),
        name="finish",
    )(weight, update, factor, new_row, new_col)


def statistics(tokens, boxes, near, parts, recvs, w_sq, row_old, col_old, hyper, index):
    rows, cols = row_old.shape[0], col_old.shape[0]
    n_piece = len(parts)
    vmem = pl.BlockSpec(memory_space=pltpu.VMEM)
    smem = pl.BlockSpec(memory_space=pltpu.SMEM)
    anyw = pl.BlockSpec(memory_space=pl.ANY)
    f32 = jnp.float32
    staged = rows * cols > 500000
    near = near if staged else 1
    spaces = [pltpu.VMEM if k < near else pltpu.HBM for k in range(n_piece)]
    spaces += [pltpu.HBM if staged else pltpu.VMEM] * n_piece
    places = [pl.BlockSpec(memory_space=v) for v in spaces]
    stage = [pltpu.VMEM((rows, cols), f32)] * 2 + [pltpu.SemaphoreType.DMA((2 * n_piece,))] if staged else []
    halves = [pltpu.with_memory_space_constraint(v, space) for v, space in zip(parts + recvs, spaces)]
    shapes = ((rows, cols), (1, rows if staged else LANES), (1, rows), (1, cols))
    return pl.pallas_call(
        functools.partial(stats_kernel, len(tokens), boxes, near, not staged, 16, 2 * rows, 2 * cols),
        out_shape=[jax.ShapeDtypeStruct(s, f32) for s in shapes],
        in_specs=[anyw] * len(tokens) + [smem] + [vmem] * 3 + places,
        out_specs=[vmem] * 4,
        scratch_shapes=[
            pltpu.VMEM((rows, LANES), f32),
            pltpu.VMEM((1, rows), f32), pltpu.VMEM((1, cols), f32),
            pltpu.VMEM((1, rows), f32), pltpu.VMEM((1, cols), f32),
            pltpu.VMEM((1, rows + LANES), f32), pltpu.VMEM((1, rows + LANES), f32),
            pltpu.VMEM((8, LANES), f32), pltpu.VMEM((8, LANES), f32),
            pltpu.SemaphoreType.DMA((4,)), pltpu.SemaphoreType.DMA((4,)),
        ] + stage,
        compiler_params=pltpu.CompilerParams(collective_id=index, has_side_effects=True,
                                             vmem_limit_bytes=16 * 1024 * 1024 if staged else 6 * 1024 * 1024),
        cost_estimate=pl.CostEstimate(flops=8 * rows * cols * 100, bytes_accessed=12 * rows * cols, transcendentals=0),
    )(*tokens, w_sq.reshape(1, 1), hyper, row_old.reshape(1, rows), col_old.reshape(1, cols), *halves)


def solution(mesh):
    act_spec = P('dp', 'row')
    grad_spec = P('dp', 'col')
    w_spec = P('row', 'col')
    row_spec = P('row')
    col_spec = P('col')
    in_specs = (act_spec, grad_spec, act_spec, grad_spec, grad_spec, act_spec, grad_spec,
                w_spec, w_spec, w_spec, w_spec,
                row_spec, col_spec, row_spec, col_spec, row_spec, col_spec, row_spec, col_spec, P())
    out_specs = (w_spec, row_spec, col_spec) * 4

    def product(x_block, dy_block):
        return jnp.einsum('tm,tn->mn', x_block, dy_block, preferred_element_type=jnp.float32)

    def per_device(x_attn, dy_attn, x_mlp, dy_gate, dy_up, h_mlp, dy_out, w_attn, w_gate, w_up, w_down,
                   r_attn, c_attn, r_gate, c_gate, r_up, c_up, r_down, c_down, hyper_params):
        order = [('gate', x_mlp, dy_gate, box) for box in GATE_BOXES]
        order += [('up', x_mlp, dy_up, None), ('down', h_mlp, dy_out, None), ('attn', x_attn, dy_attn, None)]
        parts = {name: [] for name in NAMES}
        recvs = {name: [] for name in NAMES}
        before = None
        for number, (name, x_block, dy_block, box) in enumerate(order):
            if before is not None:
                x_block, before = lax.optimization_barrier((x_block, before))
            if number < N_HEAD:
                before = head_product(x_block, dy_block, box[0], box[2], box[1], box[3])
            elif box is not None:
                before = product(x_block, dy_block[:, box[1]:box[1] + box[3]])
            else:
                before = product(x_block, dy_block)
            recvs[name].append(lax.ppermute(before, 'dp', SWAP))
            parts[name].append(before)
        results = {}
        hyper_rows = jnp.broadcast_to(jnp.pad(hyper_params, (0, 5))[:, None], (8, LANES))
        tokens = [parts['up'][0], parts['down'][0], parts['attn'][0]]
        weights = {'gate': w_gate, 'up': w_up, 'down': w_down, 'attn': w_attn}
        stats = {'gate': (r_gate, c_gate), 'up': (r_up, c_up), 'down': (r_down, c_down), 'attn': (r_attn, c_attn)}
        for index, name in enumerate(NAMES):
            weight = weights[name]
            rows, cols = weight.shape
            grad, row_scale, new_row, new_col = statistics(
                tokens, tuple(b[:2] for b in GATE_BOXES) if name == 'gate' else ((0, 0),),
                N_HEAD if name == 'gate' else 0, parts[name], recvs[name],
                jnp.sum(weight * weight), *stats[name], hyper_rows, index)
            if index < 3:
                new_weight = weight - grad * row_scale.reshape(rows, 1)
                new_row, new_col = emit((new_row, new_col))
            else:
                new_weight, new_row, new_col = finish(weight, grad, row_scale, new_row, new_col)
            results[name] = (new_weight, new_row.reshape(rows), new_col.reshape(cols))
            tokens = [new_weight, new_row, new_col]
        return results['attn'] + results['gate'] + results['up'] + results['down']

    return jax.shard_map(per_device, mesh=mesh, in_specs=in_specs, out_specs=out_specs, check_vma=False)
```

```python
import functools
import jax
import jax.numpy as jnp
from jax import lax
from jax.experimental import pallas as pl
from jax.experimental.pallas import tpu as pltpu
from jax.sharding import PartitionSpec as P

EPS_ONE = 1e-30
EPS_TWO = 1e-3
SWAP = [(0, 1), (1, 0)]
MESH = pl.DeviceIdType.MESH
LANES = 128
NAMES = ('gate', 'up', 'down', 'attn')
GATE_BOXES = ((0, 0, 256, 256), (256, 0, 256, 256), (0, 256, 256, 256), (256, 256, 256, 256),
              (0, 512, 512, 256), (0, 768, 512, 256), (0, 1024, 512, 384), (0, 1408, 512, 640))
N_HEAD = 6
N_NEAR = 4
WAVE = 4
HEAD_LIMIT = 58 * 1024 * 1024


def peers():
    row_other = 1 - lax.axis_index('row')
    col_other = 1 - lax.axis_index('col')
    return ({'row': row_other}, {'col': col_other})


def stats_kernel(n_token, boxes, near, direct, step, m_total, n_total, *refs):
    n_piece = len(boxes)
    refs = refs[n_token:]
    w_sq, hyper, row_old, col_old = refs[:4]
    parts = refs[4:4 + n_piece]
    recvs = refs[4 + n_piece:4 + 2 * n_piece]
    (grad, row_scale, new_row, new_col,
     row_acc, send_row, send_col, recv_row, recv_col, send_upd, recv_upd, send_val, recv_val,
     swap_send, swap_recv) = refs[4 + 2 * n_piece:4 + 2 * n_piece + 15]
    staged = refs[4 + 2 * n_piece + 15:]
    rows, cols = grad.shape
    others = peers()
    row_peer, col_peer = others

    def swap(k, src, dst, other):
        return pltpu.make_async_remote_copy(src, dst, swap_send.at[k], swap_recv.at[k],
                                            device_id=other, device_id_type=MESH)

    barrier = pltpu.get_barrier_semaphore()
    for other in others:
        pl.semaphore_signal(barrier, inc=1, device_id=other, device_id_type=MESH)

    part, recv = parts[0], recvs[0]
    if staged:
        part, recv, load = staged
        loads = []
        for k, (top, left) in enumerate(boxes):
            box = (pl.ds(top, parts[k].shape[0]), pl.ds(left, parts[k].shape[1]))
            loads.append(pltpu.make_async_copy(recvs[k], recv.at[box], load.at[2 * k + 1]))
            if k >= near:
                loads.append(pltpu.make_async_copy(parts[k], part.at[box], load.at[2 * k]))
        for copy in loads:
            copy.start()
        for k, (top, left) in enumerate(boxes[:near]):
            width = parts[k].shape[1]

            def place(i, carry):
                src = pl.ds(pl.multiple_of(i * step, step), step)
                dst = pl.ds(pl.multiple_of(top + i * step, step), step)
                part[dst, left:left + width] = parts[k][src, :]
                return carry

            lax.fori_loop(0, parts[k].shape[0] // step, place, 0)
        for copy in loads:
            copy.wait()

    def first(i, col_acc):
        band = pl.ds(pl.multiple_of(i * step, step), step)
        piece = part[band, :] + recv[band, :]
        grad[band, :] = piece
        sq = piece * piece + EPS_ONE
        lane_sum = sq[:, :LANES]
        for j in range(1, cols // LANES):
            lane_sum = lane_sum + sq[:, j * LANES:(j + 1) * LANES]
        row_acc[band, :] = lane_sum
        return col_acc + sq.reshape(step // 8, 8, cols).sum(axis=0)

    col_acc = lax.fori_loop(0, rows // step, first, jnp.zeros((8, cols), jnp.float32))
    send_col[...] = jnp.sum(col_acc, axis=0, keepdims=True)
    pl.semaphore_wait(barrier, 2)
    row_copy = swap(0, send_row, recv_row, col_peer)
    col_copy = swap(1, send_col, recv_col, row_peer)
    col_copy.start()
    for k in range(rows // LANES):
        tile = row_acc[k * LANES:(k + 1) * LANES, :].T
        send_row[:, k * LANES:(k + 1) * LANES] = jnp.sum(tile, axis=0, keepdims=True)
    row_copy.start()
    beta_two = hyper[0:1, 0:1]

    col_copy.wait()
    col_now = beta_two * col_old[...] + (1.0 - beta_two) * ((send_col[...] + recv_col[...]) / m_total)
    new_col[...] = col_now
    col_inv = 1.0 / jnp.sqrt(col_now)

    def second(i, carry):
        band = pl.ds(pl.multiple_of(i * step, step), step)
        upd = grad[band, :] * col_inv
        grad[band, :] = upd
        sq = upd * upd
        lane_sum = sq[:, :LANES]
        for j in range(1, cols // LANES):
            lane_sum = lane_sum + sq[:, j * LANES:(j + 1) * LANES]
        row_acc[band, :] = lane_sum
        return carry

    lax.fori_loop(0, rows // step, second, 0)
    for k in range(rows // LANES):
        tile = row_acc[k * LANES:(k + 1) * LANES, :].T
        send_upd[:, k * LANES:(k + 1) * LANES] = jnp.sum(tile, axis=0, keepdims=True)
    lane = lax.broadcasted_iota(jnp.int32, (1, LANES), 1)
    send_upd[:, rows:] = jnp.where(lane == 0, w_sq[0, 0], 0.0)
    upd_copy = swap(2, send_upd, recv_upd, col_peer)
    upd_copy.start()

    row_copy.wait()
    row_now = beta_two * row_old[...] + (1.0 - beta_two) * ((send_row[...] + recv_row[...]) / n_total)
    new_row[...] = row_now
    row_inv = 1.0 / jnp.sqrt(row_now)
    row_part = jnp.zeros((1, LANES), jnp.float32)
    for k in range(rows // LANES):
        row_part = row_part + row_now[:, k * LANES:(k + 1) * LANES]
    if direct:
        for k in range(rows // LANES):
            band = pl.ds(k * LANES, LANES)
            scale = jnp.broadcast_to(row_inv[:, k * LANES:(k + 1) * LANES], (LANES, LANES)).T
            for j in range(cols // LANES):
                lanes = pl.ds(j * LANES, LANES)
                grad[band, lanes] = grad[band, lanes] * scale
    upd_copy.wait()
    upd_both = send_upd[...] + recv_upd[...]
    upd_sq = jnp.zeros((1, LANES), jnp.float32)
    for k in range(rows // LANES):
        inv = row_inv[:, k * LANES:(k + 1) * LANES]
        upd_sq = upd_sq + upd_both[:, k * LANES:(k + 1) * LANES] * (inv * inv)
    which = lax.broadcasted_iota(jnp.int32, (8, LANES), 0)
    send_val[...] = jnp.where(which == 0, upd_sq, jnp.where(which == 1, row_part, upd_both[:, rows:]))
    val_copy = swap(3, send_val, recv_val, row_peer)
    val_copy.start()
    val_copy.wait()
    total = jnp.sum(send_val[...] + recv_val[...], axis=1, keepdims=True)
    size = m_total * n_total
    row_total = total[1:2, :]
    upd_rms = jnp.sqrt(row_total * total[0:1, :] / size)
    w_rms = jnp.sqrt(total[2:3, :] / size)
    clip = jnp.maximum(1.0, upd_rms / hyper[2:3, 0:1])
    factor = hyper[1:2, 0:1] * jnp.maximum(EPS_TWO, w_rms) * jnp.sqrt(row_total) / clip
    if direct:
        row_scale[...] = jnp.broadcast_to(factor, (1, LANES))
    else:
        row_scale[...] = row_inv * factor


def head_kernel(row_start, col_start, x_ref, dy_ref, out, x_buf, dy_buf, x_sem, dy_sem):
    n_step = x_sem.shape[0]
    depth = x_buf.shape[0] // n_step
    rows, cols = out.shape

    def at(k):
        return k * depth if isinstance(k, int) else pl.multiple_of(k * depth, depth)

    def copies(k):
        band = pl.ds(at(k), depth)
        return (pltpu.make_async_copy(x_ref.at[band, pl.ds(row_start, rows)], x_buf.at[band, :], x_sem.at[k]),
                pltpu.make_async_copy(dy_ref.at[band, pl.ds(col_start, cols)], dy_buf.at[band, :], dy_sem.at[k]))

    def begin(k):
        for copy in copies(k):
            copy.start()

    def multiply(k, add):
        for copy in copies(k):
            copy.wait()
        band = pl.ds(at(k), depth)
        term = lax.dot_general(x_buf[band, :], dy_buf[band, :], (((0,), (0,)), ((), ())),
                               preferred_element_type=jnp.float32)
        if add:
            out[...] += term
        else:
            out[...] = term

    if rows < 512:
        for k in range(WAVE):
            begin(k)
        for k in range(n_step):
            multiply(k, k > 0)
            if k + WAVE < n_step:
                begin(k + WAVE)
    else:
        for k in range(n_step):
            begin(k)
        out[...] = jnp.zeros_like(out)

        def follow(k, carry):
            multiply(k, True)
            return carry

        lax.fori_loop(0, n_step, follow, 0)


def head_product(x_block, dy_block, row_start, rows, col_start, cols):
    tokens = x_block.shape[0]
    anyw = pl.BlockSpec(memory_space=pl.ANY)
    return pl.pallas_call(
        functools.partial(head_kernel, row_start, col_start),
        out_shape=jax.ShapeDtypeStruct((rows, cols), jnp.float32),
        in_specs=[anyw, anyw],
        out_specs=pl.BlockSpec(memory_space=pltpu.VMEM),
        scratch_shapes=[pltpu.VMEM((tokens, rows), x_block.dtype), pltpu.VMEM((tokens, cols), dy_block.dtype),
                        pltpu.SemaphoreType.DMA((8,)), pltpu.SemaphoreType.DMA((8,))],
        compiler_params=pltpu.CompilerParams(vmem_limit_bytes=HEAD_LIMIT if rows == 512 else 14 * 1024 * 1024),
        cost_estimate=pl.CostEstimate(flops=2 * tokens * rows * cols, bytes_accessed=2 * tokens * (rows + cols),
                                      transcendentals=0),
        name="head_product",
    )(pltpu.with_memory_space_constraint(x_block, pltpu.HBM), pltpu.with_memory_space_constraint(dy_block, pltpu.HBM))


def emit_kernel(*refs):
    half = len(refs) // 2
    for src, dst in zip(refs[:half], refs[half:]):
        dst[...] = src[...]


def emit(values):
    vmem = pl.BlockSpec(memory_space=pltpu.VMEM)
    return pl.pallas_call(
        emit_kernel,
        out_shape=[jax.ShapeDtypeStruct(v.shape, v.dtype) for v in values],
        in_specs=[vmem] * len(values), out_specs=[vmem] * len(values),
        cost_estimate=pl.CostEstimate(flops=100000, bytes_accessed=8 * sum(v.size for v in values), transcendentals=0),
        compiler_params=pltpu.CompilerParams(vmem_limit_bytes=1024 * 1024),
        name="emit",
    )(*values)


def finish_kernel(weight, update, factor, row_in, col_in, new_weight, new_row, new_col, buf, sem):
    copies = [pltpu.make_async_copy(row_in, new_row, sem.at[0]), pltpu.make_async_copy(col_in, new_col, sem.at[1])]
    for copy in copies:
        copy.start()
    scale = factor[...]
    depth = weight.shape[0] // 4
    for k in range(4):
        band = pl.ds(k * depth, depth)
        for j in range(weight.shape[1] // LANES):
            lanes = pl.ds(j * LANES, LANES)
            buf[band, lanes] = weight[band, lanes] - update[band, lanes] * scale
        copies.append(pltpu.make_async_copy(buf.at[band, :], new_weight.at[band, :], sem.at[2 + k]))
        copies[-1].start()
    for copy in copies:
        copy.wait()


def finish(weight, update, factor, new_row, new_col):
    vmem = pl.BlockSpec(memory_space=pltpu.VMEM)
    anyw = pl.BlockSpec(memory_space=pl.ANY)
    return pl.pallas_call(
        finish_kernel,
        out_shape=[jax.ShapeDtypeStruct(v.shape, v.dtype) for v in (weight, new_row, new_col)],
        in_specs=[vmem] * 5, out_specs=[anyw] * 3,
        scratch_shapes=[pltpu.VMEM(weight.shape, weight.dtype), pltpu.SemaphoreType.DMA((6,))],
        cost_estimate=pl.CostEstimate(flops=100000, bytes_accessed=12 * weight.size, transcendentals=0),
        compiler_params=pltpu.CompilerParams(vmem_limit_bytes=6 * 1024 * 1024),
        name="finish",
    )(weight, update, factor, new_row, new_col)


def statistics(tokens, boxes, near, parts, recvs, w_sq, row_old, col_old, hyper, index):
    rows, cols = row_old.shape[0], col_old.shape[0]
    n_piece = len(parts)
    vmem = pl.BlockSpec(memory_space=pltpu.VMEM)
    smem = pl.BlockSpec(memory_space=pltpu.SMEM)
    anyw = pl.BlockSpec(memory_space=pl.ANY)
    f32 = jnp.float32
    staged = rows * cols > 500000
    near = near if staged else 1
    spaces = [pltpu.VMEM if k < near else pltpu.HBM for k in range(n_piece)]
    spaces += [pltpu.HBM if staged else pltpu.VMEM] * n_piece
    places = [pl.BlockSpec(memory_space=v) for v in spaces]
    stage = [pltpu.VMEM((rows, cols), f32)] * 2 + [pltpu.SemaphoreType.DMA((2 * n_piece,))] if staged else []
    halves = [pltpu.with_memory_space_constraint(v, space) for v, space in zip(parts + recvs, spaces)]
    shapes = ((rows, cols), (1, rows if staged else LANES), (1, rows), (1, cols))
    return pl.pallas_call(
        functools.partial(stats_kernel, len(tokens), boxes, near, not staged, 16, 2 * rows, 2 * cols),
        out_shape=[jax.ShapeDtypeStruct(s, f32) for s in shapes],
        in_specs=[anyw] * len(tokens) + [smem] + [vmem] * 3 + places,
        out_specs=[vmem] * 4,
        scratch_shapes=[
            pltpu.VMEM((rows, LANES), f32),
            pltpu.VMEM((1, rows), f32), pltpu.VMEM((1, cols), f32),
            pltpu.VMEM((1, rows), f32), pltpu.VMEM((1, cols), f32),
            pltpu.VMEM((1, rows + LANES), f32), pltpu.VMEM((1, rows + LANES), f32),
            pltpu.VMEM((8, LANES), f32), pltpu.VMEM((8, LANES), f32),
            pltpu.SemaphoreType.DMA((4,)), pltpu.SemaphoreType.DMA((4,)),
        ] + stage,
        compiler_params=pltpu.CompilerParams(collective_id=index, has_side_effects=True,
                                             vmem_limit_bytes=16 * 1024 * 1024 if staged else 6 * 1024 * 1024),
        cost_estimate=pl.CostEstimate(flops=8 * rows * cols * 100, bytes_accessed=12 * rows * cols, transcendentals=0),
    )(*tokens, w_sq.reshape(1, 1), hyper, row_old.reshape(1, rows), col_old.reshape(1, cols), *halves)


def solution(mesh):
    act_spec = P('dp', 'row')
    grad_spec = P('dp', 'col')
    w_spec = P('row', 'col')
    row_spec = P('row')
    col_spec = P('col')
    in_specs = (act_spec, grad_spec, act_spec, grad_spec, grad_spec, act_spec, grad_spec,
                w_spec, w_spec, w_spec, w_spec,
                row_spec, col_spec, row_spec, col_spec, row_spec, col_spec, row_spec, col_spec, P())
    out_specs = (w_spec, row_spec, col_spec) * 4

    def product(x_block, dy_block):
        return jnp.einsum('tm,tn->mn', x_block, dy_block, preferred_element_type=jnp.float32)

    def per_device(x_attn, dy_attn, x_mlp, dy_gate, dy_up, h_mlp, dy_out, w_attn, w_gate, w_up, w_down,
                   r_attn, c_attn, r_gate, c_gate, r_up, c_up, r_down, c_down, hyper_params):
        order = [('gate', x_mlp, dy_gate, box) for box in GATE_BOXES]
        order += [('up', x_mlp, dy_up, None), ('down', h_mlp, dy_out, None), ('attn', x_attn, dy_attn, None)]
        parts = {name: [] for name in NAMES}
        recvs = {name: [] for name in NAMES}
        before = None
        for number, (name, x_block, dy_block, box) in enumerate(order):
            if before is not None:
                x_block, before = lax.optimization_barrier((x_block, before))
            if number < N_HEAD:
                before = head_product(x_block, dy_block, box[0], box[2], box[1], box[3])
            elif box is not None:
                before = product(x_block, dy_block[:, box[1]:box[1] + box[3]])
            else:
                before = product(x_block, dy_block)
            recvs[name].append(lax.ppermute(before, 'dp', SWAP))
            parts[name].append(before)
        results = {}
        hyper_rows = jnp.broadcast_to(jnp.pad(hyper_params, (0, 5))[:, None], (8, LANES))
        tokens = [parts['up'][0], parts['down'][0], parts['attn'][0]]
        weights = {'gate': w_gate, 'up': w_up, 'down': w_down, 'attn': w_attn}
        stats = {'gate': (r_gate, c_gate), 'up': (r_up, c_up), 'down': (r_down, c_down), 'attn': (r_attn, c_attn)}
        for index, name in enumerate(NAMES):
            weight = weights[name]
            rows, cols = weight.shape
            grad, row_scale, new_row, new_col = statistics(
                tokens, tuple(b[:2] for b in GATE_BOXES) if name == 'gate' else ((0, 0),),
                N_NEAR if name == 'gate' else 0, parts[name], recvs[name],
                jnp.sum(weight * weight), *stats[name], hyper_rows, index)
            if index < 3:
                new_weight = weight - grad * row_scale.reshape(rows, 1)
                new_row, new_col = emit((new_row, new_col))
            else:
                new_weight, new_row, new_col = finish(weight, grad, row_scale, new_row, new_col)
            results[name] = (new_weight, new_row.reshape(rows), new_col.reshape(cols))
            tokens = [new_weight, new_row, new_col]
        return results['attn'] + results['gate'] + results['up'] + results['down']

    return jax.shard_map(per_device, mesh=mesh, in_specs=in_specs, out_specs=out_specs, check_vma=False)
```

```python
import functools
import jax
import jax.numpy as jnp
from jax import lax
from jax.experimental import pallas as pl
from jax.experimental.pallas import tpu as pltpu
from jax.sharding import PartitionSpec as P

EPS_ONE = 1e-30
EPS_TWO = 1e-3
SWAP = [(0, 1), (1, 0)]
MESH = pl.DeviceIdType.MESH
LANES = 128
NAMES = ('gate', 'up', 'down', 'attn')
GATE_BOXES = ((0, 0, 256, 256), (256, 0, 256, 256), (0, 256, 256, 256), (256, 256, 256, 256),
              (0, 512, 512, 256), (0, 768, 512, 256), (0, 1024, 512, 384), (0, 1408, 512, 640))
N_HEAD = 6
N_NEAR = 4
MIB = 1024 * 1024
HEAD_LIMIT = 50 * MIB


def peers():
    row_other = 1 - lax.axis_index('row')
    col_other = 1 - lax.axis_index('col')
    return ({'row': row_other}, {'col': col_other})


def stats_kernel(n_token, boxes, near, direct, step, m_total, n_total, *refs):
    n_piece = len(boxes)
    refs = refs[n_token:]
    w_sq, hyper, row_old, col_old = refs[:4]
    parts = refs[4:4 + n_piece]
    recvs = refs[4 + n_piece:4 + 2 * n_piece]
    (grad, row_scale, new_row, new_col,
     row_acc, send_row, send_col, recv_row, recv_col, send_upd, recv_upd, send_val, recv_val,
     swap_send, swap_recv) = refs[4 + 2 * n_piece:4 + 2 * n_piece + 15]
    staged = refs[4 + 2 * n_piece + 15:]
    rows, cols = grad.shape
    others = peers()
    row_peer, col_peer = others

    def swap(k, src, dst, other):
        return pltpu.make_async_remote_copy(src, dst, swap_send.at[k], swap_recv.at[k],
                                            device_id=other, device_id_type=MESH)

    barrier = pltpu.get_barrier_semaphore()
    for other in others:
        pl.semaphore_signal(barrier, inc=1, device_id=other, device_id_type=MESH)

    part, recv = parts[0], recvs[0]
    if staged:
        part, recv, load = staged
        loads = []
        for k, (top, left) in enumerate(boxes):
            box = (pl.ds(top, parts[k].shape[0]), pl.ds(left, parts[k].shape[1]))
            loads.append(pltpu.make_async_copy(recvs[k], recv.at[box], load.at[2 * k + 1]))
            if k >= near:
                loads.append(pltpu.make_async_copy(parts[k], part.at[box], load.at[2 * k]))
        for copy in loads:
            copy.start()
        for k, (top, left) in enumerate(boxes[:near]):
            width = parts[k].shape[1]

            def place(i, carry):
                src = pl.ds(pl.multiple_of(i * step, step), step)
                dst = pl.ds(pl.multiple_of(top + i * step, step), step)
                part[dst, left:left + width] = parts[k][src, :]
                return carry

            lax.fori_loop(0, parts[k].shape[0] // step, place, 0)
        for copy in loads:
            copy.wait()

    def first(i, col_acc):
        band = pl.ds(pl.multiple_of(i * step, step), step)
        piece = part[band, :] + recv[band, :]
        grad[band, :] = piece
        sq = piece * piece + EPS_ONE
        lane_sum = sq[:, :LANES]
        for j in range(1, cols // LANES):
            lane_sum = lane_sum + sq[:, j * LANES:(j + 1) * LANES]
        row_acc[band, :] = lane_sum
        return col_acc + sq.reshape(step // 8, 8, cols).sum(axis=0)

    col_acc = lax.fori_loop(0, rows // step, first, jnp.zeros((8, cols), jnp.float32))
    send_col[...] = jnp.sum(col_acc, axis=0, keepdims=True)
    pl.semaphore_wait(barrier, 2)
    row_copy = swap(0, send_row, recv_row, col_peer)
    col_copy = swap(1, send_col, recv_col, row_peer)
    col_copy.start()
    for k in range(rows // LANES):
        tile = row_acc[k * LANES:(k + 1) * LANES, :].T
        send_row[:, k * LANES:(k + 1) * LANES] = jnp.sum(tile, axis=0, keepdims=True)
    row_copy.start()
    beta_two = hyper[0:1, 0:1]

    col_copy.wait()
    col_now = beta_two * col_old[...] + (1.0 - beta_two) * ((send_col[...] + recv_col[...]) / m_total)
    new_col[...] = col_now
    col_inv = 1.0 / jnp.sqrt(col_now)

    def second(i, carry):
        band = pl.ds(pl.multiple_of(i * step, step), step)
        upd = grad[band, :] * col_inv
        grad[band, :] = upd
        sq = upd * upd
        lane_sum = sq[:, :LANES]
        for j in range(1, cols // LANES):
            lane_sum = lane_sum + sq[:, j * LANES:(j + 1) * LANES]
        row_acc[band, :] = lane_sum
        return carry

    lax.fori_loop(0, rows // step, second, 0)
    for k in range(rows // LANES):
        tile = row_acc[k * LANES:(k + 1) * LANES, :].T
        send_upd[:, k * LANES:(k + 1) * LANES] = jnp.sum(tile, axis=0, keepdims=True)
    lane = lax.broadcasted_iota(jnp.int32, (1, LANES), 1)
    send_upd[:, rows:] = jnp.where(lane == 0, w_sq[0, 0], 0.0)
    upd_copy = swap(2, send_upd, recv_upd, col_peer)
    upd_copy.start()

    row_copy.wait()
    row_now = beta_two * row_old[...] + (1.0 - beta_two) * ((send_row[...] + recv_row[...]) / n_total)
    new_row[...] = row_now
    row_inv = 1.0 / jnp.sqrt(row_now)
    row_part = jnp.zeros((1, LANES), jnp.float32)
    for k in range(rows // LANES):
        row_part = row_part + row_now[:, k * LANES:(k + 1) * LANES]
    if direct:
        for k in range(rows // LANES):
            band = pl.ds(k * LANES, LANES)
            scale = jnp.broadcast_to(row_inv[:, k * LANES:(k + 1) * LANES], (LANES, LANES)).T
            for j in range(cols // LANES):
                lanes = pl.ds(j * LANES, LANES)
                grad[band, lanes] = grad[band, lanes] * scale
    upd_copy.wait()
    upd_both = send_upd[...] + recv_upd[...]
    upd_sq = jnp.zeros((1, LANES), jnp.float32)
    for k in range(rows // LANES):
        inv = row_inv[:, k * LANES:(k + 1) * LANES]
        upd_sq = upd_sq + upd_both[:, k * LANES:(k + 1) * LANES] * (inv * inv)
    which = lax.broadcasted_iota(jnp.int32, (8, LANES), 0)
    send_val[...] = jnp.where(which == 0, upd_sq, jnp.where(which == 1, row_part, upd_both[:, rows:]))
    val_copy = swap(3, send_val, recv_val, row_peer)
    val_copy.start()
    val_copy.wait()
    total = jnp.sum(send_val[...] + recv_val[...], axis=1, keepdims=True)
    size = m_total * n_total
    row_total = total[1:2, :]
    upd_rms = jnp.sqrt(row_total * total[0:1, :] / size)
    w_rms = jnp.sqrt(total[2:3, :] / size)
    clip = jnp.maximum(1.0, upd_rms / hyper[2:3, 0:1])
    factor = hyper[1:2, 0:1] * jnp.maximum(EPS_TWO, w_rms) * jnp.sqrt(row_total) / clip
    if direct:
        row_scale[...] = jnp.broadcast_to(factor, (1, LANES))
    else:
        row_scale[...] = row_inv * factor


def head_kernel(row_start, col_start, n_x, *refs):
    refs = list(refs)
    x_bufs = [refs.pop(0) for _ in range(n_x)]
    dy_buf = refs.pop(0)
    out = refs.pop(0)
    loads = []
    if row_start is not None:
        source, x_bufs = x_bufs[0], [refs.pop(0)]
        loads.append((source, row_start, x_bufs[0]))
    if col_start is not None:
        source, dy_buf = dy_buf, refs.pop(0)
        loads.append((source, col_start, dy_buf))
    sem = refs.pop(0) if loads else None
    n_step = 8
    depth = dy_buf.shape[0] // n_step
    rows = x_bufs[0].shape[1]

    def copies(k):
        band = pl.ds(k * depth if isinstance(k, int) else pl.multiple_of(k * depth, depth), depth)
        return [pltpu.make_async_copy(source.at[band, pl.ds(start, buf.shape[1])], buf.at[band, :], sem.at[j, k])
                for j, (source, start, buf) in enumerate(loads)]

    def multiply(k, add):
        for copy in copies(k):
            copy.wait()
        band = pl.ds(k * depth if isinstance(k, int) else pl.multiple_of(k * depth, depth), depth)
        for j, x_buf in enumerate(x_bufs):
            own = pl.ds(j * rows, rows)
            term = lax.dot_general(x_buf[band, :], dy_buf[band, :], (((0,), (0,)), ((), ())),
                                   preferred_element_type=jnp.float32)
            if add:
                out[own, :] += term
            else:
                out[own, :] = term

    for k in range(n_step):
        for copy in copies(k):
            copy.start()
    if n_x == 1:
        for k in range(n_step):
            multiply(k, k > 0)
    else:
        out[...] = jnp.zeros_like(out)

        def follow(k, carry):
            multiply(k, True)
            return carry

        lax.fori_loop(0, n_step, follow, 0)


def head_product(x_blocks, dy_block, row_start, col_start, keep, limit):
    tokens = dy_block.shape[0]
    n_x = len(x_blocks)
    rows = 256 * n_x
    vmem = pl.BlockSpec(memory_space=pltpu.VMEM)
    anyw = pl.BlockSpec(memory_space=pl.ANY)
    x_far, dy_far = row_start is not None, col_start is not None
    held = jax.ShapeDtypeStruct((tokens, 256), dy_block.dtype)
    outs = [jax.ShapeDtypeStruct((rows, 256), jnp.float32)] + [held] * (x_far + (dy_far and keep))
    scratch = [pltpu.VMEM((tokens, 256), dy_block.dtype)] * (dy_far and not keep)
    if x_far or dy_far:
        scratch.append(pltpu.SemaphoreType.DMA((x_far + dy_far, 8)))
    far = [x_far] * n_x + [dy_far]
    operands = [pltpu.with_memory_space_constraint(v, pltpu.HBM if f else pltpu.VMEM)
                for v, f in zip(list(x_blocks) + [dy_block], far)]
    return pl.pallas_call(
        functools.partial(head_kernel, row_start, col_start, n_x),
        out_shape=outs,
        in_specs=[anyw if f else vmem for f in far],
        out_specs=[vmem] * len(outs),
        scratch_shapes=scratch,
        compiler_params=pltpu.CompilerParams(vmem_limit_bytes=limit),
        cost_estimate=pl.CostEstimate(flops=2 * tokens * rows * 256, bytes_accessed=2 * tokens * 256 * sum(far),
                                      transcendentals=0),
        name="head_product",
    )(*operands)


def emit_kernel(*refs):
    half = len(refs) // 2
    for src, dst in zip(refs[:half], refs[half:]):
        dst[...] = src[...]


def emit(values):
    vmem = pl.BlockSpec(memory_space=pltpu.VMEM)
    return pl.pallas_call(
        emit_kernel,
        out_shape=[jax.ShapeDtypeStruct(v.shape, v.dtype) for v in values],
        in_specs=[vmem] * len(values), out_specs=[vmem] * len(values),
        cost_estimate=pl.CostEstimate(flops=100000, bytes_accessed=8 * sum(v.size for v in values), transcendentals=0),
        compiler_params=pltpu.CompilerParams(vmem_limit_bytes=1024 * 1024),
        name="emit",
    )(*values)


def finish_kernel(weight, update, factor, row_in, col_in, new_weight, new_row, new_col, buf, sem):
    copies = [pltpu.make_async_copy(row_in, new_row, sem.at[0]), pltpu.make_async_copy(col_in, new_col, sem.at[1])]
    for copy in copies:
        copy.start()
    scale = factor[...]
    depth = weight.shape[0] // 4
    for k in range(4):
        band = pl.ds(k * depth, depth)
        for j in range(weight.shape[1] // LANES):
            lanes = pl.ds(j * LANES, LANES)
            buf[band, lanes] = weight[band, lanes] - update[band, lanes] * scale
        copies.append(pltpu.make_async_copy(buf.at[band, :], new_weight.at[band, :], sem.at[2 + k]))
        copies[-1].start()
    for copy in copies:
        copy.wait()


def finish(weight, update, factor, new_row, new_col):
    vmem = pl.BlockSpec(memory_space=pltpu.VMEM)
    anyw = pl.BlockSpec(memory_space=pl.ANY)
    return pl.pallas_call(
        finish_kernel,
        out_shape=[jax.ShapeDtypeStruct(v.shape, v.dtype) for v in (weight, new_row, new_col)],
        in_specs=[vmem] * 5, out_specs=[anyw] * 3,
        scratch_shapes=[pltpu.VMEM(weight.shape, weight.dtype), pltpu.SemaphoreType.DMA((6,))],
        cost_estimate=pl.CostEstimate(flops=100000, bytes_accessed=12 * weight.size, transcendentals=0),
        compiler_params=pltpu.CompilerParams(vmem_limit_bytes=6 * 1024 * 1024),
        name="finish",
    )(weight, update, factor, new_row, new_col)


def statistics(tokens, boxes, near, parts, recvs, w_sq, row_old, col_old, hyper, index):
    rows, cols = row_old.shape[0], col_old.shape[0]
    n_piece = len(parts)
    vmem = pl.BlockSpec(memory_space=pltpu.VMEM)
    smem = pl.BlockSpec(memory_space=pltpu.SMEM)
    anyw = pl.BlockSpec(memory_space=pl.ANY)
    f32 = jnp.float32
    staged = rows * cols > 500000
    near = near if staged else 1
    spaces = [pltpu.VMEM if k < near else pltpu.HBM for k in range(n_piece)]
    spaces += [pltpu.HBM if staged else pltpu.VMEM] * n_piece
    places = [pl.BlockSpec(memory_space=v) for v in spaces]
    stage = [pltpu.VMEM((rows, cols), f32)] * 2 + [pltpu.SemaphoreType.DMA((2 * n_piece,))] if staged else []
    halves = [pltpu.with_memory_space_constraint(v, space) for v, space in zip(parts + recvs, spaces)]
    shapes = ((rows, cols), (1, rows if staged else LANES), (1, rows), (1, cols))
    return pl.pallas_call(
        functools.partial(stats_kernel, len(tokens), boxes, near, not staged, 16 if staged else 64, 2 * rows, 2 * cols),
        out_shape=[jax.ShapeDtypeStruct(s, f32) for s in shapes],
        in_specs=[anyw] * len(tokens) + [smem] + [vmem] * 3 + places,
        out_specs=[vmem] * 4,
        scratch_shapes=[
            pltpu.VMEM((rows, LANES), f32),
            pltpu.VMEM((1, rows), f32), pltpu.VMEM((1, cols), f32),
            pltpu.VMEM((1, rows), f32), pltpu.VMEM((1, cols), f32),
            pltpu.VMEM((1, rows + LANES), f32), pltpu.VMEM((1, rows + LANES), f32),
            pltpu.VMEM((8, LANES), f32), pltpu.VMEM((8, LANES), f32),
            pltpu.SemaphoreType.DMA((4,)), pltpu.SemaphoreType.DMA((4,)),
        ] + stage,
        compiler_params=pltpu.CompilerParams(collective_id=index, has_side_effects=True,
                                             vmem_limit_bytes=16 * 1024 * 1024 if staged else 6 * 1024 * 1024),
        cost_estimate=pl.CostEstimate(flops=8 * rows * cols * 100, bytes_accessed=12 * rows * cols, transcendentals=0),
    )(*tokens, w_sq.reshape(1, 1), hyper, row_old.reshape(1, rows), col_old.reshape(1, cols), *halves)


def solution(mesh):
    act_spec = P('dp', 'row')
    grad_spec = P('dp', 'col')
    w_spec = P('row', 'col')
    row_spec = P('row')
    col_spec = P('col')
    in_specs = (act_spec, grad_spec, act_spec, grad_spec, grad_spec, act_spec, grad_spec,
                w_spec, w_spec, w_spec, w_spec,
                row_spec, col_spec, row_spec, col_spec, row_spec, col_spec, row_spec, col_spec, P())
    out_specs = (w_spec, row_spec, col_spec) * 4

    def product(x_block, dy_block):
        return jnp.einsum('tm,tn->mn', x_block, dy_block, preferred_element_type=jnp.float32)

    def per_device(x_attn, dy_attn, x_mlp, dy_gate, dy_up, h_mlp, dy_out, w_attn, w_gate, w_up, w_down,
                   r_attn, c_attn, r_gate, c_gate, r_up, c_up, r_down, c_down, hyper_params):
        order = [('gate', x_mlp, dy_gate, box) for box in GATE_BOXES]
        order += [('up', x_mlp, dy_up, None), ('down', h_mlp, dy_out, None), ('attn', x_attn, dy_attn, None)]
        parts = {name: [] for name in NAMES}
        recvs = {name: [] for name in NAMES}
        held = {}

        def head(held, number, x_block, dy_block):
            if number == 0:
                part, held['x0'], held['dy0'] = head_product([x_block], dy_block, 0, 0, True, 14 * MIB)
            elif number == 1:
                part, held['x1'] = head_product([x_block], held['dy0'], 256, None, True, 14 * MIB)
            elif number == 2:
                part, held['dy1'] = head_product([held['x0']], dy_block, None, 256, True, 14 * MIB)
            elif number == 3:
                part, = head_product([held['x1']], held['dy1'], None, None, True, 14 * MIB)
            else:
                part, = head_product([held['x0'], held['x1']], dy_block, None, GATE_BOXES[number][1], False, HEAD_LIMIT)
            return part

        before = None
        for number, (name, x_block, dy_block, box) in enumerate(order):
            if before is not None and number < N_HEAD:
                x_block, dy_block, held, before = lax.optimization_barrier((x_block, dy_block, held, before))
            elif before is not None:
                x_block, before = lax.optimization_barrier((x_block, before))
            if number < N_HEAD:
                before = head(held, number, x_block, dy_block)
            elif box is not None:
                before = product(x_block, dy_block[:, box[1]:box[1] + box[3]])
            else:
                before = product(x_block, dy_block)
            recvs[name].append(lax.ppermute(before, 'dp', SWAP))
            parts[name].append(before)
        results = {}
        hyper_rows = jnp.broadcast_to(jnp.pad(hyper_params, (0, 5))[:, None], (8, LANES))
        tokens = [parts['up'][0], parts['down'][0], parts['attn'][0]]
        weights = {'gate': w_gate, 'up': w_up, 'down': w_down, 'attn': w_attn}
        stats = {'gate': (r_gate, c_gate), 'up': (r_up, c_up), 'down': (r_down, c_down), 'attn': (r_attn, c_attn)}
        for index, name in enumerate(NAMES):
            weight = weights[name]
            rows, cols = weight.shape
            grad, row_scale, new_row, new_col = statistics(
                tokens, tuple(b[:2] for b in GATE_BOXES) if name == 'gate' else ((0, 0),),
                N_NEAR if name == 'gate' else 0, parts[name], recvs[name],
                jnp.sum(weight * weight), *stats[name], hyper_rows, index)
            if index < 3:
                new_weight = weight - grad * row_scale.reshape(rows, 1)
                new_row, new_col = emit((new_row, new_col))
            else:
                new_weight, new_row, new_col = finish(weight, grad, row_scale, new_row, new_col)
            results[name] = (new_weight, new_row.reshape(rows), new_col.reshape(cols))
            tokens = [new_weight, new_row, new_col]
        return results['attn'] + results['gate'] + results['up'] + results['down']

    return jax.shard_map(per_device, mesh=mesh, in_specs=in_specs, out_specs=out_specs, check_vma=False)
```

```python
import functools
import jax
import jax.numpy as jnp
from jax import lax
from jax.experimental import pallas as pl
from jax.experimental.pallas import tpu as pltpu
from jax.sharding import PartitionSpec as P

EPS_ONE = 1e-30
EPS_TWO = 1e-3
SWAP = [(0, 1), (1, 0)]
MESH = pl.DeviceIdType.MESH
LANES = 128
NAMES = ('gate', 'up', 'down', 'attn')
GATE_BOXES = ((0, 0, 256, 256), (256, 0, 256, 256), (0, 256, 256, 256), (256, 256, 256, 256),
              (0, 512, 512, 256), (0, 768, 512, 256), (0, 1024, 512, 384), (0, 1408, 512, 640))
N_HEAD = 6
N_NEAR = 4
N_COPY = 4
MIB = 1024 * 1024
HEAD_LIMIT = 50 * MIB


def peers():
    row_other = 1 - lax.axis_index('row')
    col_other = 1 - lax.axis_index('col')
    return ({'row': row_other}, {'col': col_other})


def stats_kernel(n_token, boxes, near, direct, step, m_total, n_total, *refs):
    n_piece = len(boxes)
    refs = refs[n_token:]
    w_sq, hyper, row_old, col_old = refs[:4]
    parts = refs[4:4 + n_piece]
    recvs = refs[4 + n_piece:4 + 2 * n_piece]
    (grad, row_scale, new_row, new_col,
     row_acc, send_row, send_col, recv_row, recv_col, send_upd, recv_upd, send_val, recv_val,
     swap_send, swap_recv) = refs[4 + 2 * n_piece:4 + 2 * n_piece + 15]
    staged = refs[4 + 2 * n_piece + 15:]
    rows, cols = grad.shape
    others = peers()
    row_peer, col_peer = others

    def swap(k, src, dst, other):
        return pltpu.make_async_remote_copy(src, dst, swap_send.at[k], swap_recv.at[k],
                                            device_id=other, device_id_type=MESH)

    barrier = pltpu.get_barrier_semaphore()
    for other in others:
        pl.semaphore_signal(barrier, inc=1, device_id=other, device_id_type=MESH)

    part, recv = parts[0], recvs[0]
    if staged:
        part, recv, load = staged
        loads = []
        for k, (top, left) in enumerate(boxes):
            box = (pl.ds(top, parts[k].shape[0]), pl.ds(left, parts[k].shape[1]))
            loads.append(pltpu.make_async_copy(recvs[k], recv.at[box], load.at[2 * k + 1]))
            if k >= near:
                loads.append(pltpu.make_async_copy(parts[k], part.at[box], load.at[2 * k]))
        for copy in loads:
            copy.start()
        for k, (top, left) in enumerate(boxes[:near]):
            width = parts[k].shape[1]

            def place(i, carry):
                src = pl.ds(pl.multiple_of(i * step, step), step)
                dst = pl.ds(pl.multiple_of(top + i * step, step), step)
                part[dst, left:left + width] = parts[k][src, :]
                return carry

            lax.fori_loop(0, parts[k].shape[0] // step, place, 0)
        for copy in loads:
            copy.wait()

    def first(i, col_acc):
        band = pl.ds(pl.multiple_of(i * step, step), step)
        piece = part[band, :] + recv[band, :]
        grad[band, :] = piece
        sq = piece * piece + EPS_ONE
        lane_sum = sq[:, :LANES]
        for j in range(1, cols // LANES):
            lane_sum = lane_sum + sq[:, j * LANES:(j + 1) * LANES]
        row_acc[band, :] = lane_sum
        return col_acc + sq.reshape(step // 8, 8, cols).sum(axis=0)

    col_acc = lax.fori_loop(0, rows // step, first, jnp.zeros((8, cols), jnp.float32))
    send_col[...] = jnp.sum(col_acc, axis=0, keepdims=True)
    pl.semaphore_wait(barrier, 2)
    row_copy = swap(0, send_row, recv_row, col_peer)
    col_copy = swap(1, send_col, recv_col, row_peer)
    col_copy.start()
    for k in range(rows // LANES):
        tile = row_acc[k * LANES:(k + 1) * LANES, :].T
        send_row[:, k * LANES:(k + 1) * LANES] = jnp.sum(tile, axis=0, keepdims=True)
    row_copy.start()
    beta_two = hyper[0:1, 0:1]

    col_copy.wait()
    col_now = beta_two * col_old[...] + (1.0 - beta_two) * ((send_col[...] + recv_col[...]) / m_total)
    new_col[...] = col_now
    col_inv = 1.0 / jnp.sqrt(col_now)

    def second(i, carry):
        band = pl.ds(pl.multiple_of(i * step, step), step)
        upd = grad[band, :] * col_inv
        grad[band, :] = upd
        sq = upd * upd
        lane_sum = sq[:, :LANES]
        for j in range(1, cols // LANES):
            lane_sum = lane_sum + sq[:, j * LANES:(j + 1) * LANES]
        row_acc[band, :] = lane_sum
        return carry

    lax.fori_loop(0, rows // step, second, 0)
    for k in range(rows // LANES):
        tile = row_acc[k * LANES:(k + 1) * LANES, :].T
        send_upd[:, k * LANES:(k + 1) * LANES] = jnp.sum(tile, axis=0, keepdims=True)
    lane = lax.broadcasted_iota(jnp.int32, (1, LANES), 1)
    send_upd[:, rows:] = jnp.where(lane == 0, w_sq[0, 0], 0.0)
    upd_copy = swap(2, send_upd, recv_upd, col_peer)
    upd_copy.start()

    row_copy.wait()
    row_now = beta_two * row_old[...] + (1.0 - beta_two) * ((send_row[...] + recv_row[...]) / n_total)
    new_row[...] = row_now
    row_inv = 1.0 / jnp.sqrt(row_now)
    row_part = jnp.zeros((1, LANES), jnp.float32)
    for k in range(rows // LANES):
        row_part = row_part + row_now[:, k * LANES:(k + 1) * LANES]
    if direct:
        for k in range(rows // LANES):
            band = pl.ds(k * LANES, LANES)
            scale = jnp.broadcast_to(row_inv[:, k * LANES:(k + 1) * LANES], (LANES, LANES)).T
            for j in range(cols // LANES):
                lanes = pl.ds(j * LANES, LANES)
                grad[band, lanes] = grad[band, lanes] * scale
    upd_copy.wait()
    upd_both = send_upd[...] + recv_upd[...]
    upd_sq = jnp.zeros((1, LANES), jnp.float32)
    for k in range(rows // LANES):
        inv = row_inv[:, k * LANES:(k + 1) * LANES]
        upd_sq = upd_sq + upd_both[:, k * LANES:(k + 1) * LANES] * (inv * inv)
    which = lax.broadcasted_iota(jnp.int32, (8, LANES), 0)
    send_val[...] = jnp.where(which == 0, upd_sq, jnp.where(which == 1, row_part, upd_both[:, rows:]))
    val_copy = swap(3, send_val, recv_val, row_peer)
    val_copy.start()
    val_copy.wait()
    total = jnp.sum(send_val[...] + recv_val[...], axis=1, keepdims=True)
    size = m_total * n_total
    row_total = total[1:2, :]
    upd_rms = jnp.sqrt(row_total * total[0:1, :] / size)
    w_rms = jnp.sqrt(total[2:3, :] / size)
    clip = jnp.maximum(1.0, upd_rms / hyper[2:3, 0:1])
    factor = hyper[1:2, 0:1] * jnp.maximum(EPS_TWO, w_rms) * jnp.sqrt(row_total) / clip
    if direct:
        row_scale[...] = jnp.broadcast_to(factor, (1, LANES))
    else:
        row_scale[...] = row_inv * factor


def head_kernel(row_start, col_start, n_x, *refs):
    refs = list(refs)
    x_bufs = [refs.pop(0) for _ in range(n_x)]
    dy_buf = refs.pop(0)
    out = refs.pop(0)
    loads = []
    if row_start is not None:
        source, x_bufs = x_bufs[0], [refs.pop(0)]
        loads.append((source, row_start, x_bufs[0]))
    if col_start is not None:
        source, dy_buf = dy_buf, refs.pop(0)
        loads.append((source, col_start, dy_buf))
    sem = refs.pop(0) if loads else None
    n_step = 8
    depth = dy_buf.shape[0] // n_step
    rows = x_bufs[0].shape[1]

    def copies(k):
        band = pl.ds(k * depth if isinstance(k, int) else pl.multiple_of(k * depth, depth), depth)
        return [pltpu.make_async_copy(source.at[band, pl.ds(start, buf.shape[1])], buf.at[band, :], sem.at[j, k])
                for j, (source, start, buf) in enumerate(loads)]

    def multiply(k, add):
        for copy in copies(k):
            copy.wait()
        band = pl.ds(k * depth if isinstance(k, int) else pl.multiple_of(k * depth, depth), depth)
        for j, x_buf in enumerate(x_bufs):
            own = pl.ds(j * rows, rows)
            term = lax.dot_general(x_buf[band, :], dy_buf[band, :], (((0,), (0,)), ((), ())),
                                   preferred_element_type=jnp.float32)
            if add:
                out[own, :] += term
            else:
                out[own, :] = term

    small = depth // N_COPY
    for k in range(n_step):
        for c in range(N_COPY):
            band = pl.ds(k * depth + c * small, small)
            for j, (source, start, buf) in enumerate(loads):
                pltpu.make_async_copy(source.at[band, pl.ds(start, buf.shape[1])], buf.at[band, :], sem.at[j, k]).start()
    if n_x == 1:
        for k in range(n_step):
            multiply(k, k > 0)
    else:
        out[...] = jnp.zeros_like(out)

        def follow(k, carry):
            multiply(k, True)
            return carry

        lax.fori_loop(0, n_step, follow, 0)


def head_product(x_blocks, dy_block, row_start, col_start, keep, limit):
    tokens = dy_block.shape[0]
    n_x = len(x_blocks)
    rows = 256 * n_x
    vmem = pl.BlockSpec(memory_space=pltpu.VMEM)
    anyw = pl.BlockSpec(memory_space=pl.ANY)
    x_far, dy_far = row_start is not None, col_start is not None
    held = jax.ShapeDtypeStruct((tokens, 256), dy_block.dtype)
    outs = [jax.ShapeDtypeStruct((rows, 256), jnp.float32)] + [held] * (x_far + (dy_far and keep))
    scratch = [pltpu.VMEM((tokens, 256), dy_block.dtype)] * (dy_far and not keep)
    if x_far or dy_far:
        scratch.append(pltpu.SemaphoreType.DMA((x_far + dy_far, 8)))
    far = [x_far] * n_x + [dy_far]
    operands = [pltpu.with_memory_space_constraint(v, pltpu.HBM if f else pltpu.VMEM)
                for v, f in zip(list(x_blocks) + [dy_block], far)]
    return pl.pallas_call(
        functools.partial(head_kernel, row_start, col_start, n_x),
        out_shape=outs,
        in_specs=[anyw if f else vmem for f in far],
        out_specs=[vmem] * len(outs),
        scratch_shapes=scratch,
        compiler_params=pltpu.CompilerParams(vmem_limit_bytes=limit),
        cost_estimate=pl.CostEstimate(flops=2 * tokens * rows * 256, bytes_accessed=2 * tokens * 256 * sum(far),
                                      transcendentals=0),
        name="head_product",
    )(*operands)


def emit_kernel(*refs):
    half = len(refs) // 2
    for src, dst in zip(refs[:half], refs[half:]):
        dst[...] = src[...]


def emit(values):
    vmem = pl.BlockSpec(memory_space=pltpu.VMEM)
    return pl.pallas_call(
        emit_kernel,
        out_shape=[jax.ShapeDtypeStruct(v.shape, v.dtype) for v in values],
        in_specs=[vmem] * len(values), out_specs=[vmem] * len(values),
        cost_estimate=pl.CostEstimate(flops=100000, bytes_accessed=8 * sum(v.size for v in values), transcendentals=0),
        compiler_params=pltpu.CompilerParams(vmem_limit_bytes=1024 * 1024),
        name="emit",
    )(*values)


def finish_kernel(weight, update, factor, row_in, col_in, new_weight, new_row, new_col, buf, sem):
    copies = [pltpu.make_async_copy(row_in, new_row, sem.at[0]), pltpu.make_async_copy(col_in, new_col, sem.at[1])]
    for copy in copies:
        copy.start()
    scale = factor[...]
    depth = weight.shape[0] // 4
    for k in range(4):
        band = pl.ds(k * depth, depth)
        for j in range(weight.shape[1] // LANES):
            lanes = pl.ds(j * LANES, LANES)
            buf[band, lanes] = weight[band, lanes] - update[band, lanes] * scale
        copies.append(pltpu.make_async_copy(buf.at[band, :], new_weight.at[band, :], sem.at[2 + k]))
        copies[-1].start()
    for copy in copies:
        copy.wait()


def finish(weight, update, factor, new_row, new_col):
    vmem = pl.BlockSpec(memory_space=pltpu.VMEM)
    anyw = pl.BlockSpec(memory_space=pl.ANY)
    return pl.pallas_call(
        finish_kernel,
        out_shape=[jax.ShapeDtypeStruct(v.shape, v.dtype) for v in (weight, new_row, new_col)],
        in_specs=[vmem] * 5, out_specs=[anyw] * 3,
        scratch_shapes=[pltpu.VMEM(weight.shape, weight.dtype), pltpu.SemaphoreType.DMA((6,))],
        cost_estimate=pl.CostEstimate(flops=100000, bytes_accessed=12 * weight.size, transcendentals=0),
        compiler_params=pltpu.CompilerParams(vmem_limit_bytes=6 * 1024 * 1024),
        name="finish",
    )(weight, update, factor, new_row, new_col)


def statistics(tokens, boxes, near, parts, recvs, w_sq, row_old, col_old, hyper, index):
    rows, cols = row_old.shape[0], col_old.shape[0]
    n_piece = len(parts)
    vmem = pl.BlockSpec(memory_space=pltpu.VMEM)
    smem = pl.BlockSpec(memory_space=pltpu.SMEM)
    anyw = pl.BlockSpec(memory_space=pl.ANY)
    f32 = jnp.float32
    staged = rows * cols > 500000
    near = near if staged else 1
    spaces = [pltpu.VMEM if k < near else pltpu.HBM for k in range(n_piece)]
    spaces += [pltpu.HBM if staged else pltpu.VMEM] * n_piece
    places = [pl.BlockSpec(memory_space=v) for v in spaces]
    stage = [pltpu.VMEM((rows, cols), f32)] * 2 + [pltpu.SemaphoreType.DMA((2 * n_piece,))] if staged else []
    halves = [pltpu.with_memory_space_constraint(v, space) for v, space in zip(parts + recvs, spaces)]
    shapes = ((rows, cols), (1, rows if staged else LANES), (1, rows), (1, cols))
    return pl.pallas_call(
        functools.partial(stats_kernel, len(tokens), boxes, near, not staged, 16 if staged else 64, 2 * rows, 2 * cols),
        out_shape=[jax.ShapeDtypeStruct(s, f32) for s in shapes],
        in_specs=[anyw] * len(tokens) + [smem] + [vmem] * 3 + places,
        out_specs=[vmem] * 4,
        scratch_shapes=[
            pltpu.VMEM((rows, LANES), f32),
            pltpu.VMEM((1, rows), f32), pltpu.VMEM((1, cols), f32),
            pltpu.VMEM((1, rows), f32), pltpu.VMEM((1, cols), f32),
            pltpu.VMEM((1, rows + LANES), f32), pltpu.VMEM((1, rows + LANES), f32),
            pltpu.VMEM((8, LANES), f32), pltpu.VMEM((8, LANES), f32),
            pltpu.SemaphoreType.DMA((4,)), pltpu.SemaphoreType.DMA((4,)),
        ] + stage,
        compiler_params=pltpu.CompilerParams(collective_id=index, has_side_effects=True,
                                             vmem_limit_bytes=16 * 1024 * 1024 if staged else 6 * 1024 * 1024),
        cost_estimate=pl.CostEstimate(flops=8 * rows * cols * 100, bytes_accessed=12 * rows * cols, transcendentals=0),
    )(*tokens, w_sq.reshape(1, 1), hyper, row_old.reshape(1, rows), col_old.reshape(1, cols), *halves)


def solution(mesh):
    act_spec = P('dp', 'row')
    grad_spec = P('dp', 'col')
    w_spec = P('row', 'col')
    row_spec = P('row')
    col_spec = P('col')
    in_specs = (act_spec, grad_spec, act_spec, grad_spec, grad_spec, act_spec, grad_spec,
                w_spec, w_spec, w_spec, w_spec,
                row_spec, col_spec, row_spec, col_spec, row_spec, col_spec, row_spec, col_spec, P())
    out_specs = (w_spec, row_spec, col_spec) * 4

    def product(x_block, dy_block):
        return jnp.einsum('tm,tn->mn', x_block, dy_block, preferred_element_type=jnp.float32)

    def per_device(x_attn, dy_attn, x_mlp, dy_gate, dy_up, h_mlp, dy_out, w_attn, w_gate, w_up, w_down,
                   r_attn, c_attn, r_gate, c_gate, r_up, c_up, r_down, c_down, hyper_params):
        order = [('gate', x_mlp, dy_gate, box) for box in GATE_BOXES]
        order += [('up', x_mlp, dy_up, None), ('down', h_mlp, dy_out, None), ('attn', x_attn, dy_attn, None)]
        parts = {name: [] for name in NAMES}
        recvs = {name: [] for name in NAMES}
        held = {}

        def head(held, number, x_block, dy_block):
            if number == 0:
                part, held['x0'], held['dy0'] = head_product([x_block], dy_block, 0, 0, True, 14 * MIB)
            elif number == 1:
                part, held['x1'] = head_product([x_block], held['dy0'], 256, None, True, 14 * MIB)
            elif number == 2:
                part, held['dy1'] = head_product([held['x0']], dy_block, None, 256, True, 14 * MIB)
            elif number == 3:
                part, = head_product([held['x1']], held['dy1'], None, None, True, 14 * MIB)
            else:
                part, = head_product([held['x0'], held['x1']], dy_block, None, GATE_BOXES[number][1], False, HEAD_LIMIT)
            return part

        before = None
        for number, (name, x_block, dy_block, box) in enumerate(order):
            if before is not None and number < N_HEAD:
                x_block, dy_block, held, before = lax.optimization_barrier((x_block, dy_block, held, before))
            elif before is not None:
                x_block, before = lax.optimization_barrier((x_block, before))
            if number < N_HEAD:
                before = head(held, number, x_block, dy_block)
            elif box is not None:
                before = product(x_block, dy_block[:, box[1]:box[1] + box[3]])
            else:
                before = product(x_block, dy_block)
            recvs[name].append(lax.ppermute(before, 'dp', SWAP))
            parts[name].append(before)
        results = {}
        hyper_rows = jnp.broadcast_to(jnp.pad(hyper_params, (0, 5))[:, None], (8, LANES))
        tokens = [parts['up'][0], parts['down'][0], parts['attn'][0]]
        weights = {'gate': w_gate, 'up': w_up, 'down': w_down, 'attn': w_attn}
        stats = {'gate': (r_gate, c_gate), 'up': (r_up, c_up), 'down': (r_down, c_down), 'attn': (r_attn, c_attn)}
        for index, name in enumerate(NAMES):
            weight = weights[name]
            rows, cols = weight.shape
            grad, row_scale, new_row, new_col = statistics(
                tokens, tuple(b[:2] for b in GATE_BOXES) if name == 'gate' else ((0, 0),),
                N_NEAR if name == 'gate' else 0, parts[name], recvs[name],
                jnp.sum(weight * weight), *stats[name], hyper_rows, index)
            if index < 3:
                new_weight = weight - grad * row_scale.reshape(rows, 1)
                new_row, new_col = emit((new_row, new_col))
            else:
                new_weight, new_row, new_col = finish(weight, grad, row_scale, new_row, new_col)
            results[name] = (new_weight, new_row.reshape(rows), new_col.reshape(cols))
            tokens = [new_weight, new_row, new_col]
        return results['attn'] + results['gate'] + results['up'] + results['down']

    return jax.shard_map(per_device, mesh=mesh, in_specs=in_specs, out_specs=out_specs, check_vma=False)
```

```python
import functools
import jax
import jax.numpy as jnp
from jax import lax
from jax.experimental import pallas as pl
from jax.experimental.pallas import tpu as pltpu
from jax.sharding import PartitionSpec as P

EPS_ONE = 1e-30
EPS_TWO = 1e-3
SWAP = [(0, 1), (1, 0)]
MESH = pl.DeviceIdType.MESH
LANES = 128
NAMES = ('gate', 'up', 'down', 'attn')
GATE_BOXES = ((0, 0, 256, 256), (256, 0, 256, 256), (0, 256, 256, 256), (256, 256, 256, 256),
              (0, 512, 512, 256), (0, 768, 512, 256), (0, 1024, 512, 384), (0, 1408, 512, 640))
N_HEAD = 6
N_NEAR = 4
STEPS = 16
MIB = 1024 * 1024
HEAD_LIMIT = 50 * MIB


def peers():
    row_other = 1 - lax.axis_index('row')
    col_other = 1 - lax.axis_index('col')
    return ({'row': row_other}, {'col': col_other})


def stats_kernel(n_token, boxes, near, direct, step, m_total, n_total, *refs):
    n_piece = len(boxes)
    refs = refs[n_token:]
    w_sq, hyper, row_old, col_old = refs[:4]
    parts = refs[4:4 + n_piece]
    recvs = refs[4 + n_piece:4 + 2 * n_piece]
    (grad, row_scale, new_row, new_col,
     row_acc, send_row, send_col, recv_row, recv_col, send_upd, recv_upd, send_val, recv_val,
     swap_send, swap_recv) = refs[4 + 2 * n_piece:4 + 2 * n_piece + 15]
    staged = refs[4 + 2 * n_piece + 15:]
    rows, cols = grad.shape
    others = peers()
    row_peer, col_peer = others

    def swap(k, src, dst, other):
        return pltpu.make_async_remote_copy(src, dst, swap_send.at[k], swap_recv.at[k],
                                            device_id=other, device_id_type=MESH)

    barrier = pltpu.get_barrier_semaphore()
    for other in others:
        pl.semaphore_signal(barrier, inc=1, device_id=other, device_id_type=MESH)

    part, recv = parts[0], recvs[0]
    if staged:
        part, recv, load = staged
        loads = []
        for k, (top, left) in enumerate(boxes):
            box = (pl.ds(top, parts[k].shape[0]), pl.ds(left, parts[k].shape[1]))
            loads.append(pltpu.make_async_copy(recvs[k], recv.at[box], load.at[2 * k + 1]))
            if k >= near:
                loads.append(pltpu.make_async_copy(parts[k], part.at[box], load.at[2 * k]))
        for copy in loads:
            copy.start()
        for k, (top, left) in enumerate(boxes[:near]):
            width = parts[k].shape[1]

            def place(i, carry):
                src = pl.ds(pl.multiple_of(i * step, step), step)
                dst = pl.ds(pl.multiple_of(top + i * step, step), step)
                part[dst, left:left + width] = parts[k][src, :]
                return carry

            lax.fori_loop(0, parts[k].shape[0] // step, place, 0)
        for copy in loads:
            copy.wait()

    def first(i, col_acc):
        band = pl.ds(pl.multiple_of(i * step, step), step)
        piece = part[band, :] + recv[band, :]
        grad[band, :] = piece
        sq = piece * piece + EPS_ONE
        lane_sum = sq[:, :LANES]
        for j in range(1, cols // LANES):
            lane_sum = lane_sum + sq[:, j * LANES:(j + 1) * LANES]
        row_acc[band, :] = lane_sum
        return col_acc + sq.reshape(step // 8, 8, cols).sum(axis=0)

    col_acc = lax.fori_loop(0, rows // step, first, jnp.zeros((8, cols), jnp.float32))
    send_col[...] = jnp.sum(col_acc, axis=0, keepdims=True)
    pl.semaphore_wait(barrier, 2)
    row_copy = swap(0, send_row, recv_row, col_peer)
    col_copy = swap(1, send_col, recv_col, row_peer)
    col_copy.start()
    for k in range(rows // LANES):
        tile = row_acc[k * LANES:(k + 1) * LANES, :].T
        send_row[:, k * LANES:(k + 1) * LANES] = jnp.sum(tile, axis=0, keepdims=True)
    row_copy.start()
    beta_two = hyper[0:1, 0:1]

    col_copy.wait()
    col_now = beta_two * col_old[...] + (1.0 - beta_two) * ((send_col[...] + recv_col[...]) / m_total)
    new_col[...] = col_now
    col_inv = 1.0 / jnp.sqrt(col_now)

    def second(i, carry):
        band = pl.ds(pl.multiple_of(i * step, step), step)
        upd = grad[band, :] * col_inv
        grad[band, :] = upd
        sq = upd * upd
        lane_sum = sq[:, :LANES]
        for j in range(1, cols // LANES):
            lane_sum = lane_sum + sq[:, j * LANES:(j + 1) * LANES]
        row_acc[band, :] = lane_sum
        return carry

    lax.fori_loop(0, rows // step, second, 0)
    for k in range(rows // LANES):
        tile = row_acc[k * LANES:(k + 1) * LANES, :].T
        send_upd[:, k * LANES:(k + 1) * LANES] = jnp.sum(tile, axis=0, keepdims=True)
    lane = lax.broadcasted_iota(jnp.int32, (1, LANES), 1)
    send_upd[:, rows:] = jnp.where(lane == 0, w_sq[0, 0], 0.0)
    upd_copy = swap(2, send_upd, recv_upd, col_peer)
    upd_copy.start()

    row_copy.wait()
    row_now = beta_two * row_old[...] + (1.0 - beta_two) * ((send_row[...] + recv_row[...]) / n_total)
    new_row[...] = row_now
    row_inv = 1.0 / jnp.sqrt(row_now)
    row_part = jnp.zeros((1, LANES), jnp.float32)
    for k in range(rows // LANES):
        row_part = row_part + row_now[:, k * LANES:(k + 1) * LANES]
    if direct:
        for k in range(rows // LANES):
            band = pl.ds(k * LANES, LANES)
            scale = jnp.broadcast_to(row_inv[:, k * LANES:(k + 1) * LANES], (LANES, LANES)).T
            for j in range(cols // LANES):
                lanes = pl.ds(j * LANES, LANES)
                grad[band, lanes] = grad[band, lanes] * scale
    upd_copy.wait()
    upd_both = send_upd[...] + recv_upd[...]
    upd_sq = jnp.zeros((1, LANES), jnp.float32)
    for k in range(rows // LANES):
        inv = row_inv[:, k * LANES:(k + 1) * LANES]
        upd_sq = upd_sq + upd_both[:, k * LANES:(k + 1) * LANES] * (inv * inv)
    which = lax.broadcasted_iota(jnp.int32, (8, LANES), 0)
    send_val[...] = jnp.where(which == 0, upd_sq, jnp.where(which == 1, row_part, upd_both[:, rows:]))
    val_copy = swap(3, send_val, recv_val, row_peer)
    val_copy.start()
    val_copy.wait()
    total = jnp.sum(send_val[...] + recv_val[...], axis=1, keepdims=True)
    size = m_total * n_total
    row_total = total[1:2, :]
    upd_rms = jnp.sqrt(row_total * total[0:1, :] / size)
    w_rms = jnp.sqrt(total[2:3, :] / size)
    clip = jnp.maximum(1.0, upd_rms / hyper[2:3, 0:1])
    factor = hyper[1:2, 0:1] * jnp.maximum(EPS_TWO, w_rms) * jnp.sqrt(row_total) / clip
    if direct:
        row_scale[...] = jnp.broadcast_to(factor, (1, LANES))
    else:
        row_scale[...] = row_inv * factor


def head_kernel(row_start, col_start, n_x, *refs):
    refs = list(refs)
    x_bufs = [refs.pop(0) for _ in range(n_x)]
    dy_buf = refs.pop(0)
    out = refs.pop(0)
    loads = []
    if row_start is not None:
        source, x_bufs = x_bufs[0], [refs.pop(0)]
        loads.append((source, row_start, x_bufs[0]))
    if col_start is not None:
        source, dy_buf = dy_buf, refs.pop(0)
        loads.append((source, col_start, dy_buf))
    sem = refs.pop(0) if loads else None
    n_step = STEPS if n_x == 1 and loads else 8
    window = n_step if n_x == 2 else (12 // max(1, len(loads)))
    depth = dy_buf.shape[0] // n_step
    rows = x_bufs[0].shape[1]

    def copies(k):
        band = pl.ds(k * depth if isinstance(k, int) else pl.multiple_of(k * depth, depth), depth)
        return [pltpu.make_async_copy(source.at[band, pl.ds(start, buf.shape[1])], buf.at[band, :], sem.at[j, k])
                for j, (source, start, buf) in enumerate(loads)]

    def begin(k):
        for copy in copies(k):
            copy.start()

    def multiply(k, add):
        for copy in copies(k):
            copy.wait()
        if isinstance(k, int) and k + window < n_step:
            begin(k + window)
        band = pl.ds(k * depth if isinstance(k, int) else pl.multiple_of(k * depth, depth), depth)
        for j, x_buf in enumerate(x_bufs):
            own = pl.ds(j * rows, rows)
            term = lax.dot_general(x_buf[band, :], dy_buf[band, :], (((0,), (0,)), ((), ())),
                                   preferred_element_type=jnp.float32)
            if add:
                out[own, :] += term
            else:
                out[own, :] = term

    for k in range(min(window, n_step)):
        begin(k)
    if n_x == 1:
        for k in range(n_step):
            multiply(k, k > 0)
    else:
        out[...] = jnp.zeros_like(out)

        def follow(k, carry):
            multiply(k, True)
            return carry

        lax.fori_loop(0, n_step, follow, 0)


def head_product(x_blocks, dy_block, row_start, col_start, keep, limit):
    tokens = dy_block.shape[0]
    n_x = len(x_blocks)
    rows = 256 * n_x
    vmem = pl.BlockSpec(memory_space=pltpu.VMEM)
    anyw = pl.BlockSpec(memory_space=pl.ANY)
    x_far, dy_far = row_start is not None, col_start is not None
    held = jax.ShapeDtypeStruct((tokens, 256), dy_block.dtype)
    outs = [jax.ShapeDtypeStruct((rows, 256), jnp.float32)] + [held] * (x_far + (dy_far and keep))
    scratch = [pltpu.VMEM((tokens, 256), dy_block.dtype)] * (dy_far and not keep)
    if x_far or dy_far:
        scratch.append(pltpu.SemaphoreType.DMA((x_far + dy_far, STEPS)))
    far = [x_far] * n_x + [dy_far]
    operands = [pltpu.with_memory_space_constraint(v, pltpu.HBM if f else pltpu.VMEM)
                for v, f in zip(list(x_blocks) + [dy_block], far)]
    return pl.pallas_call(
        functools.partial(head_kernel, row_start, col_start, n_x),
        out_shape=outs,
        in_specs=[anyw if f else vmem for f in far],
        out_specs=[vmem] * len(outs),
        scratch_shapes=scratch,
        compiler_params=pltpu.CompilerParams(vmem_limit_bytes=limit),
        cost_estimate=pl.CostEstimate(flops=2 * tokens * rows * 256, bytes_accessed=2 * tokens * 256 * sum(far),
                                      transcendentals=0),
        name="head_product",
    )(*operands)


def emit_kernel(*refs):
    half = len(refs) // 2
    for src, dst in zip(refs[:half], refs[half:]):
        dst[...] = src[...]


def emit(values):
    vmem = pl.BlockSpec(memory_space=pltpu.VMEM)
    return pl.pallas_call(
        emit_kernel,
        out_shape=[jax.ShapeDtypeStruct(v.shape, v.dtype) for v in values],
        in_specs=[vmem] * len(values), out_specs=[vmem] * len(values),
        cost_estimate=pl.CostEstimate(flops=100000, bytes_accessed=8 * sum(v.size for v in values), transcendentals=0),
        compiler_params=pltpu.CompilerParams(vmem_limit_bytes=1024 * 1024),
        name="emit",
    )(*values)


def finish_kernel(weight, update, factor, row_in, col_in, new_weight, new_row, new_col, buf, sem):
    copies = [pltpu.make_async_copy(row_in, new_row, sem.at[0]), pltpu.make_async_copy(col_in, new_col, sem.at[1])]
    for copy in copies:
        copy.start()
    scale = factor[...]
    depth = weight.shape[0] // 4
    for k in range(4):
        band = pl.ds(k * depth, depth)
        for j in range(weight.shape[1] // LANES):
            lanes = pl.ds(j * LANES, LANES)
            buf[band, lanes] = weight[band, lanes] - update[band, lanes] * scale
        copies.append(pltpu.make_async_copy(buf.at[band, :], new_weight.at[band, :], sem.at[2 + k]))
        copies[-1].start()
    for copy in copies:
        copy.wait()


def finish(weight, update, factor, new_row, new_col):
    vmem = pl.BlockSpec(memory_space=pltpu.VMEM)
    anyw = pl.BlockSpec(memory_space=pl.ANY)
    return pl.pallas_call(
        finish_kernel,
        out_shape=[jax.ShapeDtypeStruct(v.shape, v.dtype) for v in (weight, new_row, new_col)],
        in_specs=[vmem] * 5, out_specs=[anyw] * 3,
        scratch_shapes=[pltpu.VMEM(weight.shape, weight.dtype), pltpu.SemaphoreType.DMA((6,))],
        cost_estimate=pl.CostEstimate(flops=100000, bytes_accessed=12 * weight.size, transcendentals=0),
        compiler_params=pltpu.CompilerParams(vmem_limit_bytes=6 * 1024 * 1024),
        name="finish",
    )(weight, update, factor, new_row, new_col)


def statistics(tokens, boxes, near, parts, recvs, w_sq, row_old, col_old, hyper, index):
    rows, cols = row_old.shape[0], col_old.shape[0]
    n_piece = len(parts)
    vmem = pl.BlockSpec(memory_space=pltpu.VMEM)
    smem = pl.BlockSpec(memory_space=pltpu.SMEM)
    anyw = pl.BlockSpec(memory_space=pl.ANY)
    f32 = jnp.float32
    staged = rows * cols > 500000
    near = near if staged else 1
    spaces = [pltpu.VMEM if k < near else pltpu.HBM for k in range(n_piece)]
    spaces += [pltpu.HBM if staged else pltpu.VMEM] * n_piece
    places = [pl.BlockSpec(memory_space=v) for v in spaces]
    stage = [pltpu.VMEM((rows, cols), f32)] * 2 + [pltpu.SemaphoreType.DMA((2 * n_piece,))] if staged else []
    halves = [pltpu.with_memory_space_constraint(v, space) for v, space in zip(parts + recvs, spaces)]
    shapes = ((rows, cols), (1, rows if staged else LANES), (1, rows), (1, cols))
    return pl.pallas_call(
        functools.partial(stats_kernel, len(tokens), boxes, near, not staged, 16 if staged else 64, 2 * rows, 2 * cols),
        out_shape=[jax.ShapeDtypeStruct(s, f32) for s in shapes],
        in_specs=[anyw] * len(tokens) + [smem] + [vmem] * 3 + places,
        out_specs=[vmem] * 4,
        scratch_shapes=[
            pltpu.VMEM((rows, LANES), f32),
            pltpu.VMEM((1, rows), f32), pltpu.VMEM((1, cols), f32),
            pltpu.VMEM((1, rows), f32), pltpu.VMEM((1, cols), f32),
            pltpu.VMEM((1, rows + LANES), f32), pltpu.VMEM((1, rows + LANES), f32),
            pltpu.VMEM((8, LANES), f32), pltpu.VMEM((8, LANES), f32),
            pltpu.SemaphoreType.DMA((4,)), pltpu.SemaphoreType.DMA((4,)),
        ] + stage,
        compiler_params=pltpu.CompilerParams(collective_id=index, has_side_effects=True,
                                             vmem_limit_bytes=16 * 1024 * 1024 if staged else 6 * 1024 * 1024),
        cost_estimate=pl.CostEstimate(flops=8 * rows * cols * 100, bytes_accessed=12 * rows * cols, transcendentals=0),
    )(*tokens, w_sq.reshape(1, 1), hyper, row_old.reshape(1, rows), col_old.reshape(1, cols), *halves)


def solution(mesh):
    act_spec = P('dp', 'row')
    grad_spec = P('dp', 'col')
    w_spec = P('row', 'col')
    row_spec = P('row')
    col_spec = P('col')
    in_specs = (act_spec, grad_spec, act_spec, grad_spec, grad_spec, act_spec, grad_spec,
                w_spec, w_spec, w_spec, w_spec,
                row_spec, col_spec, row_spec, col_spec, row_spec, col_spec, row_spec, col_spec, P())
    out_specs = (w_spec, row_spec, col_spec) * 4

    def product(x_block, dy_block):
        return jnp.einsum('tm,tn->mn', x_block, dy_block, preferred_element_type=jnp.float32)

    def per_device(x_attn, dy_attn, x_mlp, dy_gate, dy_up, h_mlp, dy_out, w_attn, w_gate, w_up, w_down,
                   r_attn, c_attn, r_gate, c_gate, r_up, c_up, r_down, c_down, hyper_params):
        order = [('gate', x_mlp, dy_gate, box) for box in GATE_BOXES]
        order += [('up', x_mlp, dy_up, None), ('down', h_mlp, dy_out, None), ('attn', x_attn, dy_attn, None)]
        parts = {name: [] for name in NAMES}
        recvs = {name: [] for name in NAMES}
        held = {}

        def head(held, number, x_block, dy_block):
            if number == 0:
                part, held['x0'], held['dy0'] = head_product([x_block], dy_block, 0, 0, True, 14 * MIB)
            elif number == 1:
                part, held['x1'] = head_product([x_block], held['dy0'], 256, None, True, 14 * MIB)
            elif number == 2:
                part, held['dy1'] = head_product([held['x0']], dy_block, None, 256, True, 14 * MIB)
            elif number == 3:
                part, = head_product([held['x1']], held['dy1'], None, None, True, 14 * MIB)
            else:
                part, = head_product([held['x0'], held['x1']], dy_block, None, GATE_BOXES[number][1], False, HEAD_LIMIT)
            return part

        before = None
        for number, (name, x_block, dy_block, box) in enumerate(order):
            if before is not None and number < N_HEAD:
                x_block, dy_block, held, before = lax.optimization_barrier((x_block, dy_block, held, before))
            elif before is not None:
                x_block, before = lax.optimization_barrier((x_block, before))
            if number < N_HEAD:
                before = head(held, number, x_block, dy_block)
            elif box is not None:
                before = product(x_block, dy_block[:, box[1]:box[1] + box[3]])
            else:
                before = product(x_block, dy_block)
            recvs[name].append(lax.ppermute(before, 'dp', SWAP))
            parts[name].append(before)
        results = {}
        hyper_rows = jnp.broadcast_to(jnp.pad(hyper_params, (0, 5))[:, None], (8, LANES))
        tokens = [parts['up'][0], parts['down'][0], parts['attn'][0]]
        weights = {'gate': w_gate, 'up': w_up, 'down': w_down, 'attn': w_attn}
        stats = {'gate': (r_gate, c_gate), 'up': (r_up, c_up), 'down': (r_down, c_down), 'attn': (r_attn, c_attn)}
        for index, name in enumerate(NAMES):
            weight = weights[name]
            rows, cols = weight.shape
            grad, row_scale, new_row, new_col = statistics(
                tokens, tuple(b[:2] for b in GATE_BOXES) if name == 'gate' else ((0, 0),),
                N_NEAR if name == 'gate' else 0, parts[name], recvs[name],
                jnp.sum(weight * weight), *stats[name], hyper_rows, index)
            if index < 3:
                new_weight = weight - grad * row_scale.reshape(rows, 1)
                new_row, new_col = emit((new_row, new_col))
            else:
                new_weight, new_row, new_col = finish(weight, grad, row_scale, new_row, new_col)
            results[name] = (new_weight, new_row.reshape(rows), new_col.reshape(cols))
            tokens = [new_weight, new_row, new_col]
        return results['attn'] + results['gate'] + results['up'] + results['down']

    return jax.shard_map(per_device, mesh=mesh, in_specs=in_specs, out_specs=out_specs, check_vma=False)
```

```python
import functools
import jax
import jax.numpy as jnp
from jax import lax
from jax.experimental import pallas as pl
from jax.experimental.pallas import tpu as pltpu
from jax.sharding import PartitionSpec as P

EPS_ONE = 1e-30
EPS_TWO = 1e-3
SWAP = [(0, 1), (1, 0)]
MESH = pl.DeviceIdType.MESH
LANES = 128
NAMES = ('gate', 'up', 'down', 'attn')
GATE_BOXES = ((0, 0, 256, 256), (256, 0, 256, 256), (0, 256, 256, 256), (256, 256, 256, 256),
              (0, 512, 512, 256), (0, 768, 512, 256), (0, 1024, 512, 384), (0, 1408, 512, 640))
N_HEAD = 6
N_NEAR = 4
STEPS = 4
MIB = 1024 * 1024
HEAD_LIMIT = 50 * MIB


def peers():
    row_other = 1 - lax.axis_index('row')
    col_other = 1 - lax.axis_index('col')
    return ({'row': row_other}, {'col': col_other})


def stats_kernel(n_token, boxes, near, direct, step, m_total, n_total, *refs):
    n_piece = len(boxes)
    refs = refs[n_token:]
    w_sq, hyper, row_old, col_old = refs[:4]
    parts = refs[4:4 + n_piece]
    recvs = refs[4 + n_piece:4 + 2 * n_piece]
    (grad, row_scale, new_row, new_col,
     row_acc, send_row, send_col, recv_row, recv_col, send_upd, recv_upd, send_val, recv_val,
     swap_send, swap_recv) = refs[4 + 2 * n_piece:4 + 2 * n_piece + 15]
    staged = refs[4 + 2 * n_piece + 15:]
    rows, cols = grad.shape
    others = peers()
    row_peer, col_peer = others

    def swap(k, src, dst, other):
        return pltpu.make_async_remote_copy(src, dst, swap_send.at[k], swap_recv.at[k],
                                            device_id=other, device_id_type=MESH)

    barrier = pltpu.get_barrier_semaphore()
    for other in others:
        pl.semaphore_signal(barrier, inc=1, device_id=other, device_id_type=MESH)

    part, recv = parts[0], recvs[0]
    if staged:
        part, recv, load = staged
        loads = []
        for k, (top, left) in enumerate(boxes):
            box = (pl.ds(top, parts[k].shape[0]), pl.ds(left, parts[k].shape[1]))
            loads.append(pltpu.make_async_copy(recvs[k], recv.at[box], load.at[2 * k + 1]))
            if k >= near:
                loads.append(pltpu.make_async_copy(parts[k], part.at[box], load.at[2 * k]))
        for copy in loads:
            copy.start()
        for k, (top, left) in enumerate(boxes[:near]):
            width = parts[k].shape[1]

            def place(i, carry):
                src = pl.ds(pl.multiple_of(i * step, step), step)
                dst = pl.ds(pl.multiple_of(top + i * step, step), step)
                part[dst, left:left + width] = parts[k][src, :]
                return carry

            lax.fori_loop(0, parts[k].shape[0] // step, place, 0)
        for copy in loads:
            copy.wait()

    def first(i, col_acc):
        band = pl.ds(pl.multiple_of(i * step, step), step)
        piece = part[band, :] + recv[band, :]
        grad[band, :] = piece
        sq = piece * piece + EPS_ONE
        lane_sum = sq[:, :LANES]
        for j in range(1, cols // LANES):
            lane_sum = lane_sum + sq[:, j * LANES:(j + 1) * LANES]
        row_acc[band, :] = lane_sum
        return col_acc + sq.reshape(step // 8, 8, cols).sum(axis=0)

    col_acc = lax.fori_loop(0, rows // step, first, jnp.zeros((8, cols), jnp.float32))
    send_col[...] = jnp.sum(col_acc, axis=0, keepdims=True)
    pl.semaphore_wait(barrier, 2)
    row_copy = swap(0, send_row, recv_row, col_peer)
    col_copy = swap(1, send_col, recv_col, row_peer)
    col_copy.start()
    for k in range(rows // LANES):
        tile = row_acc[k * LANES:(k + 1) * LANES, :].T
        send_row[:, k * LANES:(k + 1) * LANES] = jnp.sum(tile, axis=0, keepdims=True)
    row_copy.start()
    beta_two = hyper[0:1, 0:1]

    col_copy.wait()
    col_now = beta_two * col_old[...] + (1.0 - beta_two) * ((send_col[...] + recv_col[...]) / m_total)
    new_col[...] = col_now
    col_inv = 1.0 / jnp.sqrt(col_now)

    def second(i, carry):
        band = pl.ds(pl.multiple_of(i * step, step), step)
        upd = grad[band, :] * col_inv
        grad[band, :] = upd
        sq = upd * upd
        lane_sum = sq[:, :LANES]
        for j in range(1, cols // LANES):
            lane_sum = lane_sum + sq[:, j * LANES:(j + 1) * LANES]
        row_acc[band, :] = lane_sum
        return carry

    lax.fori_loop(0, rows // step, second, 0)
    for k in range(rows // LANES):
        tile = row_acc[k * LANES:(k + 1) * LANES, :].T
        send_upd[:, k * LANES:(k + 1) * LANES] = jnp.sum(tile, axis=0, keepdims=True)
    lane = lax.broadcasted_iota(jnp.int32, (1, LANES), 1)
    send_upd[:, rows:] = jnp.where(lane == 0, w_sq[0, 0], 0.0)
    upd_copy = swap(2, send_upd, recv_upd, col_peer)
    upd_copy.start()

    row_copy.wait()
    row_now = beta_two * row_old[...] + (1.0 - beta_two) * ((send_row[...] + recv_row[...]) / n_total)
    new_row[...] = row_now
    row_inv = 1.0 / jnp.sqrt(row_now)
    row_part = jnp.zeros((1, LANES), jnp.float32)
    for k in range(rows // LANES):
        row_part = row_part + row_now[:, k * LANES:(k + 1) * LANES]
    if direct:
        for k in range(rows // LANES):
            band = pl.ds(k * LANES, LANES)
            scale = jnp.broadcast_to(row_inv[:, k * LANES:(k + 1) * LANES], (LANES, LANES)).T
            for j in range(cols // LANES):
                lanes = pl.ds(j * LANES, LANES)
                grad[band, lanes] = grad[band, lanes] * scale
    upd_copy.wait()
    upd_both = send_upd[...] + recv_upd[...]
    upd_sq = jnp.zeros((1, LANES), jnp.float32)
    for k in range(rows // LANES):
        inv = row_inv[:, k * LANES:(k + 1) * LANES]
        upd_sq = upd_sq + upd_both[:, k * LANES:(k + 1) * LANES] * (inv * inv)
    which = lax.broadcasted_iota(jnp.int32, (8, LANES), 0)
    send_val[...] = jnp.where(which == 0, upd_sq, jnp.where(which == 1, row_part, upd_both[:, rows:]))
    val_copy = swap(3, send_val, recv_val, row_peer)
    val_copy.start()
    val_copy.wait()
    total = jnp.sum(send_val[...] + recv_val[...], axis=1, keepdims=True)
    size = m_total * n_total
    row_total = total[1:2, :]
    upd_rms = jnp.sqrt(row_total * total[0:1, :] / size)
    w_rms = jnp.sqrt(total[2:3, :] / size)
    clip = jnp.maximum(1.0, upd_rms / hyper[2:3, 0:1])
    factor = hyper[1:2, 0:1] * jnp.maximum(EPS_TWO, w_rms) * jnp.sqrt(row_total) / clip
    if direct:
        row_scale[...] = jnp.broadcast_to(factor, (1, LANES))
    else:
        row_scale[...] = row_inv * factor


def head_kernel(row_start, col_start, n_x, *refs):
    refs = list(refs)
    x_bufs = [refs.pop(0) for _ in range(n_x)]
    dy_buf = refs.pop(0)
    out = refs.pop(0)
    loads = []
    if row_start is not None:
        source, x_bufs = x_bufs[0], [refs.pop(0)]
        loads.append((source, row_start, x_bufs[0]))
    if col_start is not None:
        source, dy_buf = dy_buf, refs.pop(0)
        loads.append((source, col_start, dy_buf))
    sem = refs.pop(0) if loads else None
    n_step = STEPS if loads and n_x == 1 else 8
    depth = dy_buf.shape[0] // n_step
    rows = x_bufs[0].shape[1]

    def copies(k):
        band = pl.ds(k * depth if isinstance(k, int) else pl.multiple_of(k * depth, depth), depth)
        return [pltpu.make_async_copy(source.at[band, pl.ds(start, buf.shape[1])], buf.at[band, :], sem.at[j, k])
                for j, (source, start, buf) in enumerate(loads)]

    def multiply(k, add):
        for copy in copies(k):
            copy.wait()
        band = pl.ds(k * depth if isinstance(k, int) else pl.multiple_of(k * depth, depth), depth)
        for j, x_buf in enumerate(x_bufs):
            own = pl.ds(j * rows, rows)
            term = lax.dot_general(x_buf[band, :], dy_buf[band, :], (((0,), (0,)), ((), ())),
                                   preferred_element_type=jnp.float32)
            if add:
                out[own, :] += term
            else:
                out[own, :] = term

    for k in range(n_step):
        for j, copy in enumerate(copies(k)):
            copy.start(priority=(k + j) % 2)
    if n_x == 1:
        for k in range(n_step):
            multiply(k, k > 0)
    else:
        out[...] = jnp.zeros_like(out)

        def follow(k, carry):
            multiply(k, True)
            return carry

        lax.fori_loop(0, n_step, follow, 0)


def head_product(x_blocks, dy_block, row_start, col_start, keep, limit):
    tokens = dy_block.shape[0]
    n_x = len(x_blocks)
    rows = 256 * n_x
    vmem = pl.BlockSpec(memory_space=pltpu.VMEM)
    anyw = pl.BlockSpec(memory_space=pl.ANY)
    x_far, dy_far = row_start is not None, col_start is not None
    held = jax.ShapeDtypeStruct((tokens, 256), dy_block.dtype)
    outs = [jax.ShapeDtypeStruct((rows, 256), jnp.float32)] + [held] * (x_far + (dy_far and keep))
    scratch = [pltpu.VMEM((tokens, 256), dy_block.dtype)] * (dy_far and not keep)
    if x_far or dy_far:
        scratch.append(pltpu.SemaphoreType.DMA((x_far + dy_far, 8)))
    far = [x_far] * n_x + [dy_far]
    operands = [pltpu.with_memory_space_constraint(v, pltpu.HBM if f else pltpu.VMEM)
                for v, f in zip(list(x_blocks) + [dy_block], far)]
    return pl.pallas_call(
        functools.partial(head_kernel, row_start, col_start, n_x),
        out_shape=outs,
        in_specs=[anyw if f else vmem for f in far],
        out_specs=[vmem] * len(outs),
        scratch_shapes=scratch,
        compiler_params=pltpu.CompilerParams(vmem_limit_bytes=limit),
        cost_estimate=pl.CostEstimate(flops=2 * tokens * rows * 256, bytes_accessed=2 * tokens * 256 * sum(far),
                                      transcendentals=0),
        name="head_product",
    )(*operands)


def emit_kernel(*refs):
    half = len(refs) // 2
    for src, dst in zip(refs[:half], refs[half:]):
        dst[...] = src[...]


def emit(values):
    vmem = pl.BlockSpec(memory_space=pltpu.VMEM)
    return pl.pallas_call(
        emit_kernel,
        out_shape=[jax.ShapeDtypeStruct(v.shape, v.dtype) for v in values],
        in_specs=[vmem] * len(values), out_specs=[vmem] * len(values),
        cost_estimate=pl.CostEstimate(flops=100000, bytes_accessed=8 * sum(v.size for v in values), transcendentals=0),
        compiler_params=pltpu.CompilerParams(vmem_limit_bytes=1024 * 1024),
        name="emit",
    )(*values)


def finish_kernel(weight, update, factor, row_in, col_in, new_weight, new_row, new_col, buf, sem):
    copies = [pltpu.make_async_copy(row_in, new_row, sem.at[0]), pltpu.make_async_copy(col_in, new_col, sem.at[1])]
    for copy in copies:
        copy.start()
    scale = factor[...]
    depth = weight.shape[0] // 4
    for k in range(4):
        band = pl.ds(k * depth, depth)
        for j in range(weight.shape[1] // LANES):
            lanes = pl.ds(j * LANES, LANES)
            buf[band, lanes] = weight[band, lanes] - update[band, lanes] * scale
        copies.append(pltpu.make_async_copy(buf.at[band, :], new_weight.at[band, :], sem.at[2 + k]))
        copies[-1].start()
    for copy in copies:
        copy.wait()


def finish(weight, update, factor, new_row, new_col):
    vmem = pl.BlockSpec(memory_space=pltpu.VMEM)
    anyw = pl.BlockSpec(memory_space=pl.ANY)
    return pl.pallas_call(
        finish_kernel,
        out_shape=[jax.ShapeDtypeStruct(v.shape, v.dtype) for v in (weight, new_row, new_col)],
        in_specs=[vmem] * 5, out_specs=[anyw] * 3,
        scratch_shapes=[pltpu.VMEM(weight.shape, weight.dtype), pltpu.SemaphoreType.DMA((6,))],
        cost_estimate=pl.CostEstimate(flops=100000, bytes_accessed=12 * weight.size, transcendentals=0),
        compiler_params=pltpu.CompilerParams(vmem_limit_bytes=6 * 1024 * 1024),
        name="finish",
    )(weight, update, factor, new_row, new_col)


def statistics(tokens, boxes, near, parts, recvs, w_sq, row_old, col_old, hyper, index):
    rows, cols = row_old.shape[0], col_old.shape[0]
    n_piece = len(parts)
    vmem = pl.BlockSpec(memory_space=pltpu.VMEM)
    smem = pl.BlockSpec(memory_space=pltpu.SMEM)
    anyw = pl.BlockSpec(memory_space=pl.ANY)
    f32 = jnp.float32
    staged = rows * cols > 500000
    near = near if staged else 1
    spaces = [pltpu.VMEM if k < near else pltpu.HBM for k in range(n_piece)]
    spaces += [pltpu.HBM if staged else pltpu.VMEM] * n_piece
    places = [pl.BlockSpec(memory_space=v) for v in spaces]
    stage = [pltpu.VMEM((rows, cols), f32)] * 2 + [pltpu.SemaphoreType.DMA((2 * n_piece,))] if staged else []
    halves = [pltpu.with_memory_space_constraint(v, space) for v, space in zip(parts + recvs, spaces)]
    shapes = ((rows, cols), (1, rows if staged else LANES), (1, rows), (1, cols))
    return pl.pallas_call(
        functools.partial(stats_kernel, len(tokens), boxes, near, not staged, 16 if staged else 64, 2 * rows, 2 * cols),
        out_shape=[jax.ShapeDtypeStruct(s, f32) for s in shapes],
        in_specs=[anyw] * len(tokens) + [smem] + [vmem] * 3 + places,
        out_specs=[vmem] * 4,
        scratch_shapes=[
            pltpu.VMEM((rows, LANES), f32),
            pltpu.VMEM((1, rows), f32), pltpu.VMEM((1, cols), f32),
            pltpu.VMEM((1, rows), f32), pltpu.VMEM((1, cols), f32),
            pltpu.VMEM((1, rows + LANES), f32), pltpu.VMEM((1, rows + LANES), f32),
            pltpu.VMEM((8, LANES), f32), pltpu.VMEM((8, LANES), f32),
            pltpu.SemaphoreType.DMA((4,)), pltpu.SemaphoreType.DMA((4,)),
        ] + stage,
        compiler_params=pltpu.CompilerParams(collective_id=index, has_side_effects=True,
                                             vmem_limit_bytes=16 * 1024 * 1024 if staged else 6 * 1024 * 1024),
        cost_estimate=pl.CostEstimate(flops=8 * rows * cols * 100, bytes_accessed=12 * rows * cols, transcendentals=0),
    )(*tokens, w_sq.reshape(1, 1), hyper, row_old.reshape(1, rows), col_old.reshape(1, cols), *halves)


def solution(mesh):
    act_spec = P('dp', 'row')
    grad_spec = P('dp', 'col')
    w_spec = P('row', 'col')
    row_spec = P('row')
    col_spec = P('col')
    in_specs = (act_spec, grad_spec, act_spec, grad_spec, grad_spec, act_spec, grad_spec,
                w_spec, w_spec, w_spec, w_spec,
                row_spec, col_spec, row_spec, col_spec, row_spec, col_spec, row_spec, col_spec, P())
    out_specs = (w_spec, row_spec, col_spec) * 4

    def product(x_block, dy_block):
        return jnp.einsum('tm,tn->mn', x_block, dy_block, preferred_element_type=jnp.float32)

    def per_device(x_attn, dy_attn, x_mlp, dy_gate, dy_up, h_mlp, dy_out, w_attn, w_gate, w_up, w_down,
                   r_attn, c_attn, r_gate, c_gate, r_up, c_up, r_down, c_down, hyper_params):
        order = [('gate', x_mlp, dy_gate, box) for box in GATE_BOXES]
        order += [('up', x_mlp, dy_up, None), ('down', h_mlp, dy_out, None), ('attn', x_attn, dy_attn, None)]
        parts = {name: [] for name in NAMES}
        recvs = {name: [] for name in NAMES}
        held = {}

        def head(held, number, x_block, dy_block):
            if number == 0:
                part, held['x0'], held['dy0'] = head_product([x_block], dy_block, 0, 0, True, 14 * MIB)
            elif number == 1:
                part, held['x1'] = head_product([x_block], held['dy0'], 256, None, True, 14 * MIB)
            elif number == 2:
                part, held['dy1'] = head_product([held['x0']], dy_block, None, 256, True, 14 * MIB)
            elif number == 3:
                part, = head_product([held['x1']], held['dy1'], None, None, True, 14 * MIB)
            else:
                part, = head_product([held['x0'], held['x1']], dy_block, None, GATE_BOXES[number][1], False, HEAD_LIMIT)
            return part

        before = None
        for number, (name, x_block, dy_block, box) in enumerate(order):
            if before is not None and number < N_HEAD:
                x_block, dy_block, held, before = lax.optimization_barrier((x_block, dy_block, held, before))
            elif before is not None:
                x_block, before = lax.optimization_barrier((x_block, before))
            if number < N_HEAD:
                before = head(held, number, x_block, dy_block)
            elif box is not None:
                before = product(x_block, dy_block[:, box[1]:box[1] + box[3]])
            else:
                before = product(x_block, dy_block)
            recvs[name].append(lax.ppermute(before, 'dp', SWAP))
            parts[name].append(before)
        results = {}
        hyper_rows = jnp.broadcast_to(jnp.pad(hyper_params, (0, 5))[:, None], (8, LANES))
        tokens = [parts['up'][0], parts['down'][0], parts['attn'][0]]
        weights = {'gate': w_gate, 'up': w_up, 'down': w_down, 'attn': w_attn}
        stats = {'gate': (r_gate, c_gate), 'up': (r_up, c_up), 'down': (r_down, c_down), 'attn': (r_attn, c_attn)}
        for index, name in enumerate(NAMES):
            weight = weights[name]
            rows, cols = weight.shape
            grad, row_scale, new_row, new_col = statistics(
                tokens, tuple(b[:2] for b in GATE_BOXES) if name == 'gate' else ((0, 0),),
                N_NEAR if name == 'gate' else 0, parts[name], recvs[name],
                jnp.sum(weight * weight), *stats[name], hyper_rows, index)
            if index < 3:
                new_weight = weight - grad * row_scale.reshape(rows, 1)
                new_row, new_col = emit((new_row, new_col))
            else:
                new_weight, new_row, new_col = finish(weight, grad, row_scale, new_row, new_col)
            results[name] = (new_weight, new_row.reshape(rows), new_col.reshape(cols))
            tokens = [new_weight, new_row, new_col]
        return results['attn'] + results['gate'] + results['up'] + results['down']

    return jax.shard_map(per_device, mesh=mesh, in_specs=in_specs, out_specs=out_specs, check_vma=False)
```

```python
import functools
import jax
import jax.numpy as jnp
from jax import lax
from jax.experimental import pallas as pl
from jax.experimental.pallas import tpu as pltpu
from jax.sharding import PartitionSpec as P

EPS_ONE = 1e-30
EPS_TWO = 1e-3
SWAP = [(0, 1), (1, 0)]
MESH = pl.DeviceIdType.MESH
LANES = 128
NAMES = ('gate', 'up', 'down', 'attn')
GATE_BOXES = ((0, 0, 256, 256), (256, 0, 256, 256), (0, 256, 256, 256), (256, 256, 256, 256),
              (0, 512, 512, 256), (0, 768, 512, 256), (0, 1024, 512, 384), (0, 1408, 512, 640))
N_HEAD = 6
N_NEAR = 4
MIB = 1024 * 1024
HEAD_LIMIT = 50 * MIB


def peers():
    row_other = 1 - lax.axis_index('row')
    col_other = 1 - lax.axis_index('col')
    return ({'row': row_other}, {'col': col_other})


def stats_kernel(n_token, boxes, near, direct, step, m_total, n_total, *refs):
    n_piece = len(boxes)
    refs = refs[n_token:]
    w_sq, hyper, row_old, col_old = refs[:4]
    parts = refs[4:4 + n_piece]
    recvs = refs[4 + n_piece:4 + 2 * n_piece]
    (grad, row_scale, new_row, new_col,
     row_acc, send_row, send_col, recv_row, recv_col, send_upd, recv_upd, send_val, recv_val,
     swap_send, swap_recv) = refs[4 + 2 * n_piece:4 + 2 * n_piece + 15]
    staged = refs[4 + 2 * n_piece + 15:]
    rows, cols = grad.shape
    others = peers()
    row_peer, col_peer = others

    def swap(k, src, dst, other):
        return pltpu.make_async_remote_copy(src, dst, swap_send.at[k], swap_recv.at[k],
                                            device_id=other, device_id_type=MESH)

    barrier = pltpu.get_barrier_semaphore()
    for other in others:
        pl.semaphore_signal(barrier, inc=1, device_id=other, device_id_type=MESH)

    part, recv = parts[0], recvs[0]
    if staged:
        part, recv, load = staged
        loads = []
        for k, (top, left) in enumerate(boxes):
            box = (pl.ds(top, parts[k].shape[0]), pl.ds(left, parts[k].shape[1]))
            loads.append(pltpu.make_async_copy(recvs[k], recv.at[box], load.at[2 * k + 1]))
            if k >= near:
                loads.append(pltpu.make_async_copy(parts[k], part.at[box], load.at[2 * k]))
        for copy in loads:
            copy.start()
        for k, (top, left) in enumerate(boxes[:near]):
            width = parts[k].shape[1]

            def place(i, carry):
                src = pl.ds(pl.multiple_of(i * step, step), step)
                dst = pl.ds(pl.multiple_of(top + i * step, step), step)
                part[dst, left:left + width] = parts[k][src, :]
                return carry

            lax.fori_loop(0, parts[k].shape[0] // step, place, 0)
        for copy in loads:
            copy.wait()

    def first(i, col_acc):
        band = pl.ds(pl.multiple_of(i * step, step), step)
        piece = part[band, :] + recv[band, :]
        grad[band, :] = piece
        sq = piece * piece + EPS_ONE
        lane_sum = sq[:, :LANES]
        for j in range(1, cols // LANES):
            lane_sum = lane_sum + sq[:, j * LANES:(j + 1) * LANES]
        row_acc[band, :] = lane_sum
        return col_acc + sq.reshape(step // 8, 8, cols).sum(axis=0)

    col_acc = lax.fori_loop(0, rows // step, first, jnp.zeros((8, cols), jnp.float32))
    send_col[...] = jnp.sum(col_acc, axis=0, keepdims=True)
    pl.semaphore_wait(barrier, 2)
    row_copy = swap(0, send_row, recv_row, col_peer)
    col_copy = swap(1, send_col, recv_col, row_peer)
    col_copy.start()
    for k in range(rows // LANES):
        tile = row_acc[k * LANES:(k + 1) * LANES, :].T
        send_row[:, k * LANES:(k + 1) * LANES] = jnp.sum(tile, axis=0, keepdims=True)
    row_copy.start()
    beta_two = hyper[0:1, 0:1]

    col_copy.wait()
    col_now = beta_two * col_old[...] + (1.0 - beta_two) * ((send_col[...] + recv_col[...]) / m_total)
    new_col[...] = col_now
    col_inv = 1.0 / jnp.sqrt(col_now)

    def second(i, carry):
        band = pl.ds(pl.multiple_of(i * step, step), step)
        upd = grad[band, :] * col_inv
        grad[band, :] = upd
        sq = upd * upd
        lane_sum = sq[:, :LANES]
        for j in range(1, cols // LANES):
            lane_sum = lane_sum + sq[:, j * LANES:(j + 1) * LANES]
        row_acc[band, :] = lane_sum
        return carry

    if direct:
        for k in range(rows // LANES):
            band = pl.ds(k * LANES, LANES)
            lane_sum = None
            for j in range(cols // LANES):
                lanes = pl.ds(j * LANES, LANES)
                upd = grad[band, lanes] * col_inv[:, j * LANES:(j + 1) * LANES]
                grad[band, lanes] = upd
                lane_sum = upd * upd if j == 0 else lane_sum + upd * upd
            send_upd[:, k * LANES:(k + 1) * LANES] = jnp.sum(lane_sum.T, axis=0, keepdims=True)
    else:
        lax.fori_loop(0, rows // step, second, 0)
        for k in range(rows // LANES):
            tile = row_acc[k * LANES:(k + 1) * LANES, :].T
            send_upd[:, k * LANES:(k + 1) * LANES] = jnp.sum(tile, axis=0, keepdims=True)
    lane = lax.broadcasted_iota(jnp.int32, (1, LANES), 1)
    send_upd[:, rows:] = jnp.where(lane == 0, w_sq[0, 0], 0.0)
    upd_copy = swap(2, send_upd, recv_upd, col_peer)
    upd_copy.start()

    row_copy.wait()
    row_now = beta_two * row_old[...] + (1.0 - beta_two) * ((send_row[...] + recv_row[...]) / n_total)
    new_row[...] = row_now
    row_inv = 1.0 / jnp.sqrt(row_now)
    row_part = jnp.zeros((1, LANES), jnp.float32)
    for k in range(rows // LANES):
        row_part = row_part + row_now[:, k * LANES:(k + 1) * LANES]
    if direct:
        for k in range(rows // LANES):
            band = pl.ds(k * LANES, LANES)
            scale = jnp.broadcast_to(row_inv[:, k * LANES:(k + 1) * LANES], (LANES, LANES)).T
            for j in range(cols // LANES):
                lanes = pl.ds(j * LANES, LANES)
                grad[band, lanes] = grad[band, lanes] * scale
    upd_copy.wait()
    upd_both = send_upd[...] + recv_upd[...]
    upd_sq = jnp.zeros((1, LANES), jnp.float32)
    for k in range(rows // LANES):
        inv = row_inv[:, k * LANES:(k + 1) * LANES]
        upd_sq = upd_sq + upd_both[:, k * LANES:(k + 1) * LANES] * (inv * inv)
    which = lax.broadcasted_iota(jnp.int32, (8, LANES), 0)
    send_val[...] = jnp.where(which == 0, upd_sq, jnp.where(which == 1, row_part, upd_both[:, rows:]))
    val_copy = swap(3, send_val, recv_val, row_peer)
    val_copy.start()
    val_copy.wait()
    total = jnp.sum(send_val[...] + recv_val[...], axis=1, keepdims=True)
    size = m_total * n_total
    row_total = total[1:2, :]
    upd_rms = jnp.sqrt(row_total * total[0:1, :] / size)
    w_rms = jnp.sqrt(total[2:3, :] / size)
    clip = jnp.maximum(1.0, upd_rms / hyper[2:3, 0:1])
    factor = hyper[1:2, 0:1] * jnp.maximum(EPS_TWO, w_rms) * jnp.sqrt(row_total) / clip
    if direct:
        row_scale[...] = jnp.broadcast_to(factor, (1, LANES))
    else:
        row_scale[...] = row_inv * factor


def head_kernel(row_start, col_start, n_x, *refs):
    refs = list(refs)
    x_bufs = [refs.pop(0) for _ in range(n_x)]
    dy_buf = refs.pop(0)
    out = refs.pop(0)
    loads = []
    if row_start is not None:
        source, x_bufs = x_bufs[0], [refs.pop(0)]
        loads.append((source, row_start, x_bufs[0]))
    if col_start is not None:
        source, dy_buf = dy_buf, refs.pop(0)
        loads.append((source, col_start, dy_buf))
    sem = refs.pop(0) if loads else None
    n_step = 8
    depth = dy_buf.shape[0] // n_step
    rows = x_bufs[0].shape[1]

    def copies(k):
        band = pl.ds(k * depth if isinstance(k, int) else pl.multiple_of(k * depth, depth), depth)
        return [pltpu.make_async_copy(source.at[band, pl.ds(start, buf.shape[1])], buf.at[band, :], sem.at[j, k])
                for j, (source, start, buf) in enumerate(loads)]

    def multiply(k, add):
        for copy in copies(k):
            copy.wait()
        band = pl.ds(k * depth if isinstance(k, int) else pl.multiple_of(k * depth, depth), depth)
        for j, x_buf in enumerate(x_bufs):
            own = pl.ds(j * rows, rows)
            term = lax.dot_general(x_buf[band, :], dy_buf[band, :], (((0,), (0,)), ((), ())),
                                   preferred_element_type=jnp.float32)
            if add:
                out[own, :] += term
            else:
                out[own, :] = term

    for k in range(n_step):
        for copy in copies(k):
            copy.start()
    if n_x == 1:
        for k in range(n_step):
            multiply(k, k > 0)
    else:
        out[...] = jnp.zeros_like(out)

        def follow(k, carry):
            multiply(k, True)
            return carry

        lax.fori_loop(0, n_step, follow, 0)


def head_product(x_blocks, dy_block, row_start, col_start, keep, limit):
    tokens = dy_block.shape[0]
    n_x = len(x_blocks)
    rows = 256 * n_x
    vmem = pl.BlockSpec(memory_space=pltpu.VMEM)
    anyw = pl.BlockSpec(memory_space=pl.ANY)
    x_far, dy_far = row_start is not None, col_start is not None
    held = jax.ShapeDtypeStruct((tokens, 256), dy_block.dtype)
    outs = [jax.ShapeDtypeStruct((rows, 256), jnp.float32)] + [held] * (x_far + (dy_far and keep))
    scratch = [pltpu.VMEM((tokens, 256), dy_block.dtype)] * (dy_far and not keep)
    if x_far or dy_far:
        scratch.append(pltpu.SemaphoreType.DMA((x_far + dy_far, 8)))
    far = [x_far] * n_x + [dy_far]
    operands = [pltpu.with_memory_space_constraint(v, pltpu.HBM if f else pltpu.VMEM)
                for v, f in zip(list(x_blocks) + [dy_block], far)]
    return pl.pallas_call(
        functools.partial(head_kernel, row_start, col_start, n_x),
        out_shape=outs,
        in_specs=[anyw if f else vmem for f in far],
        out_specs=[vmem] * len(outs),
        scratch_shapes=scratch,
        compiler_params=pltpu.CompilerParams(vmem_limit_bytes=limit),
        cost_estimate=pl.CostEstimate(flops=2 * tokens * rows * 256, bytes_accessed=2 * tokens * 256 * sum(far),
                                      transcendentals=0),
        name="head_product",
    )(*operands)


def emit_kernel(*refs):
    half = len(refs) // 2
    for src, dst in zip(refs[:half], refs[half:]):
        dst[...] = src[...]


def emit(values):
    vmem = pl.BlockSpec(memory_space=pltpu.VMEM)
    return pl.pallas_call(
        emit_kernel,
        out_shape=[jax.ShapeDtypeStruct(v.shape, v.dtype) for v in values],
        in_specs=[vmem] * len(values), out_specs=[vmem] * len(values),
        cost_estimate=pl.CostEstimate(flops=100000, bytes_accessed=8 * sum(v.size for v in values), transcendentals=0),
        compiler_params=pltpu.CompilerParams(vmem_limit_bytes=1024 * 1024),
        name="emit",
    )(*values)


def finish_kernel(weight, update, factor, row_in, col_in, new_weight, new_row, new_col, buf, sem):
    copies = [pltpu.make_async_copy(row_in, new_row, sem.at[0]), pltpu.make_async_copy(col_in, new_col, sem.at[1])]
    for copy in copies:
        copy.start()
    scale = factor[...]
    depth = weight.shape[0] // 4
    for k in range(4):
        band = pl.ds(k * depth, depth)
        for j in range(weight.shape[1] // LANES):
            lanes = pl.ds(j * LANES, LANES)
            buf[band, lanes] = weight[band, lanes] - update[band, lanes] * scale
        copies.append(pltpu.make_async_copy(buf.at[band, :], new_weight.at[band, :], sem.at[2 + k]))
        copies[-1].start()
    for copy in copies:
        copy.wait()


def finish(weight, update, factor, new_row, new_col):
    vmem = pl.BlockSpec(memory_space=pltpu.VMEM)
    anyw = pl.BlockSpec(memory_space=pl.ANY)
    return pl.pallas_call(
        finish_kernel,
        out_shape=[jax.ShapeDtypeStruct(v.shape, v.dtype) for v in (weight, new_row, new_col)],
        in_specs=[vmem] * 5, out_specs=[anyw] * 3,
        scratch_shapes=[pltpu.VMEM(weight.shape, weight.dtype), pltpu.SemaphoreType.DMA((6,))],
        cost_estimate=pl.CostEstimate(flops=100000, bytes_accessed=12 * weight.size, transcendentals=0),
        compiler_params=pltpu.CompilerParams(vmem_limit_bytes=6 * 1024 * 1024),
        name="finish",
    )(weight, update, factor, new_row, new_col)


def statistics(tokens, boxes, near, parts, recvs, w_sq, row_old, col_old, hyper, index):
    rows, cols = row_old.shape[0], col_old.shape[0]
    n_piece = len(parts)
    vmem = pl.BlockSpec(memory_space=pltpu.VMEM)
    smem = pl.BlockSpec(memory_space=pltpu.SMEM)
    anyw = pl.BlockSpec(memory_space=pl.ANY)
    f32 = jnp.float32
    staged = rows * cols > 500000
    near = near if staged else 1
    spaces = [pltpu.VMEM if k < near else pltpu.HBM for k in range(n_piece)]
    spaces += [pltpu.HBM if staged else pltpu.VMEM] * n_piece
    places = [pl.BlockSpec(memory_space=v) for v in spaces]
    stage = [pltpu.VMEM((rows, cols), f32)] * 2 + [pltpu.SemaphoreType.DMA((2 * n_piece,))] if staged else []
    halves = [pltpu.with_memory_space_constraint(v, space) for v, space in zip(parts + recvs, spaces)]
    shapes = ((rows, cols), (1, rows if staged else LANES), (1, rows), (1, cols))
    return pl.pallas_call(
        functools.partial(stats_kernel, len(tokens), boxes, near, not staged, 16 if staged else 64, 2 * rows, 2 * cols),
        out_shape=[jax.ShapeDtypeStruct(s, f32) for s in shapes],
        in_specs=[anyw] * len(tokens) + [smem] + [vmem] * 3 + places,
        out_specs=[vmem] * 4,
        scratch_shapes=[
            pltpu.VMEM((rows, LANES), f32),
            pltpu.VMEM((1, rows), f32), pltpu.VMEM((1, cols), f32),
            pltpu.VMEM((1, rows), f32), pltpu.VMEM((1, cols), f32),
            pltpu.VMEM((1, rows + LANES), f32), pltpu.VMEM((1, rows + LANES), f32),
            pltpu.VMEM((8, LANES), f32), pltpu.VMEM((8, LANES), f32),
            pltpu.SemaphoreType.DMA((4,)), pltpu.SemaphoreType.DMA((4,)),
        ] + stage,
        compiler_params=pltpu.CompilerParams(collective_id=index, has_side_effects=True,
                                             vmem_limit_bytes=16 * 1024 * 1024 if staged else 6 * 1024 * 1024),
        cost_estimate=pl.CostEstimate(flops=8 * rows * cols * 100, bytes_accessed=12 * rows * cols, transcendentals=0),
    )(*tokens, w_sq.reshape(1, 1), hyper, row_old.reshape(1, rows), col_old.reshape(1, cols), *halves)


def solution(mesh):
    act_spec = P('dp', 'row')
    grad_spec = P('dp', 'col')
    w_spec = P('row', 'col')
    row_spec = P('row')
    col_spec = P('col')
    in_specs = (act_spec, grad_spec, act_spec, grad_spec, grad_spec, act_spec, grad_spec,
                w_spec, w_spec, w_spec, w_spec,
                row_spec, col_spec, row_spec, col_spec, row_spec, col_spec, row_spec, col_spec, P())
    out_specs = (w_spec, row_spec, col_spec) * 4

    def product(x_block, dy_block):
        return jnp.einsum('tm,tn->mn', x_block, dy_block, preferred_element_type=jnp.float32)

    def per_device(x_attn, dy_attn, x_mlp, dy_gate, dy_up, h_mlp, dy_out, w_attn, w_gate, w_up, w_down,
                   r_attn, c_attn, r_gate, c_gate, r_up, c_up, r_down, c_down, hyper_params):
        order = [('gate', x_mlp, dy_gate, box) for box in GATE_BOXES]
        order += [('up', x_mlp, dy_up, None), ('down', h_mlp, dy_out, None), ('attn', x_attn, dy_attn, None)]
        parts = {name: [] for name in NAMES}
        recvs = {name: [] for name in NAMES}
        held = {}

        def head(held, number, x_block, dy_block):
            if number == 0:
                part, held['x0'], held['dy0'] = head_product([x_block], dy_block, 0, 0, True, 14 * MIB)
            elif number == 1:
                part, held['x1'] = head_product([x_block], held['dy0'], 256, None, True, 14 * MIB)
            elif number == 2:
                part, held['dy1'] = head_product([held['x0']], dy_block, None, 256, True, 14 * MIB)
            elif number == 3:
                part, = head_product([held['x1']], held['dy1'], None, None, True, 14 * MIB)
            else:
                part, = head_product([held['x0'], held['x1']], dy_block, None, GATE_BOXES[number][1], False, HEAD_LIMIT)
            return part

        before = None
        for number, (name, x_block, dy_block, box) in enumerate(order):
            if before is not None and number < N_HEAD:
                x_block, dy_block, held, before = lax.optimization_barrier((x_block, dy_block, held, before))
            elif before is not None:
                x_block, before = lax.optimization_barrier((x_block, before))
            if number < N_HEAD:
                before = head(held, number, x_block, dy_block)
            elif box is not None:
                before = product(x_block, dy_block[:, box[1]:box[1] + box[3]])
            else:
                before = product(x_block, dy_block)
            recvs[name].append(lax.ppermute(before, 'dp', SWAP))
            parts[name].append(before)
        results = {}
        hyper_rows = jnp.broadcast_to(jnp.pad(hyper_params, (0, 5))[:, None], (8, LANES))
        tokens = [parts['up'][0], parts['down'][0], parts['attn'][0]]
        weights = {'gate': w_gate, 'up': w_up, 'down': w_down, 'attn': w_attn}
        stats = {'gate': (r_gate, c_gate), 'up': (r_up, c_up), 'down': (r_down, c_down), 'attn': (r_attn, c_attn)}
        for index, name in enumerate(NAMES):
            weight = weights[name]
            rows, cols = weight.shape
            grad, row_scale, new_row, new_col = statistics(
                tokens, tuple(b[:2] for b in GATE_BOXES) if name == 'gate' else ((0, 0),),
                N_NEAR if name == 'gate' else 0, parts[name], recvs[name],
                jnp.sum(weight * weight), *stats[name], hyper_rows, index)
            if index < 3:
                new_weight = weight - grad * row_scale.reshape(rows, 1)
                new_row, new_col = emit((new_row, new_col))
            else:
                new_weight, new_row, new_col = finish(weight, grad, row_scale, new_row, new_col)
            results[name] = (new_weight, new_row.reshape(rows), new_col.reshape(cols))
            tokens = [new_weight, new_row, new_col]
        return results['attn'] + results['gate'] + results['up'] + results['down']

    return jax.shard_map(per_device, mesh=mesh, in_specs=in_specs, out_specs=out_specs, check_vma=False)
```
